8 devices in a mesh: data: 4 (over z, y, x), stage: 2 (over core).
Axes of the slice: x: 2, y: 2, z: 1, core: 2. Of those that a mesh axis runs over, the one named last changes fastest.
Arguments:
- x: bfloat16 [4, 32, 32, 2048], P(None, 'data')
- g: bfloat16 [4, 32, 32, 2048], P(None, 'data')
- w_gate: bfloat16 [2, 1, 2048, 8192], P('stage', None, 'data')
- w_in: bfloat16 [2, 1, 2048, 8192], P('stage', None, 'data')
- w_out: bfloat16 [2, 1, 8192, 2048], P('stage', None, 'data')
Outputs:
- output 1: bfloat16 [4, 32, 32, 2048], P(None, 'data')
- output 2: float32 [2, 1, 2048, 8192], P('stage', None, 'data')
- output 3: float32 [2, 1, 2048, 8192], P('stage', None, 'data')
- output 4: float32 [2, 1, 8192, 2048], P('stage', None, 'data')
All inputs are finite; a program needn't handle non-finite values.
Results may differ from the reference program's by a relative error of at most 0.0116315.
Values are sent between devices in bfloat16 or wider.
A program may use at most 1 GiB of HBM per device.

```python
import jax
import jax.numpy as jnp
from jax import lax

NUM_STAGES = 2
DATA_DEVS = 4
NUM_MICRO = 4
BATCH_MB = 8
SEQ_LEN = 32
LAYERS = 1
DMODEL = 2048
FFN_DIM = 8192


def setup_inputs(seed: int = 0) -> dict:
    rng_key = jax.random.key(seed)
    sub_keys = jax.random.split(rng_key, 5)
    act_shape = (NUM_MICRO, DATA_DEVS * BATCH_MB, SEQ_LEN, DMODEL)
    up_shape = (NUM_STAGES, LAYERS, DMODEL, FFN_DIM)
    down_shape = (NUM_STAGES, LAYERS, FFN_DIM, DMODEL)
    x = jax.random.normal(sub_keys[0], act_shape, jnp.float32).astype(jnp.bfloat16)
    g = jax.random.normal(sub_keys[1], act_shape, jnp.float32).astype(jnp.bfloat16)
    w_gate = (jax.random.normal(sub_keys[2], up_shape, jnp.float32) * DMODEL ** -0.5).astype(jnp.bfloat16)
    w_in = (jax.random.normal(sub_keys[3], up_shape, jnp.float32) * DMODEL ** -0.5).astype(jnp.bfloat16)
    w_out = (jax.random.normal(sub_keys[4], down_shape, jnp.float32) * FFN_DIM ** -0.5).astype(jnp.bfloat16)
    return {'x': x, 'g': g, 'w_gate': w_gate, 'w_in': w_in, 'w_out': w_out}


def rms_f32(row_vals):
    return row_vals * lax.rsqrt(jnp.mean(row_vals * row_vals, axis=-1, keepdims=True) + 1e-6)


def layer_fwd(tokens, w_gate, w_in, w_out):
    normed = rms_f32(tokens.astype(jnp.float32)).astype(jnp.bfloat16)
    pre_gate = jnp.dot(normed, w_gate, preferred_element_type=jnp.float32)
    pre_in = jnp.dot(normed, w_in, preferred_element_type=jnp.float32)
    hidden = (pre_gate * jax.nn.sigmoid(pre_gate) * pre_in).astype(jnp.bfloat16)
    branch = jnp.dot(hidden, w_out, preferred_element_type=jnp.float32)
    return tokens + branch.astype(jnp.bfloat16)


def layer_bwd(tokens, d_next, w_gate, w_in, w_out):
    normed_f, rms_pull = jax.vjp(rms_f32, tokens.astype(jnp.float32))
    normed = normed_f.astype(jnp.bfloat16)
    pre_gate = jnp.dot(normed, w_gate, preferred_element_type=jnp.float32)
    pre_in = jnp.dot(normed, w_in, preferred_element_type=jnp.float32)
    sigma_gate = jax.nn.sigmoid(pre_gate)
    gate_act = pre_gate * sigma_gate
    hidden = (gate_act * pre_in).astype(jnp.bfloat16)
    d_wout = jnp.dot(hidden.T, d_next, preferred_element_type=jnp.float32)
    d_hidden = jnp.dot(d_next, w_out.T, preferred_element_type=jnp.float32)
    d_gate = (d_hidden * pre_in * sigma_gate * (1.0 + pre_gate * (1.0 - sigma_gate))).astype(jnp.bfloat16)
    d_up = (d_hidden * gate_act).astype(jnp.bfloat16)
    d_wgate = jnp.dot(normed.T, d_gate, preferred_element_type=jnp.float32)
    d_win = jnp.dot(normed.T, d_up, preferred_element_type=jnp.float32)
    d_normed = jnp.dot(d_gate, w_gate.T, preferred_element_type=jnp.float32) + jnp.dot(d_up, w_in.T, preferred_element_type=jnp.float32)
    d_resid = rms_pull(d_normed)[0]
    d_prev = (d_next.astype(jnp.float32) + d_resid).astype(jnp.bfloat16)
    return d_prev, d_wgate, d_win, d_wout


def reference(x, g, w_gate, w_in, w_out):
    n_blocks = NUM_STAGES * LAYERS
    gate_all = w_gate.reshape(n_blocks, DMODEL, FFN_DIM)
    in_all = w_in.reshape(n_blocks, DMODEL, FFN_DIM)
    out_all = w_out.reshape(n_blocks, FFN_DIM, DMODEL)

    def one_micro(grad_sums, micro_pair):
        x_micro = micro_pair[0]
        g_micro = micro_pair[1]

        def fwd_step(tokens, weights):
            return layer_fwd(tokens, weights[0], weights[1], weights[2]), tokens

        _, block_inputs = lax.scan(fwd_step, x_micro.reshape(-1, DMODEL), (gate_all, in_all, out_all))

        def bwd_step(d_next, block_items):
            d_prev, d_wgate, d_win, d_wout = layer_bwd(block_items[0], d_next, block_items[1], block_items[2], block_items[3])
            return d_prev, (d_wgate, d_win, d_wout)

        d_first, block_grads = lax.scan(bwd_step, g_micro.reshape(-1, DMODEL), (block_inputs, gate_all, in_all, out_all), reverse=True)
        new_sums = (grad_sums[0] + block_grads[0], grad_sums[1] + block_grads[1], grad_sums[2] + block_grads[2])
        return new_sums, d_first.reshape(x_micro.shape)

    zero_up = jnp.zeros((n_blocks, DMODEL, FFN_DIM), jnp.float32)
    zero_down = jnp.zeros((n_blocks, FFN_DIM, DMODEL), jnp.float32)
    grad_sums, d_x = lax.scan(one_micro, (zero_up, zero_up, zero_down), (x, g))
    return (d_x, grad_sums[0].reshape(w_gate.shape), grad_sums[1].reshape(w_in.shape), grad_sums[2].reshape(w_out.shape))
```

```python
import jax
import jax.numpy as jnp
from jax import lax
from jax.sharding import PartitionSpec as P

N_CHUNKS = 2


def rms_f32(row_vals):
    return row_vals * lax.rsqrt(jnp.mean(row_vals * row_vals, axis=-1, keepdims=True) + 1e-6)


def mm(lhs, rhs, lhs_dim, rhs_dim):
    return lax.dot_general(lhs, rhs, (((lhs_dim,), (rhs_dim,)), ((), ())), preferred_element_type=jnp.float32)


def normed_of(tokens):
    return rms_f32(tokens.astype(jnp.float32)).astype(jnp.bfloat16)


def block_grads(normed, d_out, w_gate, w_in, w_out):
    pre_gate = mm(normed, w_gate, 1, 0)
    pre_in = mm(normed, w_in, 1, 0)
    d_hidden = mm(d_out, w_out, 1, 1)
    sigma = jax.nn.sigmoid(pre_gate)
    gate_act = pre_gate * sigma
    hidden = (gate_act * pre_in).astype(jnp.bfloat16)
    d_gate = (d_hidden * pre_in * sigma * (1.0 + pre_gate * (1.0 - sigma))).astype(jnp.bfloat16)
    d_up = (d_hidden * gate_act).astype(jnp.bfloat16)
    d_normed = mm(d_gate, w_gate, 1, 1) + mm(d_up, w_in, 1, 1)
    return hidden, d_gate, d_up, d_normed


def through_norm(tokens, d_out, d_normed):
    _, rms_pull = jax.vjp(rms_f32, tokens.astype(jnp.float32))
    return (d_out.astype(jnp.float32) + rms_pull(d_normed)[0]).astype(jnp.bfloat16)


def solution(mesh):
    chips = mesh.shape['data']
    act_spec = P(None, 'data', None, None)
    weight_spec = P('stage', None, 'data', None)

    def per_device(x, g, w_gate, w_in, w_out):
        n_micro, batch_mb, seq_len, dmodel = x.shape
        ffn = w_gate.shape[3]
        cols = ffn // chips
        core = lax.axis_index('stage')
        half = batch_mb * seq_len // 2
        per_chunk = n_micro // N_CHUNKS

        def columns_of(shard):
            pieces = lax.all_to_all(shard.reshape(-1, chips, cols), 'data', 1, 0)
            return lax.all_gather(pieces.reshape(-1, cols), 'stage')

        gate_all = columns_of(w_gate[0, 0])
        in_all = columns_of(w_in[0, 0])
        out_all = lax.all_gather(w_out[0, 0], 'stage')

        def my_rows(arr):
            rows = arr.reshape(n_micro, 2, half, dmodel)
            rows = lax.dynamic_index_in_dim(rows, core, 1, keepdims=False)
            return rows.reshape(N_CHUNKS, per_chunk * half, dmodel)

        def everywhere(rows):
            return lax.all_gather(rows, 'data', axis=0, tiled=True)

        def summed(partial):
            return lax.psum_scatter(partial, 'data', scatter_dimension=0, tiled=True)

        x_rows, g_rows = my_rows(x), my_rows(g)
        dx_rows = []
        saved = [[], []]
        for c in range(N_CHUNKS):
            x_all = everywhere(x_rows[c])
            n0 = normed_of(x_all)
            pre_gate = mm(n0, gate_all[0], 1, 0)
            pre_in = mm(n0, in_all[0], 1, 0)
            hidden = (pre_gate * jax.nn.sigmoid(pre_gate) * pre_in).astype(jnp.bfloat16)
            branch = summed(mm(hidden, out_all[0], 1, 0))
            h_rows = x_rows[c] + branch.astype(jnp.bfloat16)
            n1 = normed_of(everywhere(h_rows))
            g_all = everywhere(g_rows[c])
            hidden1, d_gate1, d_up1, d_n1 = block_grads(n1, g_all, gate_all[1], in_all[1], out_all[1])
            e_rows = through_norm(h_rows, g_rows[c], summed(d_n1))
            e_all = everywhere(e_rows)
            hidden0, d_gate0, d_up0, d_n0 = block_grads(n0, e_all, gate_all[0], in_all[0], out_all[0])
            dx_rows.append(through_norm(x_rows[c], e_rows, summed(d_n0)))
            saved[0].append((n0, e_all, hidden0, d_gate0, d_up0))
            saved[1].append((n1, g_all, hidden1, d_gate1, d_up1))

        d_parts = [[], [], []]
        for block in range(2):
            normed, d_out, hidden, d_gate, d_up = [jnp.concatenate(parts) for parts in zip(*saved[block])]
            d_parts[0].append(mm(normed, d_gate, 0, 0))
            d_parts[1].append(mm(normed, d_up, 0, 0))
            d_parts[2].append(mm(hidden, d_out, 0, 0))
        d_gate_w, d_in_w, d_out_w = [lax.psum_scatter(jnp.stack(parts), 'stage', scatter_dimension=0) for parts in d_parts]

        def rows_of(full):
            pieces = lax.all_to_all(full.reshape(chips, -1, cols), 'data', 0, 0)
            return pieces.transpose(1, 0, 2).reshape(1, 1, -1, ffn)

        dx = lax.all_gather(jnp.stack(dx_rows).reshape(n_micro, half, dmodel), 'stage', axis=1, tiled=True)
        return dx.reshape(x.shape), rows_of(d_gate_w), rows_of(d_in_w), d_out_w[None, None]

    return jax.shard_map(per_device, mesh=mesh, in_specs=(act_spec, act_spec, weight_spec, weight_spec, weight_spec),
                         out_specs=(act_spec, weight_spec, weight_spec, weight_spec), check_vma=False)
```

```python
import jax
import jax.numpy as jnp
from jax import lax
from jax.experimental import pallas as pl
from jax.experimental.pallas import tpu as pltpu
from jax.sharding import PartitionSpec as P

MESH = pl.DeviceIdType.MESH
F32 = jnp.float32
BF16 = jnp.bfloat16
EPS = 1e-6

CHUNKS = 4
ROWS = 128
BLOCK_ROWS = 4 * ROWS
WIDTH = 2048
HALF = WIDTH // 2
QUARTER = WIDTH // 4
TILE = 256
TILES = WIDTH // TILE
CHAIN = 3 * CHUNKS
GRAD_TILES = 3 * TILES
SLOTS = 4
LO, HI = pl.ds(0, HALF), pl.ds(HALF, HALF)


def mm(lhs, rhs, rhs_dim):
    return lax.dot_general(lhs, rhs, (((1,), (rhs_dim,)), ((), ())), preferred_element_type=F32)


def start_all(copies):
    for copy in copies:
        copy.start()


def run_all(copies):
    start_all(copies)
    for copy in copies:
        copy.wait()


def step_kernel(x, g, wg_in, wi_in, wo_in,
                dx, dwg, dwi, dwo, act, wg, wi, wo, part, ra1, rb1, ra2, rb2, lhs, rhs,
                wbuf, ab, tb, dab, dbb, pst, keep, snd, ld, r2, own, new, outs,
                ag_send, ag_recv, rs_send, rs_recv, w_send, w_recv, f_send, f_recv, d_send, d_recv,
                op_send, op_recv, dx_send, dx_recv, gr_send, gr_recv, p_sem, l_sem, t_sem):
    chip = lax.axis_index('data')
    core = lax.axis_index('stage')
    cx, cy = chip % 2, chip // 2
    near = (cy * 2 + (1 - cx), (1 - cy) * 2 + cx, (1 - cy) * 2 + (1 - cx))
    other = 1 - core
    x_dev, y_dev, twin = (near[0], core), (near[1], core), (chip, other)
    w_ins, w_alls = (wg_in, wi_in), (wg, wi)

    def local(src, dst, sem):
        return pltpu.make_async_copy(src, dst, sem)

    def remote(src, dst, send, recv, dev):
        return pltpu.make_async_remote_copy(src_ref=src, dst_ref=dst, send_sem=send, recv_sem=recv, device_id=dev, device_id_type=MESH)

    def shard(kind, i, n, cols=slice(None)):
        return act.at[kind, i, pl.ds(n * ROWS, ROWS), cols]

    def ag_first(kind, i, src):
        return (remote(src, shard(kind, i, 2), ag_send.at[kind, i, 0], ag_recv.at[kind, i, 0], x_dev),
                remote(src, shard(kind, i, 1), ag_send.at[kind, i, 1], ag_recv.at[kind, i, 1], y_dev))

    def ag_second(kind, i):
        return (remote(shard(kind, i, 1, LO), shard(kind, i, 3, LO), ag_send.at[kind, i, 2], ag_recv.at[kind, i, 2], x_dev),
                remote(shard(kind, i, 2, HI), shard(kind, i, 3, HI), ag_send.at[kind, i, 3], ag_recv.at[kind, i, 3], y_dev))

    def ag_forward(kind, i):
        for copy in ag_first(kind, i, shard(kind, i, 0)):
            copy.wait_recv()
        start_all(ag_second(kind, i))

    def ag_arrived(kind, i):
        for copy in ag_second(kind, i):
            copy.wait_recv()

    def rs_first(task):
        return (remote(part.at[task, 1, :, :, LO], ra1.at[task], rs_send.at[task, 0], rs_recv.at[task, 0], x_dev),
                remote(part.at[task, :, 1, :, HI], rb1.at[task], rs_send.at[task, 1], rs_recv.at[task, 1], y_dev))

    def rs_second(task):
        slot = task % 2
        return (remote(snd.at[slot, 0], ra2.at[task], rs_send.at[task, 2], rs_recv.at[task, 2], y_dev),
                remote(snd.at[slot, 1], rb2.at[task], rs_send.at[task, 3], rs_recv.at[task, 3], x_dev))

    def rs_middle(task):
        slot = task % 2

        @pl.when(task >= 2)
        def _():
            for copy in rs_second(task - 2):
                copy.wait_send()

        mine = (part.at[task, 0, :, :, LO], part.at[task, :, 0, :, HI])
        for side, (came, received) in enumerate(zip((ra1, rb1), rs_first(task))):
            received.wait_recv()
            run_all((local(mine[side], ld.at[0], l_sem.at[0]), local(came.at[task], ld.at[1], l_sem.at[1])))
            snd[slot, side] = ld[0, 1] + ld[1, 1]
            keep[slot, :, pl.ds(side * HALF, HALF)] = ld[0, 0] + ld[1, 0]
            rs_second(task)[side].start()

    def dx_copies(i, slot):
        dst = dx.at[i, pl.ds(core * ROWS, ROWS)]
        return (local(new.at[slot], dst, dx_send.at[i, 0]), remote(new.at[slot], dst, dx_send.at[i, 1], dx_recv.at[i], twin))

    def dx_sent(i):
        stored, sent = dx_copies(i, i % 2)
        stored.wait()
        sent.wait_send()

    def rs_last(task):
        slot, kind, i = task % 2, task // CHUNKS, task % CHUNKS
        for copy in rs_second(task):
            copy.wait_recv()
        run_all((local(ra2.at[task], r2.at[:, LO], l_sem.at[0]), local(rb2.at[task], r2.at[:, HI], l_sem.at[1]),
                 local(shard((3 * kind + 1) // 2, i, 0), own.at[0], l_sem.at[2]), local(shard(kind % 2, i, 0), own.at[1], l_sem.at[3])))

        @pl.when(task >= 2 * CHUNKS + 2)
        def _():
            dx_sent(i - 2)

        def rows_step(r, _):
            rows = pl.ds(r * 32, 32)
            total = keep[slot, rows, :] + r2[rows, :]

            @pl.when(kind == 0)
            def _():
                new[slot, rows, :] = own[0, rows, :] + total.astype(BF16)

            @pl.when(kind > 0)
            def _():
                tok = own[1, rows, :].astype(F32)
                inv = lax.rsqrt(jnp.mean(tok * tok, axis=-1, keepdims=True) + EPS)
                dot = jnp.mean(tok * total, axis=-1, keepdims=True)
                resid = total * inv - tok * (inv * inv * inv * dot)
                new[slot, rows, :] = (own[0, rows, :].astype(F32) + resid).astype(BF16)
            return 0

        lax.fori_loop(0, ROWS // 32, rows_step, 0)

        @pl.when(kind < 2)
        def _():
            mine = shard(2 * kind + 1, i, 0)
            run_all((local(new.at[slot], mine, l_sem.at[0]),))
            start_all(ag_first(2 * kind + 1, i, mine))

        @pl.when(kind == 2)
        def _():
            start_all(dx_copies(i, slot))

    def w_copies(mtx, n):
        rows = pl.ds(chip * QUARTER + n * TILE, TILE)
        return [remote(w_ins[mtx].at[pl.ds(n * TILE, TILE), pl.ds(to * WIDTH, WIDTH)], w_alls[mtx].at[core, rows],
                       w_send.at[mtx, n, k], w_recv.at[mtx, n, k], (to, core)) for k, to in enumerate(near)]

    def w_forwards(mtx, n, block):
        pieces = [w_alls[mtx].at[block, pl.ds(came * QUARTER + n * TILE, TILE)] for came in near]
        return [remote(piece, piece, f_send.at[mtx, n, k], f_recv.at[mtx, n, k], twin) for k, piece in enumerate(pieces)]

    def w_pass_on(mtx, n):
        for came, onward in zip(w_copies(mtx, n), w_forwards(mtx, n, core)):
            came.wait_recv()
            onward.start()

    def w_twin(block):
        rows, cols = pl.ds(chip * QUARTER, QUARTER), pl.ds(chip * WIDTH, WIDTH)
        return (remote(wg_in.at[:, cols], wg.at[block, rows], d_send.at[0], d_recv.at[0], twin),
                remote(wi_in.at[:, cols], wi.at[block, rows], d_send.at[1], d_recv.at[1], twin),
                remote(wo_in, wo.at[block], d_send.at[2], d_recv.at[2], twin))

    def w_from_twin(block):
        for mtx in range(2):
            for n in range(2):
                for copy in w_forwards(mtx, n, block):
                    copy.wait_recv()
        for copy in w_twin(block):
            copy.wait_recv()

    def op_pairs(i, src):
        rows = pl.ds(i * BLOCK_ROWS, BLOCK_ROWS)
        return ((tb.at[0], lhs.at[0, src, :, rows]), (tb.at[1], lhs.at[1, src, :, rows]), (dab, rhs.at[0, src, rows]),
                (dbb, rhs.at[1, src, rows]), (ab.at[1], rhs.at[2, src, rows]))

    def op_start(n, i, block):
        src, dst = op_pairs(i, core)[n]

        @pl.when(block == core)
        def _():
            local(src, dst, op_send.at[n]).start()

        @pl.when(block != core)
        def _():
            remote(src, dst, op_send.at[n], op_recv.at[i, n], twin).start()

    def op_sent(i):
        for n, (src, dst) in enumerate(op_pairs(i, core)):
            local(src, dst, op_send.at[n]).wait()

    def op_arrived(i):
        for n, (src, dst) in enumerate(op_pairs(i, other)):
            remote(src, dst, op_send.at[n], op_recv.at[i, n], twin).wait_recv()

    def normalize():
        def rows_step(r, _):
            rows = pl.ds(r * 64, 64)
            tok = ab[0, rows, :].astype(F32)
            inv = lax.rsqrt(jnp.mean(tok * tok, axis=-1, keepdims=True) + EPS)
            ab[0, rows, :] = (tok * inv).astype(BF16)
            return 0

        lax.fori_loop(0, BLOCK_ROWS // 64, rows_step, 0)

    def write_partials(task, product):
        def tile_copy(n, slot):
            return local(pst.at[slot], part.at[task, :, :, :, pl.ds(n * TILE, TILE)], p_sem.at[slot])

        def half_step(side, _):
            def tile_step(t, _):
                n, slot = side * (TILES // 2) + t, t % 2

                @pl.when(t >= 2)
                def _():
                    tile_copy(n - 2, slot).wait()

                pst[slot] = product(pl.ds(n * TILE, TILE)).reshape(2, 2, ROWS, TILE)
                tile_copy(n, slot).start()
                return 0

            lax.fori_loop(0, TILES // 2, tile_step, 0)
            last = (side + 1) * (TILES // 2)
            tile_copy(last - 2, 0).wait()
            tile_copy(last - 1, 1).wait()
            for n in range(2):
                @pl.when(side == n)
                def _(n=n):
                    rs_first(task)[n].start()
            return 0

        lax.fori_loop(0, 2, half_step, 0)

    def forward(task):
        ag_arrived(0, task)
        run_all((local(act.at[0, task], ab.at[0], l_sem.at[0]),))
        normalize()

        def tile_step(t, _):
            cols = pl.ds(t * TILE, TILE)
            pre_gate = mm(ab[0], wbuf[0, :, cols], 0)
            pre_in = mm(ab[0], wbuf[1, :, cols], 0)
            dab[:, cols] = (pre_gate * jax.nn.sigmoid(pre_gate) * pre_in).astype(BF16)
            return 0

        lax.fori_loop(0, TILES, tile_step, 0)
        write_partials(task, lambda cols: mm(dab[...], wbuf[2, :, cols], 0))

    def backward(task):
        kind, i = task // CHUNKS, task % CHUNKS
        block = 2 - kind

        @pl.when(task > CHUNKS)
        def _():
            op_sent(i)

        @pl.when(kind == 1)
        def _():
            ag_arrived(1, i)
            ag_arrived(2, i)

        @pl.when(kind == 2)
        def _():
            ag_arrived(3, i)

        run_all((local(act.at[2 - kind, i], ab.at[0], l_sem.at[0]), local(act.at[kind + 1, i], ab.at[1], l_sem.at[1])))
        op_start(4, i, block)
        normalize()

        def turn_step(t, _):
            cols = pl.ds(t * TILE, TILE)
            tb[0, cols, :] = ab[0, :, cols].T
            return 0

        lax.fori_loop(0, TILES, turn_step, 0)
        op_start(0, i, block)

        def tile_step(t, _):
            cols = pl.ds(t * TILE, TILE)
            pre_gate = mm(ab[0], wbuf[0, :, cols], 0)
            pre_in = mm(ab[0], wbuf[1, :, cols], 0)
            d_hidden = mm(ab[1], wbuf[2, cols, :], 1)
            sigma = jax.nn.sigmoid(pre_gate)
            gate_act = pre_gate * sigma
            tb[1, cols, :] = (gate_act * pre_in).astype(BF16).T
            dab[:, cols] = (d_hidden * pre_in * sigma * (1.0 + pre_gate * (1.0 - sigma))).astype(BF16)
            dbb[:, cols] = (d_hidden * gate_act).astype(BF16)
            return 0

        lax.fori_loop(0, TILES, tile_step, 0)
        for n in (1, 2, 3):
            op_start(n, i, block)
        write_partials(task, lambda rows: mm(dab[...], wbuf[0, rows, :], 1) + mm(dbb[...], wbuf[1, rows, :], 1))

    def rhs_copies(t):
        slot = t % 2
        cols = pl.ds((t % TILES) * TILE, TILE)
        return [local(rhs.at[t // TILES, q, :, cols], tb.at[slot, :, pl.ds(q * TILE, TILE)], t_sem.at[slot, q]) for q in range(2)]

    def grad_sent(slot):
        for k in range(4):
            local(outs.at[slot, pl.ds(0, QUARTER)], dwo.at[pl.ds(0, QUARTER), pl.ds(0, TILE)], gr_send.at[slot, k]).wait()

    def grad_tile(t):
        mtx, slot = t // TILES, t % SLOTS
        col = (t % TILES) * TILE

        @pl.when(t == 0)
        def _():
            op_sent(0)
            for i in range(CHUNKS):
                op_arrived(i)
            start_all(rhs_copies(0))

        @pl.when(t % (2 * TILES) == 0)
        def _():
            run_all([local(lhs.at[t // (2 * TILES), q], wbuf.at[q], l_sem.at[q]) for q in range(2)])

        @pl.when(t + 1 < GRAD_TILES)
        def _():
            start_all(rhs_copies(t + 1))

        for copy in rhs_copies(t):
            copy.wait()

        @pl.when(t >= SLOTS)
        def _():
            grad_sent(slot)

        def quarter_step(k, _):
            ax, ay = 1 - k % 2, ((k + 1) // 2) % 2
            to = (cy + ay - 2 * cy * ay) * 2 + (cx + ax - 2 * cx * ax)
            rows = pl.ds(to * QUARTER, QUARTER)
            outs[slot, rows, :] = mm(wbuf[0, rows, :], tb[t % 2, :, 0:TILE], 0) + mm(wbuf[1, rows, :], tb[t % 2, :, TILE:2 * TILE], 0)
            for n, dst in enumerate((dwg, dwi)):
                cols = pl.ds(chip * WIDTH + col, TILE)

                @pl.when((mtx == n) & (k < 3))
                def _():
                    remote(outs.at[slot, rows], dst.at[:, cols], gr_send.at[slot, k], gr_recv.at[n, k], (to, core)).start()

                @pl.when((mtx == n) & (k == 3))
                def _():
                    local(outs.at[slot, rows], dst.at[:, cols], gr_send.at[slot, k]).start()

            @pl.when(mtx == 2)
            def _():
                local(outs.at[slot, rows], dwo.at[rows, pl.ds(col, TILE)], gr_send.at[slot, k]).start()
            return 0

        lax.fori_loop(0, 4, quarter_step, 0)

    barrier = pltpu.get_barrier_semaphore()
    for dev in [(to, core) for to in near] + [twin]:
        pl.semaphore_signal(barrier, inc=1, device_id=dev, device_id_type=MESH)
    pl.semaphore_wait(barrier, 4)

    def my_rows(arr, i):
        return arr.at[i, pl.ds(core * ROWS, ROWS)]

    for i in range(2):
        start_all(ag_first(0, i, my_rows(x, i)))

    @pl.when(core == 0)
    def _():
        for mtx in range(2):
            for n in range(2):
                start_all(w_copies(mtx, n))

    start_all(w_twin(core))
    rows, cols = pl.ds(chip * QUARTER, QUARTER), pl.ds(chip * WIDTH, WIDTH)
    top = pl.ds(0, QUARTER)
    loads = [local(wg_in.at[:, cols], wbuf.at[0, top], l_sem.at[0]), local(wi_in.at[:, cols], wbuf.at[1, top], l_sem.at[1]),
             local(wo_in, wbuf.at[2], l_sem.at[2])]
    stores = [local(wbuf.at[0, top], wg.at[core, rows], l_sem.at[0]), local(wbuf.at[1, top], wi.at[core, rows], l_sem.at[1]),
              local(wbuf.at[2], wo.at[core], l_sem.at[2])]
    for n, (arr, kind) in enumerate(((x, 0), (g, 2))):
        for i in range(CHUNKS):
            spot = ab.at[n, pl.ds(i * ROWS, ROWS)]
            loads.append(local(my_rows(arr, i), spot, t_sem.at[n, i]))
            stores.append(local(spot, shard(kind, i, 0), t_sem.at[n, i]))
    run_all(loads)
    run_all(stores)
    for i in range(2):
        ag_forward(0, i)

    @pl.when(core == 0)
    def _():
        for mtx in range(2):
            for n in range(2):
                w_pass_on(mtx, n)

    @pl.when(core == 1)
    def _():
        w_from_twin(0)

    def tick_step(tick, _):
        @pl.when(tick < 2)
        def _():
            start_all(ag_first(0, tick + 2, my_rows(x, tick + 2)))

        @pl.when(tick < CHUNKS)
        def _():
            start_all(ag_first(2, tick, my_rows(g, tick)))

        for mtx in range(2):
            for n in range(2):
                @pl.when((tick == 2 * mtx + n) & (core == 1))
                def _(mtx=mtx, n=n):
                    start_all(w_copies(mtx, n))

        @pl.when((tick == CHUNKS) & (core == 0))
        def _():
            w_from_twin(1)

        @pl.when((tick < CHAIN) & (tick % CHUNKS == 0))
        def _():
            block = (tick // CHUNKS) % 2
            run_all([local(src.at[block], wbuf.at[n], l_sem.at[n]) for n, src in enumerate((wg, wi, wo))])

        @pl.when(tick < CHUNKS)
        def _():
            forward(tick)

        @pl.when((tick >= CHUNKS) & (tick < CHAIN))
        def _():
            backward(tick)

        @pl.when(tick >= CHAIN)
        def _():
            grad_tile(tick - CHAIN)

        @pl.when(tick < 2)
        def _():
            ag_forward(0, tick + 2)

        @pl.when(tick < CHUNKS)
        def _():
            ag_forward(2, tick)

        @pl.when((tick >= 3) & (tick < 3 + 2 * CHUNKS))
        def _():
            ag_forward(2 * ((tick - 3) // CHUNKS) + 1, (tick - 3) % CHUNKS)

        @pl.when((tick >= 2) & (tick < 2 + CHAIN))
        def _():
            rs_last(tick - 2)

        @pl.when((tick >= 1) & (tick < 1 + CHAIN))
        def _():
            rs_middle(tick - 1)

        for mtx in range(2):
            for n in range(2):
                @pl.when((tick == 2 * mtx + n) & (core == 1))
                def _(mtx=mtx, n=n):
                    w_pass_on(mtx, n)
        return 0

    lax.fori_loop(0, CHAIN + GRAD_TILES, tick_step, 0)

    for n, dst in enumerate((dwg, dwi)):
        for k, came in enumerate(near):
            block = dst.at[:, pl.ds(came * WIDTH, WIDTH)]
            local(block, block, gr_recv.at[n, k]).wait()
    for slot in range(SLOTS):
        grad_sent(slot)
    for i in range(CHUNKS):
        dx_copies(i, 0)[1].wait_recv()
    dx_sent(2)
    dx_sent(3)

    def drain_gathers(n, _):
        kind, i = n // CHUNKS, n % CHUNKS
        for copy in ag_first(kind, i, shard(kind, i, 0)) + ag_second(kind, i):
            copy.wait_send()
        return 0

    def drain_sums(task, _):
        for copy in rs_first(task):
            copy.wait_send()
        return 0

    lax.fori_loop(0, 4 * CHUNKS, drain_gathers, 0)
    lax.fori_loop(0, CHAIN, drain_sums, 0)
    for task in (CHAIN - 2, CHAIN - 1):
        for copy in rs_second(task):
            copy.wait_send()
    for mtx in range(2):
        for n in range(2):
            for copy in w_copies(mtx, n) + w_forwards(mtx, n, core):
                copy.wait_send()
    for copy in w_twin(core):
        copy.wait_send()


def solution(mesh):
    act_spec = P(None, 'data', None, None)
    weight_spec = P('stage', None, 'data', None)

    def per_device(x, g, w_gate, w_in, w_out):
        flat = (CHUNKS, 2 * ROWS, WIDTH)
        dma = pltpu.SemaphoreType.DMA
        any_space = pl.BlockSpec(memory_space=pl.ANY)

        def arr(*shape, dtype=BF16):
            return jax.ShapeDtypeStruct(shape, dtype)

        out_shapes = [
            arr(*flat), arr(QUARTER, 4 * WIDTH, dtype=F32), arr(QUARTER, 4 * WIDTH, dtype=F32), arr(WIDTH, WIDTH, dtype=F32),
            arr(4, CHUNKS, BLOCK_ROWS, WIDTH), arr(2, WIDTH, WIDTH), arr(2, WIDTH, WIDTH), arr(2, WIDTH, WIDTH),
            arr(CHAIN, 2, 2, ROWS, WIDTH, dtype=F32),
            arr(CHAIN, 2, ROWS, HALF, dtype=F32), arr(CHAIN, 2, ROWS, HALF, dtype=F32),
            arr(CHAIN, ROWS, HALF, dtype=F32), arr(CHAIN, ROWS, HALF, dtype=F32),
            arr(2, 2, WIDTH, WIDTH), arr(3, 2, WIDTH, WIDTH),
        ]
        scratch = [
            pltpu.VMEM((3, WIDTH, WIDTH), BF16), pltpu.VMEM((2, BLOCK_ROWS, WIDTH), BF16), pltpu.VMEM((2, WIDTH, BLOCK_ROWS), BF16),
            pltpu.VMEM((BLOCK_ROWS, WIDTH), BF16), pltpu.VMEM((BLOCK_ROWS, WIDTH), BF16),
            pltpu.VMEM((2, 2, 2, ROWS, TILE), F32), pltpu.VMEM((2, ROWS, WIDTH), F32), pltpu.VMEM((2, 2, ROWS, HALF), F32),
            pltpu.VMEM((2, 2, ROWS, HALF), F32), pltpu.VMEM((ROWS, WIDTH), F32), pltpu.VMEM((2, ROWS, WIDTH), BF16),
            pltpu.VMEM((2, ROWS, WIDTH), BF16), pltpu.VMEM((SLOTS, WIDTH, TILE), F32),
            dma((4, CHUNKS, 4)), dma((4, CHUNKS, 4)), dma((CHAIN, 4)), dma((CHAIN, 4)),
            dma((2, 2, 3)), dma((2, 2, 3)), dma((2, 2, 3)), dma((2, 2, 3)), dma((3,)), dma((3,)),
            dma((5,)), dma((CHUNKS, 5)), dma((CHUNKS, 2)), dma((CHUNKS,)), dma((SLOTS, 4)), dma((2, 3)),
            dma((2,)), dma((4,)), dma((2, 4)),
        ]
        results = pl.pallas_call(
            step_kernel, out_shape=out_shapes, in_specs=[any_space] * 5, out_specs=[any_space] * len(out_shapes),
            scratch_shapes=scratch, name='mlp_step',
            compiler_params=pltpu.CompilerParams(collective_id=0, has_side_effects=True, vmem_limit_bytes=67_043_328),
        )(x.reshape(flat), g.reshape(flat), w_gate[0, 0], w_in[0, 0], w_out[0, 0])
        dx, d_gate, d_in, d_out = results[:4]
        return dx.reshape(x.shape), d_gate[None, None], d_in[None, None], d_out[None, None]

    return jax.shard_map(per_device, mesh=mesh, in_specs=(act_spec, act_spec, weight_spec, weight_spec, weight_spec),
                         out_specs=(act_spec, weight_spec, weight_spec, weight_spec), check_vma=False)
```

```python
import jax
import jax.numpy as jnp
from jax import lax
from jax.experimental import pallas as pl
from jax.experimental.pallas import tpu as pltpu
from jax.sharding import PartitionSpec as P

MESH = pl.DeviceIdType.MESH
F32 = jnp.float32
BF16 = jnp.bfloat16
EPS = 1e-6

CHUNKS = 4
ROWS = 128
BLOCK_ROWS = 4 * ROWS
WIDTH = 2048
HALF = WIDTH // 2
QUARTER = WIDTH // 4
TILE = 256
TILES = WIDTH // TILE
CHAIN = 3 * CHUNKS
TURN = CHUNKS
SENT_TILES = 2 * TILES
SLOTS = 4
LO, HI = pl.ds(0, HALF), pl.ds(HALF, HALF)


def mm(lhs, rhs, rhs_dim):
    return lax.dot_general(lhs, rhs, (((1,), (rhs_dim,)), ((), ())), preferred_element_type=F32)


def start_all(copies):
    for copy in copies:
        copy.start()


def run_all(copies):
    start_all(copies)
    for copy in copies:
        copy.wait()


def step_kernel(x, g, wg_in, wi_in, wo_in,
                dx, dwg, dwi, dwo, act, wg, wi, wo, part, ra1, rb1, ra2, rb2, lhs, rhs,
                wbuf, ab, tb, dab, dbb, pst, keep, snd, ld, r2, own, new, outs, wo_out,
                ag_send, ag_recv, rs_send, rs_recv, w_send, w_recv, f_send, f_recv, d_send, d_recv,
                op_send, op_recv, dx_send, dx_recv, gr_send, gr_recv, p_sem, l_sem, t_sem, o_sem):
    chip = lax.axis_index('data')
    core = lax.axis_index('stage')
    cx, cy = chip % 2, chip // 2
    near = (cy * 2 + (1 - cx), (1 - cy) * 2 + cx, (1 - cy) * 2 + (1 - cx))
    other = 1 - core
    x_dev, y_dev, twin = (near[0], core), (near[1], core), (chip, other)
    w_ins, w_alls = (wg_in, wi_in), (wg, wi)

    def local(src, dst, sem):
        return pltpu.make_async_copy(src, dst, sem)

    def remote(src, dst, send, recv, dev):
        return pltpu.make_async_remote_copy(src_ref=src, dst_ref=dst, send_sem=send, recv_sem=recv, device_id=dev, device_id_type=MESH)

    def shard(kind, i, n, cols=slice(None)):
        return act.at[kind, i, pl.ds(n * ROWS, ROWS), cols]

    def ag_first(kind, i, src):
        return (remote(src, shard(kind, i, 2), ag_send.at[kind, i, 0], ag_recv.at[kind, i, 0], x_dev),
                remote(src, shard(kind, i, 1), ag_send.at[kind, i, 1], ag_recv.at[kind, i, 1], y_dev))

    def ag_second(kind, i):
        return (remote(shard(kind, i, 1, LO), shard(kind, i, 3, LO), ag_send.at[kind, i, 2], ag_recv.at[kind, i, 2], x_dev),
                remote(shard(kind, i, 2, HI), shard(kind, i, 3, HI), ag_send.at[kind, i, 3], ag_recv.at[kind, i, 3], y_dev))

    def ag_forward(kind, i):
        for copy in ag_first(kind, i, shard(kind, i, 0)):
            copy.wait_recv()
        start_all(ag_second(kind, i))

    def ag_arrived(kind, i):
        for copy in ag_second(kind, i):
            copy.wait_recv()

    def rs_first(task):
        return (remote(part.at[task, 1, :, :, LO], ra1.at[task], rs_send.at[task, 0], rs_recv.at[task, 0], x_dev),
                remote(part.at[task, :, 1, :, HI], rb1.at[task], rs_send.at[task, 1], rs_recv.at[task, 1], y_dev))

    def rs_second(task):
        slot = task % 2
        return (remote(snd.at[slot, 0], ra2.at[task], rs_send.at[task, 2], rs_recv.at[task, 2], y_dev),
                remote(snd.at[slot, 1], rb2.at[task], rs_send.at[task, 3], rs_recv.at[task, 3], x_dev))

    def rs_middle(task):
        slot = task % 2

        @pl.when(task >= 2)
        def _():
            for copy in rs_second(task - 2):
                copy.wait_send()

        mine = (part.at[task, 0, :, :, LO], part.at[task, :, 0, :, HI])
        for side, (came, received) in enumerate(zip((ra1, rb1), rs_first(task))):
            received.wait_recv()
            run_all((local(mine[side], ld.at[0], l_sem.at[0]), local(came.at[task], ld.at[1], l_sem.at[1])))
            snd[slot, side] = ld[0, 1] + ld[1, 1]
            keep[slot, :, pl.ds(side * HALF, HALF)] = ld[0, 0] + ld[1, 0]
            rs_second(task)[side].start()

    def dx_copies(i, slot):
        dst = dx.at[i, pl.ds(core * ROWS, ROWS)]
        return (local(new.at[slot], dst, dx_send.at[i, 0]), remote(new.at[slot], dst, dx_send.at[i, 1], dx_recv.at[i], twin))

    def dx_sent(i):
        stored, sent = dx_copies(i, i % 2)
        stored.wait()
        sent.wait_send()

    def rs_last(task):
        slot, kind, i = task % 2, task // CHUNKS, task % CHUNKS
        for copy in rs_second(task):
            copy.wait_recv()
        run_all((local(ra2.at[task], r2.at[:, LO], l_sem.at[0]), local(rb2.at[task], r2.at[:, HI], l_sem.at[1]),
                 local(shard((3 * kind + 1) // 2, i, 0), own.at[0], l_sem.at[2]), local(shard(kind % 2, i, 0), own.at[1], l_sem.at[3])))

        @pl.when(task >= 2 * CHUNKS + 2)
        def _():
            dx_sent(i - 2)

        def rows_step(r, _):
            rows = pl.ds(r * 32, 32)
            total = keep[slot, rows, :] + r2[rows, :]

            @pl.when(kind == 0)
            def _():
                new[slot, rows, :] = own[0, rows, :] + total.astype(BF16)

            @pl.when(kind > 0)
            def _():
                tok = own[1, rows, :].astype(F32)
                inv = lax.rsqrt(jnp.mean(tok * tok, axis=-1, keepdims=True) + EPS)
                dot = jnp.mean(tok * total, axis=-1, keepdims=True)
                resid = total * inv - tok * (inv * inv * inv * dot)
                new[slot, rows, :] = (own[0, rows, :].astype(F32) + resid).astype(BF16)
            return 0

        lax.fori_loop(0, ROWS // 32, rows_step, 0)

        @pl.when(kind < 2)
        def _():
            mine = shard(2 * kind + 1, i, 0)
            run_all((local(new.at[slot], mine, l_sem.at[0]),))
            start_all(ag_first(2 * kind + 1, i, mine))

        @pl.when(kind == 2)
        def _():
            start_all(dx_copies(i, slot))

    def w_copies(mtx, n):
        rows = pl.ds(chip * QUARTER + n * TILE, TILE)
        return [remote(w_ins[mtx].at[pl.ds(n * TILE, TILE), pl.ds(to * WIDTH, WIDTH)], w_alls[mtx].at[core, rows],
                       w_send.at[mtx, n, k], w_recv.at[mtx, n, k], (to, core)) for k, to in enumerate(near)]

    def w_forwards(mtx, n, block):
        pieces = [w_alls[mtx].at[block, pl.ds(came * QUARTER + n * TILE, TILE)] for came in near]
        return [remote(piece, piece, f_send.at[mtx, n, k], f_recv.at[mtx, n, k], twin) for k, piece in enumerate(pieces)]

    def w_pass_on(mtx, n):
        for came, onward in zip(w_copies(mtx, n), w_forwards(mtx, n, core)):
            came.wait_recv()
            onward.start()

    def w_twin(block):
        rows, cols = pl.ds(chip * QUARTER, QUARTER), pl.ds(chip * WIDTH, WIDTH)
        return (remote(wg_in.at[:, cols], wg.at[block, rows], d_send.at[0], d_recv.at[0], twin),
                remote(wi_in.at[:, cols], wi.at[block, rows], d_send.at[1], d_recv.at[1], twin),
                remote(wo_in, wo.at[block], d_send.at[2], d_recv.at[2], twin))

    def w_from_twin(block):
        for mtx in range(2):
            for n in range(2):
                for copy in w_forwards(mtx, n, block):
                    copy.wait_recv()
        for copy in w_twin(block):
            copy.wait_recv()

    def op_pairs(i, src):
        rows = pl.ds(i * BLOCK_ROWS, BLOCK_ROWS)
        return ((tb.at[0], lhs.at[0, src, :, rows]), (tb.at[1], lhs.at[1, src, :, rows]), (dab, rhs.at[0, src, rows]),
                (dbb, rhs.at[1, src, rows]), (ab.at[1], rhs.at[2, src, rows]))

    def op_start(n, i, block):
        src, dst = op_pairs(i, core)[n]

        @pl.when(block == core)
        def _():
            local(src, dst, op_send.at[n]).start()

        @pl.when(block != core)
        def _():
            remote(src, dst, op_send.at[n], op_recv.at[i, n], twin).start()

    def op_sent(i):
        for n, (src, dst) in enumerate(op_pairs(i, core)):
            local(src, dst, op_send.at[n]).wait()

    def op_arrived(i):
        for n, (src, dst) in enumerate(op_pairs(i, other)):
            remote(src, dst, op_send.at[n], op_recv.at[i, n], twin).wait_recv()

    def normalize():
        def rows_step(r, _):
            rows = pl.ds(r * 64, 64)
            tok = ab[0, rows, :].astype(F32)
            inv = lax.rsqrt(jnp.mean(tok * tok, axis=-1, keepdims=True) + EPS)
            ab[0, rows, :] = (tok * inv).astype(BF16)
            return 0

        lax.fori_loop(0, BLOCK_ROWS // 64, rows_step, 0)

    def write_partials(task, product):
        def tile_copy(n, slot):
            return local(pst.at[slot], part.at[task, :, :, :, pl.ds(n * TILE, TILE)], p_sem.at[slot])

        def half_step(side, _):
            def tile_step(t, _):
                n, slot = side * (TILES // 2) + t, t % 2

                @pl.when(t >= 2)
                def _():
                    tile_copy(n - 2, slot).wait()

                pst[slot] = product(pl.ds(n * TILE, TILE)).reshape(2, 2, ROWS, TILE)
                tile_copy(n, slot).start()
                return 0

            lax.fori_loop(0, TILES // 2, tile_step, 0)
            last = (side + 1) * (TILES // 2)
            tile_copy(last - 2, 0).wait()
            tile_copy(last - 1, 1).wait()
            for n in range(2):
                @pl.when(side == n)
                def _(n=n):
                    rs_first(task)[n].start()
            return 0

        lax.fori_loop(0, 2, half_step, 0)

    def forward(task):
        ag_arrived(0, task)
        run_all((local(act.at[0, task], ab.at[0], l_sem.at[0]),))
        normalize()

        def tile_step(t, _):
            cols = pl.ds(t * TILE, TILE)
            pre_gate = mm(ab[0], wbuf[0, :, cols], 0)
            pre_in = mm(ab[0], wbuf[1, :, cols], 0)
            dab[:, cols] = (pre_gate * jax.nn.sigmoid(pre_gate) * pre_in).astype(BF16)
            return 0

        lax.fori_loop(0, TILES, tile_step, 0)
        write_partials(task, lambda cols: mm(dab[...], wbuf[2, :, cols], 0))

    def backward(task):
        kind, i = task // CHUNKS, task % CHUNKS
        block = 2 - kind

        @pl.when(task > CHUNKS)
        def _():
            op_sent(i)

        @pl.when(kind == 1)
        def _():
            ag_arrived(1, i)
            ag_arrived(2, i)

        @pl.when(kind == 2)
        def _():
            ag_arrived(3, i)

        run_all((local(act.at[2 - kind, i], ab.at[0], l_sem.at[0]), local(act.at[kind + 1, i], ab.at[1], l_sem.at[1])))
        op_start(4, i, block)
        normalize()

        def turn_step(t, _):
            cols = pl.ds(t * TILE, TILE)
            tb[0, cols, :] = ab[0, :, cols].T
            return 0

        lax.fori_loop(0, TILES, turn_step, 0)
        op_start(0, i, block)

        def tile_step(t, _):
            cols = pl.ds(t * TILE, TILE)
            pre_gate = mm(ab[0], wbuf[0, :, cols], 0)
            pre_in = mm(ab[0], wbuf[1, :, cols], 0)
            d_hidden = mm(ab[1], wbuf[2, cols, :], 1)
            sigma = jax.nn.sigmoid(pre_gate)
            gate_act = pre_gate * sigma
            tb[1, cols, :] = (gate_act * pre_in).astype(BF16).T
            dab[:, cols] = (d_hidden * pre_in * sigma * (1.0 + pre_gate * (1.0 - sigma))).astype(BF16)
            dbb[:, cols] = (d_hidden * gate_act).astype(BF16)
            return 0

        lax.fori_loop(0, TILES, tile_step, 0)
        for n in (1, 2, 3):
            op_start(n, i, block)
        write_partials(task, lambda rows: mm(dab[...], wbuf[0, rows, :], 1) + mm(dbb[...], wbuf[1, rows, :], 1))

    def rhs_copies(mtx, n, slot):
        return [local(rhs.at[mtx, q, :, pl.ds(n * TILE, TILE)], tb.at[slot, :, pl.ds(q * TILE, TILE)], t_sem.at[slot, q]) for q in range(2)]

    def grad_sent(slot):
        for k in range(4):
            local(outs.at[slot, pl.ds(0, QUARTER)], dwo.at[pl.ds(0, QUARTER), pl.ds(0, TILE)], gr_send.at[slot, k]).wait()

    def grad_tile(t):
        mtx, slot = t // TILES, t % SLOTS
        col = (t % TILES) * TILE

        @pl.when(t == 0)
        def _():
            op_sent(0)
            for i in range(CHUNKS):
                op_arrived(i)
            start_all(rhs_copies(0, 0, 0))
            run_all([local(lhs.at[0, q], wbuf.at[q], l_sem.at[q]) for q in range(2)])

        for copy in rhs_copies(mtx, t % TILES, 0):
            copy.wait()

        @pl.when(t >= SLOTS)
        def _():
            grad_sent(slot)

        def quarter_step(k, _):
            ax, ay = 1 - k % 2, ((k + 1) // 2) % 2
            to = (cy + ay - 2 * cy * ay) * 2 + (cx + ax - 2 * cx * ax)
            rows = pl.ds(to * QUARTER, QUARTER)
            outs[slot, rows, :] = mm(wbuf[0, rows, :], tb[0, :, 0:TILE], 0) + mm(wbuf[1, rows, :], tb[0, :, TILE:2 * TILE], 0)
            cols = pl.ds(chip * WIDTH + col, TILE)
            for n, dst in enumerate((dwg, dwi)):
                @pl.when((mtx == n) & (k < 3))
                def _(n=n, dst=dst):
                    remote(outs.at[slot, rows], dst.at[:, cols], gr_send.at[slot, k], gr_recv.at[n, k], (to, core)).start()

                @pl.when((mtx == n) & (k == 3))
                def _(dst=dst):
                    local(outs.at[slot, rows], dst.at[:, cols], gr_send.at[slot, k]).start()
            return 0

        lax.fori_loop(0, 4, quarter_step, 0)

        @pl.when(t + 1 < SENT_TILES)
        def _():
            start_all(rhs_copies((t + 1) // TILES, (t + 1) % TILES, 0))

    def out_loads(k, slot):
        return [local(lhs.at[1, q, pl.ds(k * QUARTER, QUARTER)], wbuf.at[2, pl.ds(slot * HALF + q * QUARTER, QUARTER)], o_sem.at[slot, q]) for q in range(2)]

    def out_store(n, k, slot):
        return local(wo_out.at[slot], dwo.at[pl.ds(k * QUARTER, QUARTER), pl.ds(n * TILE, TILE)], o_sem.at[slot, 2])

    def out_tile(n):
        start_all(rhs_copies(2, n, 1))
        start_all(out_loads(0, 0))
        for copy in rhs_copies(2, n, 1):
            copy.wait()

        def quarter_step(k, _):
            slot = k % 2

            @pl.when(k < 3)
            def _():
                start_all(out_loads(k + 1, 1 - slot))

            for copy in out_loads(k, slot):
                copy.wait()

            @pl.when(4 * n + k >= 2)
            def _():
                out_store(n, k, slot).wait()

            top, low = pl.ds(slot * HALF, QUARTER), pl.ds(slot * HALF + QUARTER, QUARTER)
            wo_out[slot] = mm(wbuf[2, top, :], tb[1, :, 0:TILE], 0) + mm(wbuf[2, low, :], tb[1, :, TILE:2 * TILE], 0)
            out_store(n, k, slot).start()
            return 0

        lax.fori_loop(0, 4, quarter_step, 0)

    barrier = pltpu.get_barrier_semaphore()
    for dev in [(to, core) for to in near] + [twin]:
        pl.semaphore_signal(barrier, inc=1, device_id=dev, device_id_type=MESH)
    pl.semaphore_wait(barrier, 4)

    def my_rows(arr, i):
        return arr.at[i, pl.ds(core * ROWS, ROWS)]

    for i in range(2):
        start_all(ag_first(0, i, my_rows(x, i)))

    @pl.when(core == 0)
    def _():
        for mtx in range(2):
            for n in range(2):
                start_all(w_copies(mtx, n))

    start_all(w_twin(core))
    rows, cols = pl.ds(chip * QUARTER, QUARTER), pl.ds(chip * WIDTH, WIDTH)
    top = pl.ds(0, QUARTER)
    loads = [local(wg_in.at[:, cols], wbuf.at[0, top], l_sem.at[0]), local(wi_in.at[:, cols], wbuf.at[1, top], l_sem.at[1]),
             local(wo_in, wbuf.at[2], l_sem.at[2])]
    stores = [local(wbuf.at[0, top], wg.at[core, rows], l_sem.at[0]), local(wbuf.at[1, top], wi.at[core, rows], l_sem.at[1]),
              local(wbuf.at[2], wo.at[core], l_sem.at[2])]
    for n, (arr, kind) in enumerate(((x, 0), (g, 2))):
        for i in range(CHUNKS):
            spot = ab.at[n, pl.ds(i * ROWS, ROWS)]
            loads.append(local(my_rows(arr, i), spot, t_sem.at[n, i]))
            stores.append(local(spot, shard(kind, i, 0), t_sem.at[n, i]))
    run_all(loads)
    run_all(stores)
    for i in range(2):
        ag_forward(0, i)

    @pl.when(core == 0)
    def _():
        for mtx in range(2):
            for n in range(2):
                w_pass_on(mtx, n)

    @pl.when(core == 1)
    def _():
        w_from_twin(0)

    def when_task(tick, first, last):
        def run(body):
            @pl.when((tick >= 0) & (tick != TURN) & (tick <= CHAIN))
            def _():
                task = tick - jnp.where(tick > TURN, 1, 0)

                @pl.when((task >= first) & (task < last))
                def _():
                    body(task)
        return run

    def tick_step(tick, _):
        @pl.when(tick < 2)
        def _():
            start_all(ag_first(0, tick + 2, my_rows(x, tick + 2)))

        @pl.when((tick >= 2) & (tick < 2 + CHUNKS))
        def _():
            start_all(ag_first(2, tick - 2, my_rows(g, tick - 2)))

        for mtx in range(2):
            for n in range(2):
                @pl.when((tick == 2 * mtx + n) & (core == 1))
                def _(mtx=mtx, n=n):
                    start_all(w_copies(mtx, n))

        @pl.when((tick == TURN + 1) & (core == 0))
        def _():
            w_from_twin(1)

        @when_task(tick, 0, CHAIN)
        def _(task):
            @pl.when(task % CHUNKS == 0)
            def _():
                block = (task // CHUNKS) % 2
                run_all([local(src.at[block], wbuf.at[n], l_sem.at[n]) for n, src in enumerate((wg, wi, wo))])

        when_task(tick, 0, CHUNKS)(forward)
        when_task(tick, CHUNKS, CHAIN)(backward)

        @pl.when(tick > CHAIN)
        def _():
            grad_tile(tick - CHAIN - 1)

        @pl.when((tick > CHAIN + SLOTS) & (tick <= CHAIN + SLOTS + TILES))
        def _():
            out_tile(tick - CHAIN - SLOTS - 1)

        @pl.when(tick < 2)
        def _():
            ag_forward(0, tick + 2)

        @when_task(tick - 3, 0, 2 * CHUNKS)
        def _(task):
            ag_forward(2 * (task // CHUNKS) + 1, task % CHUNKS)

        when_task(tick - 2, 0, CHAIN)(rs_last)
        when_task(tick - 1, 0, CHAIN)(rs_middle)

        @pl.when((tick >= 2) & (tick < 2 + CHUNKS))
        def _():
            ag_forward(2, tick - 2)

        for mtx in range(2):
            for n in range(2):
                @pl.when((tick == 2 * mtx + n) & (core == 1))
                def _(mtx=mtx, n=n):
                    w_pass_on(mtx, n)
        return 0

    lax.fori_loop(0, CHAIN + 1 + SENT_TILES, tick_step, 0)

    for n, dst in enumerate((dwg, dwi)):
        for k, came in enumerate(near):
            block = dst.at[:, pl.ds(came * WIDTH, WIDTH)]
            local(block, block, gr_recv.at[n, k]).wait()
    for slot in range(SLOTS):
        grad_sent(slot)
    for slot in range(2):
        out_store(0, 0, slot).wait()
    for i in range(CHUNKS):
        dx_copies(i, 0)[1].wait_recv()
    dx_sent(2)
    dx_sent(3)

    def drain_gathers(n, _):
        kind, i = n // CHUNKS, n % CHUNKS
        for copy in ag_first(kind, i, shard(kind, i, 0)) + ag_second(kind, i):
            copy.wait_send()
        return 0

    def drain_sums(task, _):
        for copy in rs_first(task):
            copy.wait_send()
        return 0

    lax.fori_loop(0, 4 * CHUNKS, drain_gathers, 0)
    lax.fori_loop(0, CHAIN, drain_sums, 0)
    for task in (CHAIN - 2, CHAIN - 1):
        for copy in rs_second(task):
            copy.wait_send()
    for mtx in range(2):
        for n in range(2):
            for copy in w_copies(mtx, n) + w_forwards(mtx, n, core):
                copy.wait_send()
    for copy in w_twin(core):
        copy.wait_send()


def solution(mesh):
    act_spec = P(None, 'data', None, None)
    weight_spec = P('stage', None, 'data', None)

    def per_device(x, g, w_gate, w_in, w_out):
        flat = (CHUNKS, 2 * ROWS, WIDTH)
        dma = pltpu.SemaphoreType.DMA
        any_space = pl.BlockSpec(memory_space=pl.ANY)

        def arr(*shape, dtype=BF16):
            return jax.ShapeDtypeStruct(shape, dtype)

        out_shapes = [
            arr(*flat), arr(QUARTER, 4 * WIDTH, dtype=F32), arr(QUARTER, 4 * WIDTH, dtype=F32), arr(WIDTH, WIDTH, dtype=F32),
            arr(4, CHUNKS, BLOCK_ROWS, WIDTH), arr(2, WIDTH, WIDTH), arr(2, WIDTH, WIDTH), arr(2, WIDTH, WIDTH),
            arr(CHAIN, 2, 2, ROWS, WIDTH, dtype=F32),
            arr(CHAIN, 2, ROWS, HALF, dtype=F32), arr(CHAIN, 2, ROWS, HALF, dtype=F32),
            arr(CHAIN, ROWS, HALF, dtype=F32), arr(CHAIN, ROWS, HALF, dtype=F32),
            arr(2, 2, WIDTH, WIDTH), arr(3, 2, WIDTH, WIDTH),
        ]
        scratch = [
            pltpu.VMEM((3, WIDTH, WIDTH), BF16), pltpu.VMEM((2, BLOCK_ROWS, WIDTH), BF16), pltpu.VMEM((2, WIDTH, BLOCK_ROWS), BF16),
            pltpu.VMEM((BLOCK_ROWS, WIDTH), BF16), pltpu.VMEM((BLOCK_ROWS, WIDTH), BF16),
            pltpu.VMEM((2, 2, 2, ROWS, TILE), F32), pltpu.VMEM((2, ROWS, WIDTH), F32), pltpu.VMEM((2, 2, ROWS, HALF), F32),
            pltpu.VMEM((2, 2, ROWS, HALF), F32), pltpu.VMEM((ROWS, WIDTH), F32), pltpu.VMEM((2, ROWS, WIDTH), BF16),
            pltpu.VMEM((2, ROWS, WIDTH), BF16), pltpu.VMEM((SLOTS, WIDTH, TILE), F32),
            pltpu.VMEM((2, QUARTER, TILE), F32),
            dma((4, CHUNKS, 4)), dma((4, CHUNKS, 4)), dma((CHAIN, 4)), dma((CHAIN, 4)),
            dma((2, 2, 3)), dma((2, 2, 3)), dma((2, 2, 3)), dma((2, 2, 3)), dma((3,)), dma((3,)),
            dma((5,)), dma((CHUNKS, 5)), dma((CHUNKS, 2)), dma((CHUNKS,)), dma((SLOTS, 4)), dma((2, 3)),
            dma((2,)), dma((4,)), dma((2, 4)), dma((2, 3)),
        ]
        results = pl.pallas_call(
            step_kernel, out_shape=out_shapes, in_specs=[any_space] * 5, out_specs=[any_space] * len(out_shapes),
            scratch_shapes=scratch, name='mlp_step',
            compiler_params=pltpu.CompilerParams(collective_id=0, has_side_effects=True, vmem_limit_bytes=67_043_328),
        )(x.reshape(flat), g.reshape(flat), w_gate[0, 0], w_in[0, 0], w_out[0, 0])
        dx, d_gate, d_in, d_out = results[:4]
        return dx.reshape(x.shape), d_gate[None, None], d_in[None, None], d_out[None, None]

    return jax.shard_map(per_device, mesh=mesh, in_specs=(act_spec, act_spec, weight_spec, weight_spec, weight_spec),
                         out_specs=(act_spec, weight_spec, weight_spec, weight_spec), check_vma=False)
```

```python
import jax
import jax.numpy as jnp
from jax import lax
from jax.experimental import pallas as pl
from jax.experimental.pallas import tpu as pltpu
from jax.sharding import PartitionSpec as P

MESH = pl.DeviceIdType.MESH
F32 = jnp.float32
BF16 = jnp.bfloat16
EPS = 1e-6

CHUNKS = 4
ROWS = 128
BLOCK_ROWS = 4 * ROWS
WIDTH = 2048
HALF = WIDTH // 2
QUARTER = WIDTH // 4
TILE = 256
TILES = WIDTH // TILE
CHAIN = 3 * CHUNKS
TURN = CHUNKS
SENT_TILES = 2 * TILES
LATE_TILES = 2
SETTLE_FLOPS = 2 ** 30
SLOTS = 4
LO, HI = pl.ds(0, HALF), pl.ds(HALF, HALF)


def mm(lhs, rhs, rhs_dim):
    return lax.dot_general(lhs, rhs, (((1,), (rhs_dim,)), ((), ())), preferred_element_type=F32)


def start_all(copies):
    for copy in copies:
        copy.start()


def run_all(copies):
    start_all(copies)
    for copy in copies:
        copy.wait()


def step_kernel(x, g, wg_in, wi_in, wo_in,
                dx, dwg, dwi, dwo, late, act, wg, wi, wo, wx, part, ra1, rb1, ra2, rb2, lhs, rhs,
                wbuf, ab, tb, dab, dbb, pst, keep, snd, ld, r2, own, new, outs, wo_out,
                ag_send, ag_recv, rs_send, rs_recv, w_send, w_recv, f_send, f_recv, d_send, d_recv,
                op_send, op_recv, dx_send, dx_recv, gr_send, gr_recv, p_sem, l_sem, t_sem, o_sem):
    chip = lax.axis_index('data')
    core = lax.axis_index('stage')
    cx, cy = chip % 2, chip // 2
    near = (cy * 2 + (1 - cx), (1 - cy) * 2 + cx, (1 - cy) * 2 + (1 - cx))
    other = 1 - core
    x_dev, y_dev, twin = (near[0], core), (near[1], core), (chip, other)

    def local(src, dst, sem):
        return pltpu.make_async_copy(src, dst, sem)

    def remote(src, dst, send, recv, dev):
        return pltpu.make_async_remote_copy(src_ref=src, dst_ref=dst, send_sem=send, recv_sem=recv, device_id=dev, device_id_type=MESH)

    def shard(kind, i, n, cols=slice(None)):
        return act.at[kind, i, pl.ds(n * ROWS, ROWS), cols]

    def ag_first(kind, i, src):
        return (remote(src, shard(kind, i, 2), ag_send.at[kind, i, 0], ag_recv.at[kind, i, 0], x_dev),
                remote(src, shard(kind, i, 1), ag_send.at[kind, i, 1], ag_recv.at[kind, i, 1], y_dev))

    def ag_second(kind, i):
        return (remote(shard(kind, i, 1, LO), shard(kind, i, 3, LO), ag_send.at[kind, i, 2], ag_recv.at[kind, i, 2], x_dev),
                remote(shard(kind, i, 2, HI), shard(kind, i, 3, HI), ag_send.at[kind, i, 3], ag_recv.at[kind, i, 3], y_dev))

    def ag_forward(kind, i):
        for copy in ag_first(kind, i, shard(kind, i, 0)):
            copy.wait_recv()
        start_all(ag_second(kind, i))

    def ag_arrived(kind, i):
        for copy in ag_second(kind, i):
            copy.wait_recv()

    def rs_first(task):
        return (remote(part.at[task, 1, :, :, LO], ra1.at[task], rs_send.at[task, 0], rs_recv.at[task, 0], x_dev),
                remote(part.at[task, :, 1, :, HI], rb1.at[task], rs_send.at[task, 1], rs_recv.at[task, 1], y_dev))

    def rs_second(task):
        slot = task % 2
        return (remote(snd.at[slot, 0], ra2.at[task], rs_send.at[task, 2], rs_recv.at[task, 2], y_dev),
                remote(snd.at[slot, 1], rb2.at[task], rs_send.at[task, 3], rs_recv.at[task, 3], x_dev))

    def rs_middle(task):
        slot = task % 2

        @pl.when(task >= 2)
        def _():
            for copy in rs_second(task - 2):
                copy.wait_send()

        mine = (part.at[task, 0, :, :, LO], part.at[task, :, 0, :, HI])
        for side, (came, received) in enumerate(zip((ra1, rb1), rs_first(task))):
            received.wait_recv()
            run_all((local(mine[side], ld.at[0], l_sem.at[0]), local(came.at[task], ld.at[1], l_sem.at[1])))
            snd[slot, side] = ld[0, 1] + ld[1, 1]
            keep[slot, :, pl.ds(side * HALF, HALF)] = ld[0, 0] + ld[1, 0]
            rs_second(task)[side].start()

    def dx_copies(i, slot):
        dst = dx.at[i, pl.ds(core * ROWS, ROWS)]
        return (local(new.at[slot], dst, dx_send.at[i, 0]), remote(new.at[slot], dst, dx_send.at[i, 1], dx_recv.at[i], twin))

    def dx_sent(i):
        stored, sent = dx_copies(i, i % 2)
        stored.wait()
        sent.wait_send()

    def rs_last(task):
        slot, kind, i = task % 2, task // CHUNKS, task % CHUNKS
        for copy in rs_second(task):
            copy.wait_recv()
        run_all((local(ra2.at[task], r2.at[:, LO], l_sem.at[0]), local(rb2.at[task], r2.at[:, HI], l_sem.at[1]),
                 local(shard((3 * kind + 1) // 2, i, 0), own.at[0], l_sem.at[2]), local(shard(kind % 2, i, 0), own.at[1], l_sem.at[3])))

        @pl.when(task >= 2 * CHUNKS + 2)
        def _():
            dx_sent(i - 2)

        def rows_step(r, _):
            rows = pl.ds(r * 32, 32)
            total = keep[slot, rows, :] + r2[rows, :]

            @pl.when(kind == 0)
            def _():
                new[slot, rows, :] = own[0, rows, :] + total.astype(BF16)

            @pl.when(kind > 0)
            def _():
                tok = own[1, rows, :].astype(F32)
                inv = lax.rsqrt(jnp.mean(tok * tok, axis=-1, keepdims=True) + EPS)
                dot = jnp.mean(tok * total, axis=-1, keepdims=True)
                resid = total * inv - tok * (inv * inv * inv * dot)
                new[slot, rows, :] = (own[0, rows, :].astype(F32) + resid).astype(BF16)
            return 0

        lax.fori_loop(0, ROWS // 32, rows_step, 0)

        @pl.when(kind < 2)
        def _():
            mine = shard(2 * kind + 1, i, 0)
            run_all((local(new.at[slot], mine, l_sem.at[0]),))
            start_all(ag_first(2 * kind + 1, i, mine))

        @pl.when(kind == 2)
        def _():
            start_all(dx_copies(i, slot))

    def w_copies(mtx, block, n):
        src, dst = ((wg_in, wx), (wx, wi_in))[mtx][block], (wg, wi)[mtx]
        rows = pl.ds(chip * QUARTER + n * ROWS, ROWS)
        return [remote(src.at[pl.ds(n * ROWS, ROWS), pl.ds(to * WIDTH, WIDTH)], dst.at[block, rows],
                       w_send.at[block, n, k], w_recv.at[block, n, k], (to, core)) for k, to in enumerate(near)]

    def w_forwards(mtx, block, n):
        pieces = [(wg, wi)[mtx].at[block, pl.ds(came * QUARTER + n * ROWS, ROWS)] for came in near]
        return [remote(piece, piece, f_send.at[block, n, k], f_recv.at[block, n, k], twin) for k, piece in enumerate(pieces)]

    def w_start(block, n):
        for mtx in range(2):
            @pl.when(core == mtx)
            def _(mtx=mtx):
                start_all(w_copies(mtx, block, n))

    def w_pass_on(block, n):
        for mtx in range(2):
            @pl.when(core == mtx)
            def _(mtx=mtx):
                for came, onward in zip(w_copies(mtx, block, n), w_forwards(mtx, block, n)):
                    came.wait_recv()
                    onward.start()

    def w_hand(mtx):
        return remote((wg_in, wi_in)[mtx], wx, d_send.at[3], d_recv.at[3], twin)

    def w_twin(block):
        rows, cols = pl.ds(chip * QUARTER, QUARTER), pl.ds(chip * WIDTH, WIDTH)
        return (remote(wg_in.at[:, cols], wg.at[block, rows], d_send.at[0], d_recv.at[0], twin),
                remote(wi_in.at[:, cols], wi.at[block, rows], d_send.at[1], d_recv.at[1], twin),
                remote(wo_in, wo.at[block], d_send.at[2], d_recv.at[2], twin))

    def w_arrived(block):
        for n in range(QUARTER // ROWS):
            for copy in w_forwards(0, block, n):
                copy.wait_recv()

        @pl.when(core != block)
        def _():
            for copy in w_twin(block):
                copy.wait_recv()

    def op_pairs(i, src):
        rows = pl.ds(i * BLOCK_ROWS, BLOCK_ROWS)
        return ((tb.at[0], lhs.at[0, src, :, rows]), (tb.at[1], lhs.at[1, src, :, rows]), (dab, rhs.at[0, src, rows]),
                (dbb, rhs.at[1, src, rows]), (ab.at[1], rhs.at[2, src, rows]))

    def op_start(n, i, block):
        src, dst = op_pairs(i, core)[n]

        @pl.when(block == core)
        def _():
            local(src, dst, op_send.at[n]).start()

        @pl.when(block != core)
        def _():
            remote(src, dst, op_send.at[n], op_recv.at[i, n], twin).start()

    def op_sent(i):
        for n, (src, dst) in enumerate(op_pairs(i, core)):
            local(src, dst, op_send.at[n]).wait()

    def op_arrived(i):
        for n, (src, dst) in enumerate(op_pairs(i, other)):
            remote(src, dst, op_send.at[n], op_recv.at[i, n], twin).wait_recv()

    def normalize():
        def rows_step(r, _):
            rows = pl.ds(r * 64, 64)
            tok = ab[0, rows, :].astype(F32)
            inv = lax.rsqrt(jnp.mean(tok * tok, axis=-1, keepdims=True) + EPS)
            ab[0, rows, :] = (tok * inv).astype(BF16)
            return 0

        lax.fori_loop(0, BLOCK_ROWS // 64, rows_step, 0)

    def write_partials(task, product):
        def tile_copy(n, slot):
            return local(pst.at[slot], part.at[task, :, :, :, pl.ds(n * TILE, TILE)], p_sem.at[slot])

        def half_step(side, _):
            def tile_step(t, _):
                n, slot = side * (TILES // 2) + t, t % 2

                @pl.when(t >= 2)
                def _():
                    tile_copy(n - 2, slot).wait()

                pst[slot] = product(pl.ds(n * TILE, TILE)).reshape(2, 2, ROWS, TILE)
                tile_copy(n, slot).start()
                return 0

            lax.fori_loop(0, TILES // 2, tile_step, 0)
            last = (side + 1) * (TILES // 2)
            tile_copy(last - 2, 0).wait()
            tile_copy(last - 1, 1).wait()
            for n in range(2):
                @pl.when(side == n)
                def _(n=n):
                    rs_first(task)[n].start()
            return 0

        lax.fori_loop(0, 2, half_step, 0)

    def forward(task):
        ag_arrived(0, task)
        run_all((local(act.at[0, task], ab.at[0], l_sem.at[0]),))
        normalize()

        def tile_step(t, _):
            cols = pl.ds(t * TILE, TILE)
            pre_gate = mm(ab[0], wbuf[0, :, cols], 0)
            pre_in = mm(ab[0], wbuf[1, :, cols], 0)
            dab[:, cols] = (pre_gate * jax.nn.sigmoid(pre_gate) * pre_in).astype(BF16)
            return 0

        lax.fori_loop(0, TILES, tile_step, 0)

    def forward_out(task):
        write_partials(task, lambda cols: mm(dab[...], wbuf[2, :, cols], 0))

    def backward(task):
        kind, i = task // CHUNKS, task % CHUNKS
        block = 2 - kind

        @pl.when(task > CHUNKS)
        def _():
            op_sent(i)

        @pl.when(kind == 1)
        def _():
            ag_arrived(1, i)
            ag_arrived(2, i)

        @pl.when(kind == 2)
        def _():
            ag_arrived(3, i)

        run_all((local(act.at[2 - kind, i], ab.at[0], l_sem.at[0]), local(act.at[kind + 1, i], ab.at[1], l_sem.at[1])))
        op_start(4, i, block)
        normalize()

        def turn_step(t, _):
            cols = pl.ds(t * TILE, TILE)
            tb[0, cols, :] = ab[0, :, cols].T
            return 0

        lax.fori_loop(0, TILES, turn_step, 0)
        op_start(0, i, block)

        def tile_step(t, _):
            cols = pl.ds(t * TILE, TILE)
            pre_gate = mm(ab[0], wbuf[0, :, cols], 0)
            pre_in = mm(ab[0], wbuf[1, :, cols], 0)
            d_hidden = mm(ab[1], wbuf[2, cols, :], 1)
            sigma = jax.nn.sigmoid(pre_gate)
            gate_act = pre_gate * sigma
            tb[1, cols, :] = (gate_act * pre_in).astype(BF16).T
            dab[:, cols] = (d_hidden * pre_in * sigma * (1.0 + pre_gate * (1.0 - sigma))).astype(BF16)
            dbb[:, cols] = (d_hidden * gate_act).astype(BF16)
            return 0

        lax.fori_loop(0, TILES, tile_step, 0)
        for n in (1, 2, 3):
            op_start(n, i, block)

    def backward_out(task):
        write_partials(task, lambda rows: mm(dab[...], wbuf[0, rows, :], 1) + mm(dbb[...], wbuf[1, rows, :], 1))

    def rhs_copies(mtx, n, slot):
        return [local(rhs.at[mtx, q, :, pl.ds(n * TILE, TILE)], tb.at[slot, :, pl.ds(q * TILE, TILE)], t_sem.at[slot, q]) for q in range(2)]

    def grad_sent(slot):
        for k in range(4):
            local(outs.at[slot, pl.ds(0, QUARTER)], dwo.at[pl.ds(0, QUARTER), pl.ds(0, TILE)], gr_send.at[slot, k]).wait()

    def grad_tile(t):
        mtx, slot = t // TILES, t % SLOTS
        col = (t % TILES) * TILE

        @pl.when(t == 0)
        def _():
            op_sent(0)
            for i in range(CHUNKS):
                op_arrived(i)
            start_all(rhs_copies(0, 0, 0))
            run_all([local(lhs.at[0, q], wbuf.at[q], l_sem.at[q]) for q in range(2)])

        for copy in rhs_copies(mtx, t % TILES, 0):
            copy.wait()

        @pl.when(t >= SLOTS)
        def _():
            grad_sent(slot)

        def quarter_step(k, _):
            ax, ay = 1 - k % 2, ((k + 1) // 2) % 2
            to = (cy + ay - 2 * cy * ay) * 2 + (cx + ax - 2 * cx * ax)
            rows = pl.ds(to * QUARTER, QUARTER)
            outs[slot, rows, :] = mm(wbuf[0, rows, :], tb[0, :, 0:TILE], 0) + mm(wbuf[1, rows, :], tb[0, :, TILE:2 * TILE], 0)
            cols = pl.ds(chip * WIDTH + col, TILE)
            for n, dst in enumerate((dwg, dwi)):
                @pl.when((mtx == n) & (k < 3) & (t < SENT_TILES - LATE_TILES))
                def _(n=n, dst=dst):
                    remote(outs.at[slot, rows], dst.at[:, cols], gr_send.at[slot, k], gr_recv.at[n, k], (to, core)).start()

                @pl.when((mtx == n) & (k == 3) & (t < SENT_TILES - LATE_TILES))
                def _(dst=dst):
                    local(outs.at[slot, rows], dst.at[:, cols], gr_send.at[slot, k]).start()

            @pl.when(t >= SENT_TILES - LATE_TILES)
            def _():
                cols = pl.ds((t - SENT_TILES + LATE_TILES) * TILE, TILE)
                local(outs.at[slot, rows], late.at[to, :, cols], gr_send.at[slot, k]).start()
            return 0

        lax.fori_loop(0, 4, quarter_step, 0)

        @pl.when(t + 1 < SENT_TILES)
        def _():
            start_all(rhs_copies((t + 1) // TILES, (t + 1) % TILES, 0))

    def out_loads(k, slot):
        return [local(lhs.at[1, q, pl.ds(k * QUARTER, QUARTER)], wbuf.at[2, pl.ds(slot * HALF + q * QUARTER, QUARTER)], o_sem.at[slot, q]) for q in range(2)]

    def out_store(n, k, slot):
        return local(wo_out.at[slot], dwo.at[pl.ds(k * QUARTER, QUARTER), pl.ds(n * TILE, TILE)], o_sem.at[slot, 2])

    def out_tile(n):
        start_all(rhs_copies(2, n, 1))
        start_all(out_loads(0, 0))
        for copy in rhs_copies(2, n, 1):
            copy.wait()

        def quarter_step(k, _):
            slot = k % 2

            @pl.when(k < 3)
            def _():
                start_all(out_loads(k + 1, 1 - slot))

            for copy in out_loads(k, slot):
                copy.wait()

            @pl.when(4 * n + k >= 2)
            def _():
                out_store(n, k, slot).wait()

            top, low = pl.ds(slot * HALF, QUARTER), pl.ds(slot * HALF + QUARTER, QUARTER)
            wo_out[slot] = mm(wbuf[2, top, :], tb[1, :, 0:TILE], 0) + mm(wbuf[2, low, :], tb[1, :, TILE:2 * TILE], 0)
            out_store(n, k, slot).start()
            return 0

        lax.fori_loop(0, 4, quarter_step, 0)

    barrier = pltpu.get_barrier_semaphore()
    for dev in [(to, core) for to in near] + [twin]:
        pl.semaphore_signal(barrier, inc=1, device_id=dev, device_id_type=MESH)
    pl.semaphore_wait(barrier, 4)

    def my_rows(arr, i):
        return arr.at[i, pl.ds(core * ROWS, ROWS)]

    for i in range(2):
        start_all(ag_first(0, i, my_rows(x, i)))

    @pl.when(core == 0)
    def _():
        w_hand(1).start()
        for n in range(4):
            start_all(w_copies(0, 0, n))

    @pl.when(core == 1)
    def _():
        w_hand(0).start()

    w_hand(0).wait_recv()

    @pl.when(core == 1)
    def _():
        for n in range(4):
            start_all(w_copies(1, 0, n))

    start_all(w_twin(core))
    rows, cols = pl.ds(chip * QUARTER, QUARTER), pl.ds(chip * WIDTH, WIDTH)
    top = pl.ds(0, QUARTER)
    loads = [local(wg_in.at[:, cols], wbuf.at[0, top], l_sem.at[0]), local(wi_in.at[:, cols], wbuf.at[1, top], l_sem.at[1]),
             local(wo_in, wbuf.at[2], l_sem.at[2])]
    stores = [local(wbuf.at[0, top], wg.at[core, rows], l_sem.at[0]), local(wbuf.at[1, top], wi.at[core, rows], l_sem.at[1]),
              local(wbuf.at[2], wo.at[core], l_sem.at[2])]
    for n, (arr, kind) in enumerate(((x, 0), (g, 2))):
        for i in range(CHUNKS):
            spot = ab.at[n, pl.ds(i * ROWS, ROWS)]
            loads.append(local(my_rows(arr, i), spot, t_sem.at[n, i]))
            stores.append(local(spot, shard(kind, i, 0), t_sem.at[n, i]))
    run_all(loads)
    run_all(stores)
    for i in range(2):
        ag_forward(0, i)

    for n in range(4):
        w_pass_on(0, n)
    w_arrived(0)

    def when_task(tick, first, last):
        def run(body):
            @pl.when((tick >= 0) & (tick != TURN) & (tick <= CHAIN))
            def _():
                task = tick - jnp.where(tick > TURN, 1, 0)

                @pl.when((task >= first) & (task < last))
                def _():
                    body(task)
        return run

    def tick_step(tick, _):
        @pl.when(tick < 2)
        def _():
            start_all(ag_first(0, tick + 2, my_rows(x, tick + 2)))

        @pl.when((tick >= 2) & (tick < 2 + CHUNKS))
        def _():
            start_all(ag_first(2, tick - 2, my_rows(g, tick - 2)))

        @pl.when(tick < 4)
        def _():
            w_start(1, tick)

        @pl.when(tick == TURN + 1)
        def _():
            w_arrived(1)

        @when_task(tick, 0, CHAIN)
        def _(task):
            @pl.when(task % CHUNKS == 0)
            def _():
                block = (task // CHUNKS) % 2
                run_all([local(src.at[block], wbuf.at[n], l_sem.at[n]) for n, src in enumerate((wg, wi, wo))])

        when_task(tick, 0, CHUNKS)(forward)
        when_task(tick, CHUNKS, CHAIN)(backward)

        @pl.when(tick > CHAIN)
        def _():
            grad_tile(tick - CHAIN - 1)

        @pl.when((tick > CHAIN + SLOTS) & (tick <= CHAIN + SLOTS + TILES))
        def _():
            out_tile(tick - CHAIN - SLOTS - 1)

        @pl.when(tick < 2)
        def _():
            ag_forward(0, tick + 2)

        @when_task(tick - 3, 0, 2 * CHUNKS)
        def _(task):
            ag_forward(2 * (task // CHUNKS) + 1, task % CHUNKS)

        when_task(tick - 2, 0, CHAIN)(rs_last)
        when_task(tick - 1, 0, CHAIN)(rs_middle)

        @pl.when((tick >= 2) & (tick < 2 + CHUNKS))
        def _():
            ag_forward(2, tick - 2)

        @pl.when((tick >= 1) & (tick < 5))
        def _():
            w_pass_on(1, tick - 1)
        when_task(tick, 0, CHUNKS)(forward_out)
        when_task(tick, CHUNKS, CHAIN)(backward_out)
        return 0

    lax.fori_loop(0, CHAIN + 1 + SENT_TILES, tick_step, 0)

    for n, dst in enumerate((dwg, dwi)):
        for k, came in enumerate(near):
            block = dst.at[:, pl.ds(came * WIDTH, WIDTH - n * LATE_TILES * TILE)]
            local(block, block, gr_recv.at[n, k]).wait()
    for slot in range(SLOTS):
        grad_sent(slot)
    for slot in range(2):
        out_store(0, 0, slot).wait()
    for i in range(CHUNKS):
        dx_copies(i, 0)[1].wait_recv()
    dx_sent(2)
    dx_sent(3)

    def drain_gathers(n, _):
        kind, i = n // CHUNKS, n % CHUNKS
        for copy in ag_first(kind, i, shard(kind, i, 0)) + ag_second(kind, i):
            copy.wait_send()
        return 0

    def drain_sums(task, _):
        for copy in rs_first(task):
            copy.wait_send()
        return 0

    lax.fori_loop(0, 4 * CHUNKS, drain_gathers, 0)
    lax.fori_loop(0, CHAIN, drain_sums, 0)
    for task in (CHAIN - 2, CHAIN - 1):
        for copy in rs_second(task):
            copy.wait_send()
    for block in range(2):
        for n in range(4):
            for copy in w_copies(0, block, n) + w_forwards(0, block, n):
                copy.wait_send()
    for copy in w_twin(core) + (w_hand(0),):
        copy.wait_send()


def settle_kernel(*refs):
    for src, dst in zip(refs[:len(refs) // 2], refs[len(refs) // 2:]):
        dst[...] = src[...]


def settle(arrays, steps=16):
    specs = [pl.BlockSpec((arr.shape[0] // steps, arr.shape[1]), lambda i: (i, 0)) for arr in arrays]
    size = sum(arr.size * arr.dtype.itemsize for arr in arrays)
    return pl.pallas_call(
        settle_kernel, grid=(steps,), out_shape=[jax.ShapeDtypeStruct(arr.shape, arr.dtype) for arr in arrays], in_specs=specs, out_specs=specs,
        name='settle', cost_estimate=pl.CostEstimate(flops=SETTLE_FLOPS, bytes_accessed=2 * size, transcendentals=0),
        compiler_params=pltpu.CompilerParams(vmem_limit_bytes=48 * 2 ** 20),
    )(*arrays)


def insert_kernel(late, whole, out):
    out[...] = late[0]


def insert_late(whole, late):
    chips, rows, cols = late.shape
    step = rows // 2
    return pl.pallas_call(
        insert_kernel, grid=(chips, 2), out_shape=jax.ShapeDtypeStruct(whole.shape, whole.dtype),
        in_specs=[pl.BlockSpec((1, step, cols), lambda c, r: (c, r, 0)), pl.BlockSpec(memory_space=pl.ANY)],
        out_specs=pl.BlockSpec((step, cols), lambda c, r: (r, (c + 1) * (WIDTH // cols) - 1)), input_output_aliases={1: 0}, name='insert_late',
    )(late, whole)


def solution(mesh):
    act_spec = P(None, 'data', None, None)
    weight_spec = P('stage', None, 'data', None)

    def per_device(x, g, w_gate, w_in, w_out):
        flat = (CHUNKS, 2 * ROWS, WIDTH)
        dma = pltpu.SemaphoreType.DMA
        any_space = pl.BlockSpec(memory_space=pl.ANY)

        def arr(*shape, dtype=BF16):
            return jax.ShapeDtypeStruct(shape, dtype)

        out_shapes = [
            arr(*flat), arr(QUARTER, 4 * WIDTH, dtype=F32), arr(QUARTER, 4 * WIDTH, dtype=F32), arr(WIDTH, WIDTH, dtype=F32), arr(4, QUARTER, LATE_TILES * TILE, dtype=F32),
            arr(4, CHUNKS, BLOCK_ROWS, WIDTH), arr(2, WIDTH, WIDTH), arr(2, WIDTH, WIDTH), arr(2, WIDTH, WIDTH), arr(QUARTER, 4 * WIDTH),
            arr(CHAIN, 2, 2, ROWS, WIDTH, dtype=F32),
            arr(CHAIN, 2, ROWS, HALF, dtype=F32), arr(CHAIN, 2, ROWS, HALF, dtype=F32),
            arr(CHAIN, ROWS, HALF, dtype=F32), arr(CHAIN, ROWS, HALF, dtype=F32),
            arr(2, 2, WIDTH, WIDTH), arr(3, 2, WIDTH, WIDTH),
        ]
        scratch = [
            pltpu.VMEM((3, WIDTH, WIDTH), BF16), pltpu.VMEM((2, BLOCK_ROWS, WIDTH), BF16), pltpu.VMEM((2, WIDTH, BLOCK_ROWS), BF16),
            pltpu.VMEM((BLOCK_ROWS, WIDTH), BF16), pltpu.VMEM((BLOCK_ROWS, WIDTH), BF16),
            pltpu.VMEM((2, 2, 2, ROWS, TILE), F32), pltpu.VMEM((2, ROWS, WIDTH), F32), pltpu.VMEM((2, 2, ROWS, HALF), F32),
            pltpu.VMEM((2, 2, ROWS, HALF), F32), pltpu.VMEM((ROWS, WIDTH), F32), pltpu.VMEM((2, ROWS, WIDTH), BF16),
            pltpu.VMEM((2, ROWS, WIDTH), BF16), pltpu.VMEM((SLOTS, WIDTH, TILE), F32),
            pltpu.VMEM((2, QUARTER, TILE), F32),
            dma((4, CHUNKS, 4)), dma((4, CHUNKS, 4)), dma((CHAIN, 4)), dma((CHAIN, 4)),
            dma((2, 4, 3)), dma((2, 4, 3)), dma((2, 4, 3)), dma((2, 4, 3)), dma((4,)), dma((4,)),
            dma((5,)), dma((CHUNKS, 5)), dma((CHUNKS, 2)), dma((CHUNKS,)), dma((SLOTS, 4)), dma((2, 3)),
            dma((2,)), dma((4,)), dma((2, 4)), dma((2, 3)),
        ]
        results = pl.pallas_call(
            step_kernel, out_shape=out_shapes, in_specs=[any_space] * 5, out_specs=[any_space] * len(out_shapes),
            scratch_shapes=scratch, name='mlp_step',
            compiler_params=pltpu.CompilerParams(collective_id=0, has_side_effects=True, vmem_limit_bytes=67_043_328),
        )(x.reshape(flat), g.reshape(flat), w_gate[0, 0], w_in[0, 0], w_out[0, 0])
        dx, d_gate, d_in, d_out, late = results[:5]
        late = lax.all_to_all(late, 'data', 0, 0)
        dx, d_gate, d_in, d_out = settle((dx.reshape(-1, WIDTH), d_gate, d_in, d_out))
        d_in = insert_late(d_in, late)
        return dx.reshape(x.shape), d_gate[None, None], d_in[None, None], d_out[None, None]

    return jax.shard_map(per_device, mesh=mesh, in_specs=(act_spec, act_spec, weight_spec, weight_spec, weight_spec),
                         out_specs=(act_spec, weight_spec, weight_spec, weight_spec), check_vma=False)
```

```python
import jax
import jax.numpy as jnp
from jax import lax
from jax.experimental import pallas as pl
from jax.experimental.pallas import tpu as pltpu
from jax.sharding import PartitionSpec as P

MESH = pl.DeviceIdType.MESH
F32 = jnp.float32
BF16 = jnp.bfloat16
EPS = 1e-6

CHUNKS = 4
ROWS = 128
BLOCK_ROWS = 4 * ROWS
WIDTH = 2048
HALF = WIDTH // 2
QUARTER = WIDTH // 4
TILE = 256
TILES = WIDTH // TILE
CHAIN = 3 * CHUNKS
TURN = CHUNKS
G_TICKS = ((2, (0,)), (3, (1,)), (TURN + 1, (2, 3)))
SENT_TILES = 2 * TILES
LATE_TILES = 2
SETTLE_FLOPS = 2 ** 30
SLOTS = 4
LO, HI = pl.ds(0, HALF), pl.ds(HALF, HALF)


def mm(lhs, rhs, rhs_dim):
    return lax.dot_general(lhs, rhs, (((1,), (rhs_dim,)), ((), ())), preferred_element_type=F32)


def start_all(copies):
    for copy in copies:
        copy.start()


def run_all(copies):
    start_all(copies)
    for copy in copies:
        copy.wait()


def step_kernel(x, g, wg_in, wi_in, wo_in,
                dx, dwg, dwi, dwo, late, act, wg, wi, wo, wx, part, ra1, rb1, ra2, rb2, lhs, rhs,
                wbuf, ab, tb, dab, dbb, pst, keep, snd, ld, r2, own, new, outs, wo_out,
                ag_send, ag_recv, rs_send, rs_recv, w_send, w_recv, f_send, f_recv, d_send, d_recv,
                op_send, op_recv, dx_send, dx_recv, gr_send, gr_recv, p_sem, l_sem, t_sem, o_sem):
    chip = lax.axis_index('data')
    core = lax.axis_index('stage')
    cx, cy = chip % 2, chip // 2
    near = (cy * 2 + (1 - cx), (1 - cy) * 2 + cx, (1 - cy) * 2 + (1 - cx))
    other = 1 - core
    x_dev, y_dev, twin = (near[0], core), (near[1], core), (chip, other)

    def local(src, dst, sem):
        return pltpu.make_async_copy(src, dst, sem)

    def remote(src, dst, send, recv, dev):
        return pltpu.make_async_remote_copy(src_ref=src, dst_ref=dst, send_sem=send, recv_sem=recv, device_id=dev, device_id_type=MESH)

    def shard(kind, i, n, cols=slice(None)):
        return act.at[kind, i, pl.ds(n * ROWS, ROWS), cols]

    def ag_first(kind, i, src):
        return (remote(src, shard(kind, i, 2), ag_send.at[kind, i, 0], ag_recv.at[kind, i, 0], x_dev),
                remote(src, shard(kind, i, 1), ag_send.at[kind, i, 1], ag_recv.at[kind, i, 1], y_dev))

    def ag_second(kind, i):
        return (remote(shard(kind, i, 1, LO), shard(kind, i, 3, LO), ag_send.at[kind, i, 2], ag_recv.at[kind, i, 2], x_dev),
                remote(shard(kind, i, 2, HI), shard(kind, i, 3, HI), ag_send.at[kind, i, 3], ag_recv.at[kind, i, 3], y_dev))

    def ag_forward(kind, i):
        for copy in ag_first(kind, i, shard(kind, i, 0)):
            copy.wait_recv()
        start_all(ag_second(kind, i))

    def ag_arrived(kind, i):
        for copy in ag_second(kind, i):
            copy.wait_recv()

    def rs_first(task):
        return (remote(part.at[task, 1, :, :, LO], ra1.at[task], rs_send.at[task, 0], rs_recv.at[task, 0], x_dev),
                remote(part.at[task, :, 1, :, HI], rb1.at[task], rs_send.at[task, 1], rs_recv.at[task, 1], y_dev))

    def rs_second(task):
        slot = task % 2
        return (remote(snd.at[slot, 0], ra2.at[task], rs_send.at[task, 2], rs_recv.at[task, 2], y_dev),
                remote(snd.at[slot, 1], rb2.at[task], rs_send.at[task, 3], rs_recv.at[task, 3], x_dev))

    def rs_middle(task):
        slot = task % 2

        @pl.when(task >= 2)
        def _():
            for copy in rs_second(task - 2):
                copy.wait_send()

        mine = (part.at[task, 0, :, :, LO], part.at[task, :, 0, :, HI])
        for side, (came, received) in enumerate(zip((ra1, rb1), rs_first(task))):
            received.wait_recv()
            run_all((local(mine[side], ld.at[0], l_sem.at[0]), local(came.at[task], ld.at[1], l_sem.at[1])))
            snd[slot, side] = ld[0, 1] + ld[1, 1]
            keep[slot, :, pl.ds(side * HALF, HALF)] = ld[0, 0] + ld[1, 0]
            rs_second(task)[side].start()

    def dx_copies(i, slot):
        dst = dx.at[i, pl.ds(core * ROWS, ROWS)]
        return (local(new.at[slot], dst, dx_send.at[i, 0]), remote(new.at[slot], dst, dx_send.at[i, 1], dx_recv.at[i], twin))

    def dx_sent(i):
        stored, sent = dx_copies(i, i % 2)
        stored.wait()
        sent.wait_send()

    def rs_last(task):
        slot, kind, i = task % 2, task // CHUNKS, task % CHUNKS
        for copy in rs_second(task):
            copy.wait_recv()
        run_all((local(ra2.at[task], r2.at[:, LO], l_sem.at[0]), local(rb2.at[task], r2.at[:, HI], l_sem.at[1]),
                 local(shard((3 * kind + 1) // 2, i, 0), own.at[0], l_sem.at[2]), local(shard(kind % 2, i, 0), own.at[1], l_sem.at[3])))

        @pl.when(task >= 2 * CHUNKS + 2)
        def _():
            dx_sent(i - 2)

        def rows_step(r, _):
            rows = pl.ds(r * 32, 32)
            total = keep[slot, rows, :] + r2[rows, :]

            @pl.when(kind == 0)
            def _():
                new[slot, rows, :] = own[0, rows, :] + total.astype(BF16)

            @pl.when(kind > 0)
            def _():
                tok = own[1, rows, :].astype(F32)
                inv = lax.rsqrt(jnp.mean(tok * tok, axis=-1, keepdims=True) + EPS)
                dot = jnp.mean(tok * total, axis=-1, keepdims=True)
                resid = total * inv - tok * (inv * inv * inv * dot)
                new[slot, rows, :] = (own[0, rows, :].astype(F32) + resid).astype(BF16)
            return 0

        lax.fori_loop(0, ROWS // 32, rows_step, 0)

        @pl.when(kind < 2)
        def _():
            mine = shard(2 * kind + 1, i, 0)
            run_all((local(new.at[slot], mine, l_sem.at[0]),))
            start_all(ag_first(2 * kind + 1, i, mine))

        @pl.when(kind == 2)
        def _():
            start_all(dx_copies(i, slot))

    def w_copies(mtx, block, n):
        src, dst = ((wg_in, wx), (wx, wi_in))[mtx][block], (wg, wi)[mtx]
        rows = pl.ds(chip * QUARTER + n * ROWS, ROWS)
        return [remote(src.at[pl.ds(n * ROWS, ROWS), pl.ds(to * WIDTH, WIDTH)], dst.at[block, rows],
                       w_send.at[block, n, k], w_recv.at[block, n, k], (to, core)) for k, to in enumerate(near)]

    def w_forwards(mtx, block, n):
        pieces = [(wg, wi)[mtx].at[block, pl.ds(came * QUARTER + n * ROWS, ROWS)] for came in near]
        return [remote(piece, piece, f_send.at[block, n, k], f_recv.at[block, n, k], twin) for k, piece in enumerate(pieces)]

    def w_start(block, n):
        for mtx in range(2):
            @pl.when(core == mtx)
            def _(mtx=mtx):
                start_all(w_copies(mtx, block, n))

    def w_pass_on(block, n):
        for mtx in range(2):
            @pl.when(core == mtx)
            def _(mtx=mtx):
                for came, onward in zip(w_copies(mtx, block, n), w_forwards(mtx, block, n)):
                    came.wait_recv()
                    onward.start()

    def w_hand(mtx):
        return remote((wg_in, wi_in)[mtx], wx, d_send.at[3], d_recv.at[3], twin)

    def w_twin(block):
        rows, cols = pl.ds(chip * QUARTER, QUARTER), pl.ds(chip * WIDTH, WIDTH)
        return (remote(wg_in.at[:, cols], wg.at[block, rows], d_send.at[0], d_recv.at[0], twin),
                remote(wi_in.at[:, cols], wi.at[block, rows], d_send.at[1], d_recv.at[1], twin),
                remote(wo_in, wo.at[block], d_send.at[2], d_recv.at[2], twin))

    def w_arrived(block):
        for n in range(QUARTER // ROWS):
            for copy in w_forwards(0, block, n):
                copy.wait_recv()

        @pl.when(core != block)
        def _():
            for copy in w_twin(block):
                copy.wait_recv()

    def op_pairs(i, src):
        rows = pl.ds(i * BLOCK_ROWS, BLOCK_ROWS)
        return ((tb.at[0], lhs.at[0, src, :, rows]), (tb.at[1], lhs.at[1, src, :, rows]), (dab, rhs.at[0, src, rows]),
                (dbb, rhs.at[1, src, rows]), (ab.at[1], rhs.at[2, src, rows]))

    def op_start(n, i, block):
        src, dst = op_pairs(i, core)[n]

        @pl.when(block == core)
        def _():
            local(src, dst, op_send.at[n]).start()

        @pl.when(block != core)
        def _():
            remote(src, dst, op_send.at[n], op_recv.at[i, n], twin).start()

    def op_sent(i):
        for n, (src, dst) in enumerate(op_pairs(i, core)):
            local(src, dst, op_send.at[n]).wait()

    def op_arrived(i):
        for n, (src, dst) in enumerate(op_pairs(i, other)):
            remote(src, dst, op_send.at[n], op_recv.at[i, n], twin).wait_recv()

    def normalize():
        def rows_step(r, _):
            rows = pl.ds(r * 64, 64)
            tok = ab[0, rows, :].astype(F32)
            inv = lax.rsqrt(jnp.mean(tok * tok, axis=-1, keepdims=True) + EPS)
            ab[0, rows, :] = (tok * inv).astype(BF16)
            return 0

        lax.fori_loop(0, BLOCK_ROWS // 64, rows_step, 0)

    def write_partials(task, product):
        def tile_copy(n, slot):
            return local(pst.at[slot], part.at[task, :, :, :, pl.ds(n * TILE, TILE)], p_sem.at[slot])

        def half_step(side, _):
            def tile_step(t, _):
                n, slot = side * (TILES // 2) + t, t % 2

                @pl.when(t >= 2)
                def _():
                    tile_copy(n - 2, slot).wait()

                pst[slot] = product(pl.ds(n * TILE, TILE)).reshape(2, 2, ROWS, TILE)
                tile_copy(n, slot).start()
                return 0

            lax.fori_loop(0, TILES // 2, tile_step, 0)
            last = (side + 1) * (TILES // 2)
            tile_copy(last - 2, 0).wait()
            tile_copy(last - 1, 1).wait()
            for n in range(2):
                @pl.when(side == n)
                def _(n=n):
                    rs_first(task)[n].start()
            return 0

        lax.fori_loop(0, 2, half_step, 0)

    def forward(task):
        ag_arrived(0, task)
        run_all((local(act.at[0, task], ab.at[0], l_sem.at[0]),))
        normalize()

        def tile_step(t, _):
            cols = pl.ds(t * TILE, TILE)
            pre_gate = mm(ab[0], wbuf[0, :, cols], 0)
            pre_in = mm(ab[0], wbuf[1, :, cols], 0)
            dab[:, cols] = (pre_gate * jax.nn.sigmoid(pre_gate) * pre_in).astype(BF16)
            return 0

        lax.fori_loop(0, TILES, tile_step, 0)

    def forward_out(task):
        write_partials(task, lambda cols: mm(dab[...], wbuf[2, :, cols], 0))

    def backward(task):
        kind, i = task // CHUNKS, task % CHUNKS
        block = 2 - kind

        @pl.when(task > CHUNKS)
        def _():
            op_sent(i)

        @pl.when(kind == 1)
        def _():
            ag_arrived(1, i)
            ag_arrived(2, i)

        @pl.when(kind == 2)
        def _():
            ag_arrived(3, i)

        run_all((local(act.at[2 - kind, i], ab.at[0], l_sem.at[0]), local(act.at[kind + 1, i], ab.at[1], l_sem.at[1])))
        op_start(4, i, block)
        normalize()

        def turn_step(t, _):
            cols = pl.ds(t * TILE, TILE)
            tb[0, cols, :] = ab[0, :, cols].T
            return 0

        lax.fori_loop(0, TILES, turn_step, 0)
        op_start(0, i, block)

        def tile_step(t, _):
            cols = pl.ds(t * TILE, TILE)
            pre_gate = mm(ab[0], wbuf[0, :, cols], 0)
            pre_in = mm(ab[0], wbuf[1, :, cols], 0)
            d_hidden = mm(ab[1], wbuf[2, cols, :], 1)
            sigma = jax.nn.sigmoid(pre_gate)
            gate_act = pre_gate * sigma
            tb[1, cols, :] = (gate_act * pre_in).astype(BF16).T
            dab[:, cols] = (d_hidden * pre_in * sigma * (1.0 + pre_gate * (1.0 - sigma))).astype(BF16)
            dbb[:, cols] = (d_hidden * gate_act).astype(BF16)
            return 0

        lax.fori_loop(0, TILES, tile_step, 0)
        for n in (1, 2, 3):
            op_start(n, i, block)

    def backward_out(task):
        write_partials(task, lambda rows: mm(dab[...], wbuf[0, rows, :], 1) + mm(dbb[...], wbuf[1, rows, :], 1))

    def rhs_copies(mtx, n, slot):
        return [local(rhs.at[mtx, q, :, pl.ds(n * TILE, TILE)], tb.at[slot, :, pl.ds(q * TILE, TILE)], t_sem.at[slot, q]) for q in range(2)]

    def grad_sent(slot):
        for k in range(4):
            local(outs.at[slot, pl.ds(0, QUARTER)], dwo.at[pl.ds(0, QUARTER), pl.ds(0, TILE)], gr_send.at[slot, k]).wait()

    def grad_tile(t):
        mtx, slot = t // TILES, t % SLOTS
        col = (t % TILES) * TILE

        @pl.when(t == 0)
        def _():
            op_sent(0)
            for i in range(CHUNKS):
                op_arrived(i)
            start_all(rhs_copies(0, 0, 0))
            run_all([local(lhs.at[0, q], wbuf.at[q], l_sem.at[q]) for q in range(2)])

        for copy in rhs_copies(mtx, t % TILES, 0):
            copy.wait()

        @pl.when(t >= SLOTS)
        def _():
            grad_sent(slot)

        def quarter_step(k, _):
            ax, ay = 1 - k % 2, ((k + 1) // 2) % 2
            to = (cy + ay - 2 * cy * ay) * 2 + (cx + ax - 2 * cx * ax)
            rows = pl.ds(to * QUARTER, QUARTER)
            outs[slot, rows, :] = mm(wbuf[0, rows, :], tb[0, :, 0:TILE], 0) + mm(wbuf[1, rows, :], tb[0, :, TILE:2 * TILE], 0)
            cols = pl.ds(chip * WIDTH + col, TILE)
            for n, dst in enumerate((dwg, dwi)):
                @pl.when((mtx == n) & (k < 3) & (t < SENT_TILES - LATE_TILES))
                def _(n=n, dst=dst):
                    remote(outs.at[slot, rows], dst.at[:, cols], gr_send.at[slot, k], gr_recv.at[n, k], (to, core)).start()

                @pl.when((mtx == n) & (k == 3) & (t < SENT_TILES - LATE_TILES))
                def _(dst=dst):
                    local(outs.at[slot, rows], dst.at[:, cols], gr_send.at[slot, k]).start()

            @pl.when(t >= SENT_TILES - LATE_TILES)
            def _():
                cols = pl.ds((t - SENT_TILES + LATE_TILES) * TILE, TILE)
                local(outs.at[slot, rows], late.at[to, :, cols], gr_send.at[slot, k]).start()
            return 0

        lax.fori_loop(0, 4, quarter_step, 0)

        @pl.when(t + 1 < SENT_TILES)
        def _():
            start_all(rhs_copies((t + 1) // TILES, (t + 1) % TILES, 0))

    def out_loads(k, slot):
        return [local(lhs.at[1, q, pl.ds(k * QUARTER, QUARTER)], wbuf.at[2, pl.ds(slot * HALF + q * QUARTER, QUARTER)], o_sem.at[slot, q]) for q in range(2)]

    def out_store(n, k, slot):
        return local(wo_out.at[slot], dwo.at[pl.ds(k * QUARTER, QUARTER), pl.ds(n * TILE, TILE)], o_sem.at[slot, 2])

    def out_tile(n):
        start_all(rhs_copies(2, n, 1))
        start_all(out_loads(0, 0))
        for copy in rhs_copies(2, n, 1):
            copy.wait()

        def quarter_step(k, _):
            slot = k % 2

            @pl.when(k < 3)
            def _():
                start_all(out_loads(k + 1, 1 - slot))

            for copy in out_loads(k, slot):
                copy.wait()

            @pl.when(4 * n + k >= 2)
            def _():
                out_store(n, k, slot).wait()

            top, low = pl.ds(slot * HALF, QUARTER), pl.ds(slot * HALF + QUARTER, QUARTER)
            wo_out[slot] = mm(wbuf[2, top, :], tb[1, :, 0:TILE], 0) + mm(wbuf[2, low, :], tb[1, :, TILE:2 * TILE], 0)
            out_store(n, k, slot).start()
            return 0

        lax.fori_loop(0, 4, quarter_step, 0)

    barrier = pltpu.get_barrier_semaphore()
    for dev in [(to, core) for to in near] + [twin]:
        pl.semaphore_signal(barrier, inc=1, device_id=dev, device_id_type=MESH)
    pl.semaphore_wait(barrier, 4)

    def my_rows(arr, i):
        return arr.at[i, pl.ds(core * ROWS, ROWS)]

    for i in range(2):
        start_all(ag_first(0, i, my_rows(x, i)))

    @pl.when(core == 0)
    def _():
        w_hand(1).start()
        for n in range(4):
            start_all(w_copies(0, 0, n))

    @pl.when(core == 1)
    def _():
        w_hand(0).start()

    w_hand(0).wait_recv()

    @pl.when(core == 1)
    def _():
        for n in range(4):
            start_all(w_copies(1, 0, n))

    start_all(w_twin(core))
    rows, cols = pl.ds(chip * QUARTER, QUARTER), pl.ds(chip * WIDTH, WIDTH)
    top = pl.ds(0, QUARTER)
    loads = [local(wg_in.at[:, cols], wbuf.at[0, top], l_sem.at[0]), local(wi_in.at[:, cols], wbuf.at[1, top], l_sem.at[1]),
             local(wo_in, wbuf.at[2], l_sem.at[2])]
    stores = [local(wbuf.at[0, top], wg.at[core, rows], l_sem.at[0]), local(wbuf.at[1, top], wi.at[core, rows], l_sem.at[1]),
              local(wbuf.at[2], wo.at[core], l_sem.at[2])]
    for n, (arr, kind) in enumerate(((x, 0), (g, 2))):
        for i in range(CHUNKS):
            spot = ab.at[n, pl.ds(i * ROWS, ROWS)]
            loads.append(local(my_rows(arr, i), spot, t_sem.at[n, i]))
            stores.append(local(spot, shard(kind, i, 0), t_sem.at[n, i]))
    run_all(loads)
    run_all(stores)
    for i in range(2):
        ag_forward(0, i)

    for n in range(4):
        w_pass_on(0, n)
    w_arrived(0)

    def when_task(tick, first, last):
        def run(body):
            @pl.when((tick >= 0) & (tick != TURN) & (tick <= CHAIN))
            def _():
                task = tick - jnp.where(tick > TURN, 1, 0)

                @pl.when((task >= first) & (task < last))
                def _():
                    body(task)
        return run

    def when_g(tick):
        def run(body):
            for at, chunks in G_TICKS:
                @pl.when(tick == at)
                def _(chunks=chunks):
                    for i in chunks:
                        body(i)
        return run

    def tick_step(tick, _):
        @pl.when(tick < 2)
        def _():
            start_all(ag_first(0, tick + 2, my_rows(x, tick + 2)))

        @when_g(tick)
        def _(i):
            start_all(ag_first(2, i, my_rows(g, i)))

        @pl.when(tick < 4)
        def _():
            w_start(1, tick)

        @pl.when(tick == TURN + 1)
        def _():
            w_arrived(1)

        @when_task(tick, 0, CHAIN)
        def _(task):
            @pl.when(task % CHUNKS == 0)
            def _():
                block = (task // CHUNKS) % 2
                run_all([local(src.at[block], wbuf.at[n], l_sem.at[n]) for n, src in enumerate((wg, wi, wo))])

        when_task(tick, 0, CHUNKS)(forward)
        when_task(tick, CHUNKS, CHAIN)(backward)

        @pl.when(tick > CHAIN)
        def _():
            grad_tile(tick - CHAIN - 1)

        @pl.when((tick > CHAIN + SLOTS) & (tick <= CHAIN + SLOTS + TILES))
        def _():
            out_tile(tick - CHAIN - SLOTS - 1)

        @pl.when(tick < 2)
        def _():
            ag_forward(0, tick + 2)

        @when_task(tick - 3, 0, 2 * CHUNKS)
        def _(task):
            ag_forward(2 * (task // CHUNKS) + 1, task % CHUNKS)

        when_task(tick - 2, 0, CHAIN)(rs_last)
        when_task(tick - 1, 0, CHAIN)(rs_middle)

        @when_g(tick)
        def _(i):
            ag_forward(2, i)

        @pl.when((tick >= 1) & (tick < 5))
        def _():
            w_pass_on(1, tick - 1)
        when_task(tick, 0, CHUNKS)(forward_out)
        when_task(tick, CHUNKS, CHAIN)(backward_out)
        return 0

    lax.fori_loop(0, CHAIN + 1 + SENT_TILES, tick_step, 0)

    for n, dst in enumerate((dwg, dwi)):
        for k, came in enumerate(near):
            block = dst.at[:, pl.ds(came * WIDTH, WIDTH - n * LATE_TILES * TILE)]
            local(block, block, gr_recv.at[n, k]).wait()
    for slot in range(SLOTS):
        grad_sent(slot)
    for slot in range(2):
        out_store(0, 0, slot).wait()
    for i in range(CHUNKS):
        dx_copies(i, 0)[1].wait_recv()
    dx_sent(2)
    dx_sent(3)

    def drain_gathers(n, _):
        kind, i = n // CHUNKS, n % CHUNKS
        for copy in ag_first(kind, i, shard(kind, i, 0)) + ag_second(kind, i):
            copy.wait_send()
        return 0

    def drain_sums(task, _):
        for copy in rs_first(task):
            copy.wait_send()
        return 0

    lax.fori_loop(0, 4 * CHUNKS, drain_gathers, 0)
    lax.fori_loop(0, CHAIN, drain_sums, 0)
    for task in (CHAIN - 2, CHAIN - 1):
        for copy in rs_second(task):
            copy.wait_send()
    for block in range(2):
        for n in range(4):
            for copy in w_copies(0, block, n) + w_forwards(0, block, n):
                copy.wait_send()
    for copy in w_twin(core) + (w_hand(0),):
        copy.wait_send()


def settle_kernel(*refs):
    for src, dst in zip(refs[:len(refs) // 2], refs[len(refs) // 2:]):
        dst[...] = src[...]


def settle(arrays, steps=16):
    specs = [pl.BlockSpec((arr.shape[0] // steps, arr.shape[1]), lambda i: (i, 0)) for arr in arrays]
    size = sum(arr.size * arr.dtype.itemsize for arr in arrays)
    return pl.pallas_call(
        settle_kernel, grid=(steps,), out_shape=[jax.ShapeDtypeStruct(arr.shape, arr.dtype) for arr in arrays], in_specs=specs, out_specs=specs,
        name='settle', cost_estimate=pl.CostEstimate(flops=SETTLE_FLOPS, bytes_accessed=2 * size, transcendentals=0),
        compiler_params=pltpu.CompilerParams(vmem_limit_bytes=67_043_328),
    )(*arrays)


def insert_kernel(late, whole, out):
    out[...] = late[0]


def insert_late(whole, late):
    chips, rows, cols = late.shape
    step = rows
    return pl.pallas_call(
        insert_kernel, grid=(chips, 1), out_shape=jax.ShapeDtypeStruct(whole.shape, whole.dtype),
        in_specs=[pl.BlockSpec((1, step, cols), lambda c, r: (c, r, 0)), pl.BlockSpec(memory_space=pl.ANY)],
        out_specs=pl.BlockSpec((step, cols), lambda c, r: (r, (c + 1) * (WIDTH // cols) - 1)), input_output_aliases={1: 0}, name='insert_late',
    )(late, whole)


def solution(mesh):
    act_spec = P(None, 'data', None, None)
    weight_spec = P('stage', None, 'data', None)

    def per_device(x, g, w_gate, w_in, w_out):
        flat = (CHUNKS, 2 * ROWS, WIDTH)
        dma = pltpu.SemaphoreType.DMA
        any_space = pl.BlockSpec(memory_space=pl.ANY)

        def arr(*shape, dtype=BF16):
            return jax.ShapeDtypeStruct(shape, dtype)

        out_shapes = [
            arr(*flat), arr(QUARTER, 4 * WIDTH, dtype=F32), arr(QUARTER, 4 * WIDTH, dtype=F32), arr(WIDTH, WIDTH, dtype=F32), arr(4, QUARTER, LATE_TILES * TILE, dtype=F32),
            arr(4, CHUNKS, BLOCK_ROWS, WIDTH), arr(2, WIDTH, WIDTH), arr(2, WIDTH, WIDTH), arr(2, WIDTH, WIDTH), arr(QUARTER, 4 * WIDTH),
            arr(CHAIN, 2, 2, ROWS, WIDTH, dtype=F32),
            arr(CHAIN, 2, ROWS, HALF, dtype=F32), arr(CHAIN, 2, ROWS, HALF, dtype=F32),
            arr(CHAIN, ROWS, HALF, dtype=F32), arr(CHAIN, ROWS, HALF, dtype=F32),
            arr(2, 2, WIDTH, WIDTH), arr(3, 2, WIDTH, WIDTH),
        ]
        scratch = [
            pltpu.VMEM((3, WIDTH, WIDTH), BF16), pltpu.VMEM((2, BLOCK_ROWS, WIDTH), BF16), pltpu.VMEM((2, WIDTH, BLOCK_ROWS), BF16),
            pltpu.VMEM((BLOCK_ROWS, WIDTH), BF16), pltpu.VMEM((BLOCK_ROWS, WIDTH), BF16),
            pltpu.VMEM((2, 2, 2, ROWS, TILE), F32), pltpu.VMEM((2, ROWS, WIDTH), F32), pltpu.VMEM((2, 2, ROWS, HALF), F32),
            pltpu.VMEM((2, 2, ROWS, HALF), F32), pltpu.VMEM((ROWS, WIDTH), F32), pltpu.VMEM((2, ROWS, WIDTH), BF16),
            pltpu.VMEM((2, ROWS, WIDTH), BF16), pltpu.VMEM((SLOTS, WIDTH, TILE), F32),
            pltpu.VMEM((2, QUARTER, TILE), F32),
            dma((4, CHUNKS, 4)), dma((4, CHUNKS, 4)), dma((CHAIN, 4)), dma((CHAIN, 4)),
            dma((2, 4, 3)), dma((2, 4, 3)), dma((2, 4, 3)), dma((2, 4, 3)), dma((4,)), dma((4,)),
            dma((5,)), dma((CHUNKS, 5)), dma((CHUNKS, 2)), dma((CHUNKS,)), dma((SLOTS, 4)), dma((2, 3)),
            dma((2,)), dma((4,)), dma((2, 4)), dma((2, 3)),
        ]
        results = pl.pallas_call(
            step_kernel, out_shape=out_shapes, in_specs=[any_space] * 5, out_specs=[any_space] * len(out_shapes),
            scratch_shapes=scratch, name='mlp_step',
            compiler_params=pltpu.CompilerParams(collective_id=0, has_side_effects=True, vmem_limit_bytes=67_043_328),
        )(x.reshape(flat), g.reshape(flat), w_gate[0, 0], w_in[0, 0], w_out[0, 0])
        dx, d_gate, d_in, d_out, late = results[:5]
        late = lax.all_to_all(late, 'data', 0, 0)
        dx, d_gate, d_in, d_out = settle((dx.reshape(-1, WIDTH), d_gate, d_in, d_out))
        d_in = insert_late(d_in, late)
        return dx.reshape(x.shape), d_gate[None, None], d_in[None, None], d_out[None, None]

    return jax.shard_map(per_device, mesh=mesh, in_specs=(act_spec, act_spec, weight_spec, weight_spec, weight_spec),
                         out_specs=(act_spec, weight_spec, weight_spec, weight_spec), check_vma=False)
```

```python
import jax
import jax.numpy as jnp
from jax import lax
from jax.experimental import pallas as pl
from jax.experimental.pallas import tpu as pltpu
from jax.sharding import PartitionSpec as P

MESH = pl.DeviceIdType.MESH
F32 = jnp.float32
BF16 = jnp.bfloat16
EPS = 1e-6

CHUNKS = 4
ROWS = 128
BLOCK_ROWS = 4 * ROWS
WIDTH = 2048
HALF = WIDTH // 2
QUARTER = WIDTH // 4
TILE = 256
TILES = WIDTH // TILE
CHAIN = 3 * CHUNKS
TURN = CHUNKS
G_TICKS = ((2, (0,)), (3, (1,)), (TURN + 1, (2, 3)))
SENT_TILES = 2 * TILES
LATE_TILES = 2
SETTLE_FLOPS = 2 ** 30
SLOTS = 4
LO, HI = pl.ds(0, HALF), pl.ds(HALF, HALF)


def mm(lhs, rhs, rhs_dim):
    return lax.dot_general(lhs, rhs, (((1,), (rhs_dim,)), ((), ())), preferred_element_type=F32)


def repeat(count, body):
    def step(n, carry):
        body(n)
        return carry

    lax.fori_loop(0, count, step, 0)


def start_all(copies):
    for copy in copies:
        copy.start()


def run_all(copies):
    start_all(copies)
    for copy in copies:
        copy.wait()


def step_kernel(x, g, wg_in, wi_in, wo_in,
                dx, dwg, dwi, dwo, late_far, late_x, late_y, late_own, act, wg, wi, wo, wx, part, ra1, rb1, ra2, rb2, lhs, rhs,
                wbuf, ab, tb, dab, dbb, pst, keep, snd, ld, r2, own, new, outs, wo_out,
                ag_send, ag_recv, rs_send, rs_recv, w_send, w_recv, f_send, f_recv, d_send, d_recv,
                op_send, op_recv, dx_send, dx_recv, gr_send, gr_recv, p_sem, l_sem, t_sem, o_sem):
    chip = lax.axis_index('data')
    core = lax.axis_index('stage')
    cx, cy = chip % 2, chip // 2
    near = (cy * 2 + (1 - cx), (1 - cy) * 2 + cx, (1 - cy) * 2 + (1 - cx))
    far_first = (near[2], near[0], near[1])
    other = 1 - core
    x_dev, y_dev, twin = (near[0], core), (near[1], core), (chip, other)

    def local(src, dst, sem):
        return pltpu.make_async_copy(src, dst, sem)

    def remote(src, dst, send, recv, dev):
        return pltpu.make_async_remote_copy(src_ref=src, dst_ref=dst, send_sem=send, recv_sem=recv, device_id=dev, device_id_type=MESH)

    def shard(kind, i, n, cols=slice(None)):
        return act.at[kind, i, pl.ds(n * ROWS, ROWS), cols]

    def ag_first(kind, i, src):
        return (remote(src, shard(kind, i, 2), ag_send.at[kind, i, 0], ag_recv.at[kind, i, 0], x_dev),
                remote(src, shard(kind, i, 1), ag_send.at[kind, i, 1], ag_recv.at[kind, i, 1], y_dev))

    def ag_second(kind, i):
        return (remote(shard(kind, i, 1, LO), shard(kind, i, 3, LO), ag_send.at[kind, i, 2], ag_recv.at[kind, i, 2], x_dev),
                remote(shard(kind, i, 2, HI), shard(kind, i, 3, HI), ag_send.at[kind, i, 3], ag_recv.at[kind, i, 3], y_dev))

    def ag_forward(kind, i):
        for copy in ag_first(kind, i, shard(kind, i, 0)):
            copy.wait_recv()
        start_all(ag_second(kind, i))

    def ag_arrived(kind, i):
        for copy in ag_second(kind, i):
            copy.wait_recv()

    def rs_first(task):
        return (remote(part.at[task, 1, :, :, LO], ra1.at[task], rs_send.at[task, 0], rs_recv.at[task, 0], x_dev),
                remote(part.at[task, :, 1, :, HI], rb1.at[task], rs_send.at[task, 1], rs_recv.at[task, 1], y_dev))

    def rs_second(task):
        slot = task % 2
        return (remote(snd.at[slot, 0], ra2.at[task], rs_send.at[task, 2], rs_recv.at[task, 2], y_dev),
                remote(snd.at[slot, 1], rb2.at[task], rs_send.at[task, 3], rs_recv.at[task, 3], x_dev))

    def rs_middle(task):
        slot = task % 2

        @pl.when(task >= 2)
        def _():
            for copy in rs_second(task - 2):
                copy.wait_send()

        mine = (part.at[task, 0, :, :, LO], part.at[task, :, 0, :, HI])
        for side, (came, received) in enumerate(zip((ra1, rb1), rs_first(task))):
            received.wait_recv()
            run_all((local(mine[side], ld.at[0], l_sem.at[0]), local(came.at[task], ld.at[1], l_sem.at[1])))
            snd[slot, side] = ld[0, 1] + ld[1, 1]
            keep[slot, :, pl.ds(side * HALF, HALF)] = ld[0, 0] + ld[1, 0]
            rs_second(task)[side].start()

    def dx_copies(i, slot):
        dst = dx.at[i, pl.ds(core * ROWS, ROWS)]
        return (local(new.at[slot], dst, dx_send.at[i, 0]), remote(new.at[slot], dst, dx_send.at[i, 1], dx_recv.at[i], twin))

    def dx_sent(i):
        stored, sent = dx_copies(i, i % 2)
        stored.wait()
        sent.wait_send()

    def rs_last(task):
        slot, kind, i = task % 2, task // CHUNKS, task % CHUNKS
        for copy in rs_second(task):
            copy.wait_recv()
        run_all((local(ra2.at[task], r2.at[:, LO], l_sem.at[0]), local(rb2.at[task], r2.at[:, HI], l_sem.at[1]),
                 local(shard((3 * kind + 1) // 2, i, 0), own.at[0], l_sem.at[2]), local(shard(kind % 2, i, 0), own.at[1], l_sem.at[3])))

        @pl.when(task >= 2 * CHUNKS + 2)
        def _():
            dx_sent(i - 2)

        def rows_step(r):
            rows = pl.ds(r * 32, 32)
            total = keep[slot, rows, :] + r2[rows, :]

            @pl.when(kind == 0)
            def _():
                new[slot, rows, :] = own[0, rows, :] + total.astype(BF16)

            @pl.when(kind > 0)
            def _():
                tok = own[1, rows, :].astype(F32)
                inv = lax.rsqrt(jnp.mean(tok * tok, axis=-1, keepdims=True) + EPS)
                dot = jnp.mean(tok * total, axis=-1, keepdims=True)
                resid = total * inv - tok * (inv * inv * inv * dot)
                new[slot, rows, :] = (own[0, rows, :].astype(F32) + resid).astype(BF16)

        repeat(ROWS // 32, rows_step)

        @pl.when(kind < 2)
        def _():
            mine = shard(2 * kind + 1, i, 0)
            run_all((local(new.at[slot], mine, l_sem.at[0]),))
            start_all(ag_first(2 * kind + 1, i, mine))

        @pl.when(kind == 2)
        def _():
            start_all(dx_copies(i, slot))

    def w_copies(mtx, block, n):
        src, dst = ((wg_in, wx), (wx, wi_in))[mtx][block], (wg, wi)[mtx]
        rows = pl.ds(chip * QUARTER + n * ROWS, ROWS)
        return [remote(src.at[pl.ds(n * ROWS, ROWS), pl.ds(to * WIDTH, WIDTH)], dst.at[block, rows],
                       w_send.at[block, n, k], w_recv.at[block, n, k], (to, core)) for k, to in enumerate(far_first)]

    def w_forwards(mtx, block, n):
        pieces = [(wg, wi)[mtx].at[block, pl.ds(came * QUARTER + n * ROWS, ROWS)] for came in far_first]
        return [remote(piece, piece, f_send.at[block, n, k], f_recv.at[block, n, k], twin) for k, piece in enumerate(pieces)]

    def w_start(block, n):
        for mtx in range(2):
            @pl.when(core == mtx)
            def _(mtx=mtx):
                start_all(w_copies(mtx, block, n))

    def w_pass_on(block, n):
        for mtx in range(2):
            @pl.when(core == mtx)
            def _(mtx=mtx):
                for came, onward in zip(w_copies(mtx, block, n), w_forwards(mtx, block, n)):
                    came.wait_recv()
                    onward.start()

    def w_hand(mtx):
        return remote((wg_in, wi_in)[mtx], wx, d_send.at[3], d_recv.at[3], twin)

    def w_twin(block):
        rows, cols = pl.ds(chip * QUARTER, QUARTER), pl.ds(chip * WIDTH, WIDTH)
        return (remote(wg_in.at[:, cols], wg.at[block, rows], d_send.at[0], d_recv.at[0], twin),
                remote(wi_in.at[:, cols], wi.at[block, rows], d_send.at[1], d_recv.at[1], twin),
                remote(wo_in, wo.at[block], d_send.at[2], d_recv.at[2], twin))

    def w_arrived(block):
        for n in range(QUARTER // ROWS):
            for copy in w_forwards(0, block, n):
                copy.wait_recv()

        @pl.when(core != block)
        def _():
            for copy in w_twin(block):
                copy.wait_recv()

    def op_pairs(i, src):
        rows = pl.ds(i * BLOCK_ROWS, BLOCK_ROWS)
        return ((tb.at[0], lhs.at[0, src, :, rows]), (tb.at[1], lhs.at[1, src, :, rows]), (dab, rhs.at[0, src, rows]),
                (dbb, rhs.at[1, src, rows]), (ab.at[1], rhs.at[2, src, rows]))

    def op_start(n, i, block):
        src, dst = op_pairs(i, core)[n]

        @pl.when(block == core)
        def _():
            local(src, dst, op_send.at[n]).start()

        @pl.when(block != core)
        def _():
            remote(src, dst, op_send.at[n], op_recv.at[i, n], twin).start()

    def op_sent(i):
        for n, (src, dst) in enumerate(op_pairs(i, core)):
            local(src, dst, op_send.at[n]).wait()

    def op_arrived(i):
        for n, (src, dst) in enumerate(op_pairs(i, other)):
            remote(src, dst, op_send.at[n], op_recv.at[i, n], twin).wait_recv()

    def normalize():
        def rows_step(r):
            rows = pl.ds(r * 64, 64)
            tok = ab[0, rows, :].astype(F32)
            inv = lax.rsqrt(jnp.mean(tok * tok, axis=-1, keepdims=True) + EPS)
            ab[0, rows, :] = (tok * inv).astype(BF16)

        repeat(BLOCK_ROWS // 64, rows_step)

    def write_partials(task, product):
        def tile_copy(n, slot):
            return local(pst.at[slot], part.at[task, :, :, :, pl.ds(n * TILE, TILE)], p_sem.at[slot])

        def half_step(side):
            def tile_step(t):
                n, slot = side * (TILES // 2) + t, t % 2

                @pl.when(t >= 2)
                def _():
                    tile_copy(n - 2, slot).wait()

                pst[slot] = product(pl.ds(n * TILE, TILE)).reshape(2, 2, ROWS, TILE)
                tile_copy(n, slot).start()

            repeat(TILES // 2, tile_step)
            last = (side + 1) * (TILES // 2)
            tile_copy(last - 2, 0).wait()
            tile_copy(last - 1, 1).wait()
            for n in range(2):
                @pl.when(side == n)
                def _(n=n):
                    rs_first(task)[n].start()

        repeat(2, half_step)

    def forward(task):
        ag_arrived(0, task)
        run_all((local(act.at[0, task], ab.at[0], l_sem.at[0]),))
        normalize()

        def tile_step(t):
            cols = pl.ds(t * TILE, TILE)
            pre_gate = mm(ab[0], wbuf[0, :, cols], 0)
            pre_in = mm(ab[0], wbuf[1, :, cols], 0)
            dab[:, cols] = (pre_gate * jax.nn.sigmoid(pre_gate) * pre_in).astype(BF16)

        repeat(TILES, tile_step)

    def forward_out(task):
        write_partials(task, lambda cols: mm(dab[...], wbuf[2, :, cols], 0))

    def backward(task):
        kind, i = task // CHUNKS, task % CHUNKS
        block = 2 - kind

        @pl.when(task > CHUNKS)
        def _():
            op_sent(i)

        @pl.when(kind == 1)
        def _():
            ag_arrived(1, i)
            ag_arrived(2, i)

        @pl.when(kind == 2)
        def _():
            ag_arrived(3, i)

        run_all((local(act.at[2 - kind, i], ab.at[0], l_sem.at[0]), local(act.at[kind + 1, i], ab.at[1], l_sem.at[1])))
        op_start(4, i, block)
        normalize()

        def turn_step(t):
            cols = pl.ds(t * TILE, TILE)
            tb[0, cols, :] = ab[0, :, cols].T

        repeat(TILES, turn_step)
        op_start(0, i, block)

        def tile_step(t):
            cols = pl.ds(t * TILE, TILE)
            pre_gate = mm(ab[0], wbuf[0, :, cols], 0)
            pre_in = mm(ab[0], wbuf[1, :, cols], 0)
            d_hidden = mm(ab[1], wbuf[2, cols, :], 1)
            sigma = jax.nn.sigmoid(pre_gate)
            gate_act = pre_gate * sigma
            tb[1, cols, :] = (gate_act * pre_in).astype(BF16).T
            dab[:, cols] = (d_hidden * pre_in * sigma * (1.0 + pre_gate * (1.0 - sigma))).astype(BF16)
            dbb[:, cols] = (d_hidden * gate_act).astype(BF16)

        repeat(TILES, tile_step)
        for n in (1, 2, 3):
            op_start(n, i, block)

    def backward_out(task):
        write_partials(task, lambda rows: mm(dab[...], wbuf[0, rows, :], 1) + mm(dbb[...], wbuf[1, rows, :], 1))

    def rhs_copies(mtx, n, slot):
        return [local(rhs.at[mtx, q, :, pl.ds(n * TILE, TILE)], tb.at[slot, :, pl.ds(q * TILE, TILE)], t_sem.at[slot, q]) for q in range(2)]

    def grad_sent(slot):
        for k in range(4):
            local(outs.at[slot, pl.ds(0, QUARTER)], dwo.at[pl.ds(0, QUARTER), pl.ds(0, TILE)], gr_send.at[slot, k]).wait()

    def grad_tile(t):
        mtx, slot = t // TILES, t % SLOTS
        col = (t % TILES) * TILE

        @pl.when(t == 0)
        def _():
            op_sent(0)
            for i in range(CHUNKS):
                op_arrived(i)
            start_all(rhs_copies(0, 0, 0))
            run_all([local(lhs.at[0, q], wbuf.at[q], l_sem.at[q]) for q in range(2)])

        for copy in rhs_copies(mtx, t % TILES, 0):
            copy.wait()

        @pl.when(t >= SLOTS)
        def _():
            grad_sent(slot)

        def quarter_step(k):
            ax, ay = 1 - k // 2, 1 - k % 2
            to = (cy + ay - 2 * cy * ay) * 2 + (cx + ax - 2 * cx * ax)
            rows = pl.ds(to * QUARTER, QUARTER)
            outs[slot, rows, :] = mm(wbuf[0, rows, :], tb[0, :, 0:TILE], 0) + mm(wbuf[1, rows, :], tb[0, :, TILE:2 * TILE], 0)
            cols = pl.ds(chip * WIDTH + col, TILE)
            for n, dst in enumerate((dwg, dwi)):
                @pl.when((mtx == n) & (k < 3) & (t < SENT_TILES - LATE_TILES))
                def _(n=n, dst=dst):
                    remote(outs.at[slot, rows], dst.at[:, cols], gr_send.at[slot, k], gr_recv.at[n, k], (to, core)).start()

                @pl.when((mtx == n) & (k == 3) & (t < SENT_TILES - LATE_TILES))
                def _(dst=dst):
                    local(outs.at[slot, rows], dst.at[:, cols], gr_send.at[slot, k]).start()

            @pl.when(t >= SENT_TILES - LATE_TILES)
            def _():
                cols = pl.ds((t - SENT_TILES + LATE_TILES) * TILE, TILE)
                for n, late in enumerate((late_far, late_x, late_y, late_own)):
                    @pl.when(k == n)
                    def _(late=late):
                        local(outs.at[slot, rows], late.at[:, cols], gr_send.at[slot, k]).start()

        repeat(4, quarter_step)

        @pl.when(t + 1 < SENT_TILES)
        def _():
            start_all(rhs_copies((t + 1) // TILES, (t + 1) % TILES, 0))

    def out_loads(k, slot):
        return [local(lhs.at[1, q, pl.ds(k * QUARTER, QUARTER)], wbuf.at[2, pl.ds(slot * HALF + q * QUARTER, QUARTER)], o_sem.at[slot, q]) for q in range(2)]

    def out_store(n, k, slot):
        return local(wo_out.at[slot], dwo.at[pl.ds(k * QUARTER, QUARTER), pl.ds(n * TILE, TILE)], o_sem.at[slot, 2])

    def out_tile(n):
        start_all(rhs_copies(2, n, 1))
        start_all(out_loads(0, 0))
        for copy in rhs_copies(2, n, 1):
            copy.wait()

        def quarter_step(k):
            slot = k % 2

            @pl.when(k < 3)
            def _():
                start_all(out_loads(k + 1, 1 - slot))

            for copy in out_loads(k, slot):
                copy.wait()

            @pl.when(4 * n + k >= 2)
            def _():
                out_store(n, k, slot).wait()

            top, low = pl.ds(slot * HALF, QUARTER), pl.ds(slot * HALF + QUARTER, QUARTER)
            wo_out[slot] = mm(wbuf[2, top, :], tb[1, :, 0:TILE], 0) + mm(wbuf[2, low, :], tb[1, :, TILE:2 * TILE], 0)
            out_store(n, k, slot).start()

        repeat(4, quarter_step)

    barrier = pltpu.get_barrier_semaphore()
    for dev in [(to, core) for to in near] + [twin]:
        pl.semaphore_signal(barrier, inc=1, device_id=dev, device_id_type=MESH)
    pl.semaphore_wait(barrier, 4)

    def my_rows(arr, i):
        return arr.at[i, pl.ds(core * ROWS, ROWS)]

    for i in range(2):
        start_all(ag_first(0, i, my_rows(x, i)))

    @pl.when(core == 0)
    def _():
        w_hand(1).start()
        for n in range(4):
            start_all(w_copies(0, 0, n))

    @pl.when(core == 1)
    def _():
        w_hand(0).start()

    w_hand(0).wait_recv()

    @pl.when(core == 1)
    def _():
        for n in range(4):
            start_all(w_copies(1, 0, n))

    start_all(w_twin(core))
    rows, cols = pl.ds(chip * QUARTER, QUARTER), pl.ds(chip * WIDTH, WIDTH)
    top = pl.ds(0, QUARTER)
    loads = [local(wg_in.at[:, cols], wbuf.at[0, top], l_sem.at[0]), local(wi_in.at[:, cols], wbuf.at[1, top], l_sem.at[1]),
             local(wo_in, wbuf.at[2], l_sem.at[2])]
    stores = [local(wbuf.at[0, top], wg.at[core, rows], l_sem.at[0]), local(wbuf.at[1, top], wi.at[core, rows], l_sem.at[1]),
              local(wbuf.at[2], wo.at[core], l_sem.at[2])]
    for n, (arr, kind) in enumerate(((x, 0), (g, 2))):
        for i in range(CHUNKS):
            spot = ab.at[n, pl.ds(i * ROWS, ROWS)]
            loads.append(local(my_rows(arr, i), spot, t_sem.at[n, i]))
            stores.append(local(spot, shard(kind, i, 0), t_sem.at[n, i]))
    run_all(loads)
    run_all(stores)
    for i in range(2):
        ag_forward(0, i)

    for n in range(4):
        w_pass_on(0, n)
    w_arrived(0)

    def when_task(tick, first, last):
        def run(body):
            @pl.when((tick >= 0) & (tick != TURN) & (tick <= CHAIN))
            def _():
                task = tick - jnp.where(tick > TURN, 1, 0)

                @pl.when((task >= first) & (task < last))
                def _():
                    body(task)
        return run

    def when_g(tick):
        def run(body):
            for at, chunks in G_TICKS:
                @pl.when(tick == at)
                def _(chunks=chunks):
                    for i in chunks:
                        body(i)
        return run

    def tick_step(tick):
        @pl.when(tick < 2)
        def _():
            start_all(ag_first(0, tick + 2, my_rows(x, tick + 2)))

        @when_g(tick)
        def _(i):
            start_all(ag_first(2, i, my_rows(g, i)))

        @pl.when(tick < 4)
        def _():
            w_start(1, tick)

        @pl.when(tick == TURN + 1)
        def _():
            w_arrived(1)

        @when_task(tick, 0, CHAIN)
        def _(task):
            @pl.when(task % CHUNKS == 0)
            def _():
                block = (task // CHUNKS) % 2
                run_all([local(src.at[block], wbuf.at[n], l_sem.at[n]) for n, src in enumerate((wg, wi, wo))])

        when_task(tick, 0, CHUNKS)(forward)
        when_task(tick, CHUNKS, CHAIN)(backward)

        @pl.when(tick > CHAIN)
        def _():
            grad_tile(tick - CHAIN - 1)

        @pl.when((tick > CHAIN + SLOTS) & (tick <= CHAIN + SLOTS + TILES))
        def _():
            out_tile(tick - CHAIN - SLOTS - 1)

        @pl.when(tick < 2)
        def _():
            ag_forward(0, tick + 2)

        @when_task(tick - 3, 0, 2 * CHUNKS)
        def _(task):
            ag_forward(2 * (task // CHUNKS) + 1, task % CHUNKS)

        when_task(tick - 2, 0, CHAIN)(rs_last)
        when_task(tick - 1, 0, CHAIN)(rs_middle)

        @when_g(tick)
        def _(i):
            ag_forward(2, i)

        @pl.when((tick >= 1) & (tick < 5))
        def _():
            w_pass_on(1, tick - 1)
        when_task(tick, 0, CHUNKS)(forward_out)
        when_task(tick, CHUNKS, CHAIN)(backward_out)

    repeat(CHAIN + 1 + SENT_TILES, tick_step)

    for n, dst in enumerate((dwg, dwi)):
        for k, came in enumerate((near[2], near[0], near[1])):
            block = dst.at[:, pl.ds(came * WIDTH, WIDTH - n * LATE_TILES * TILE)]
            local(block, block, gr_recv.at[n, k]).wait()
    for slot in range(SLOTS):
        grad_sent(slot)
    for slot in range(2):
        out_store(0, 0, slot).wait()
    for i in range(CHUNKS):
        dx_copies(i, 0)[1].wait_recv()
    dx_sent(2)
    dx_sent(3)

    def drain_gathers(n):
        kind, i = n // CHUNKS, n % CHUNKS
        for copy in ag_first(kind, i, shard(kind, i, 0)) + ag_second(kind, i):
            copy.wait_send()

    def drain_sums(task):
        for copy in rs_first(task):
            copy.wait_send()

    repeat(4 * CHUNKS, drain_gathers)
    repeat(CHAIN, drain_sums)
    for task in (CHAIN - 2, CHAIN - 1):
        for copy in rs_second(task):
            copy.wait_send()
    for block in range(2):
        for n in range(4):
            for copy in w_copies(0, block, n) + w_forwards(0, block, n):
                copy.wait_send()
    for copy in w_twin(core) + (w_hand(0),):
        copy.wait_send()


def settle_kernel(*refs):
    for src, dst in zip(refs[:len(refs) // 2], refs[len(refs) // 2:]):
        dst[...] = src[...]


def settle(arrays, steps=16):
    specs = [pl.BlockSpec((arr.shape[0] // steps, arr.shape[1]), lambda i: (i, 0)) for arr in arrays]
    size = sum(arr.size * arr.dtype.itemsize for arr in arrays)
    return pl.pallas_call(
        settle_kernel, grid=(steps,), out_shape=[jax.ShapeDtypeStruct(arr.shape, arr.dtype) for arr in arrays], in_specs=specs, out_specs=specs,
        name='settle', cost_estimate=pl.CostEstimate(flops=SETTLE_FLOPS, bytes_accessed=2 * size, transcendentals=0),
        compiler_params=pltpu.CompilerParams(vmem_limit_bytes=67_043_328),
    )(*arrays)


def insert_kernel(spots, far, x_side, y_side, here, whole, out):
    for k, late in enumerate((far, x_side, y_side, here)):
        @pl.when(pl.program_id(0) == k)
        def _(late=late):
            out[...] = late[...]


def insert_late(whole, late, spots):
    rows, cols = late[0].shape
    return pl.pallas_call(
        insert_kernel, out_shape=jax.ShapeDtypeStruct(whole.shape, whole.dtype),
        grid_spec=pltpu.PrefetchScalarGridSpec(
            num_scalar_prefetch=1, grid=(4,), in_specs=[pl.BlockSpec((rows, cols), lambda k, spots: (0, 0))] * 4 + [pl.BlockSpec(memory_space=pl.ANY)],
            out_specs=pl.BlockSpec((rows, cols), lambda k, spots: (0, (spots[k] + 1) * (WIDTH // cols) - 1))),
        input_output_aliases={5: 0}, name='insert_late',
    )(spots, *late, whole)


def solution(mesh):
    act_spec = P(None, 'data', None, None)
    weight_spec = P('stage', None, 'data', None)

    def per_device(x, g, w_gate, w_in, w_out):
        flat = (CHUNKS, 2 * ROWS, WIDTH)
        dma = pltpu.SemaphoreType.DMA
        any_space = pl.BlockSpec(memory_space=pl.ANY)

        def arr(*shape, dtype=BF16):
            return jax.ShapeDtypeStruct(shape, dtype)

        out_shapes = [
            arr(*flat), arr(QUARTER, 4 * WIDTH, dtype=F32), arr(QUARTER, 4 * WIDTH, dtype=F32), arr(WIDTH, WIDTH, dtype=F32), *[arr(QUARTER, LATE_TILES * TILE, dtype=F32)] * 4,
            arr(4, CHUNKS, BLOCK_ROWS, WIDTH), arr(2, WIDTH, WIDTH), arr(2, WIDTH, WIDTH), arr(2, WIDTH, WIDTH), arr(QUARTER, 4 * WIDTH),
            arr(CHAIN, 2, 2, ROWS, WIDTH, dtype=F32),
            arr(CHAIN, 2, ROWS, HALF, dtype=F32), arr(CHAIN, 2, ROWS, HALF, dtype=F32),
            arr(CHAIN, ROWS, HALF, dtype=F32), arr(CHAIN, ROWS, HALF, dtype=F32),
            arr(2, 2, WIDTH, WIDTH), arr(3, 2, WIDTH, WIDTH),
        ]
        scratch = [
            pltpu.VMEM((3, WIDTH, WIDTH), BF16), pltpu.VMEM((2, BLOCK_ROWS, WIDTH), BF16), pltpu.VMEM((2, WIDTH, BLOCK_ROWS), BF16),
            pltpu.VMEM((BLOCK_ROWS, WIDTH), BF16), pltpu.VMEM((BLOCK_ROWS, WIDTH), BF16),
            pltpu.VMEM((2, 2, 2, ROWS, TILE), F32), pltpu.VMEM((2, ROWS, WIDTH), F32), pltpu.VMEM((2, 2, ROWS, HALF), F32),
            pltpu.VMEM((2, 2, ROWS, HALF), F32), pltpu.VMEM((ROWS, WIDTH), F32), pltpu.VMEM((2, ROWS, WIDTH), BF16),
            pltpu.VMEM((2, ROWS, WIDTH), BF16), pltpu.VMEM((SLOTS, WIDTH, TILE), F32),
            pltpu.VMEM((2, QUARTER, TILE), F32),
            dma((4, CHUNKS, 4)), dma((4, CHUNKS, 4)), dma((CHAIN, 4)), dma((CHAIN, 4)),
            dma((2, 4, 3)), dma((2, 4, 3)), dma((2, 4, 3)), dma((2, 4, 3)), dma((4,)), dma((4,)),
            dma((5,)), dma((CHUNKS, 5)), dma((CHUNKS, 2)), dma((CHUNKS,)), dma((SLOTS, 4)), dma((2, 3)),
            dma((2,)), dma((4,)), dma((2, 4)), dma((2, 3)),
        ]
        results = pl.pallas_call(
            step_kernel, out_shape=out_shapes, in_specs=[any_space] * 5, out_specs=[any_space] * len(out_shapes),
            scratch_shapes=scratch, name='mlp_step',
            compiler_params=pltpu.CompilerParams(collective_id=0, has_side_effects=True, vmem_limit_bytes=67_043_328),
        )(x.reshape(flat), g.reshape(flat), w_gate[0, 0], w_in[0, 0], w_out[0, 0])
        dx, d_gate, d_in, d_out = results[:4]
        chip = lax.axis_index('data')
        hops = (3, 1, 2)
        late = [lax.ppermute(tile, 'data', [(c, c ^ hop) for c in range(4)]) for tile, hop in zip(results[4:7], hops)] + [results[7]]
        spots = jnp.stack([jnp.bitwise_xor(chip, hop) for hop in hops] + [chip]).astype(jnp.int32)
        dx, d_gate, d_in, d_out = settle((dx.reshape(-1, WIDTH), d_gate, d_in, d_out))
        d_in = insert_late(d_in, late, spots)
        return dx.reshape(x.shape), d_gate[None, None], d_in[None, None], d_out[None, None]

    return jax.shard_map(per_device, mesh=mesh, in_specs=(act_spec, act_spec, weight_spec, weight_spec, weight_spec),
                         out_specs=(act_spec, weight_spec, weight_spec, weight_spec), check_vma=False)
```

```python
import jax
import jax.numpy as jnp
from jax import lax
from jax.experimental import pallas as pl
from jax.experimental.pallas import tpu as pltpu
from jax.sharding import PartitionSpec as P

MESH = pl.DeviceIdType.MESH
F32 = jnp.float32
BF16 = jnp.bfloat16
EPS = 1e-6

CHUNKS = 4
ROWS = 128
BLOCK_ROWS = 4 * ROWS
WIDTH = 2048
HALF = WIDTH // 2
QUARTER = WIDTH // 4
TILE = 256
TILES = WIDTH // TILE
WIDE = 2 * TILE
WIDES = WIDTH // WIDE
PART = BLOCK_ROWS // 2
HIDDEN_TILES = 2 * WIDES
SUM_TILES = HALF // TILE
TASKS = 3 * CHUNKS
BACK_AT = 2 * CHUNKS
GRADS_AT = 4 * CHUNKS
SENT_TILES = 4 * TILES
SLOTS = 4
OUT_AT, OUT_EVERY = 8, 7
LATE_TILES = 6
LAG = 6
W_PASS, W_END = (2, 3), (7, 7)
TAKE_H1, PASS_H1 = 4, 6
PAIR = ZERO, ONE = range(2)
X, H1, G, E1 = range(4)


def mm(lhs, rhs, rhs_dim):
    return lax.dot_general(lhs, rhs, (((1,), (rhs_dim,)), ((), ())), preferred_element_type=F32)


def repeat(count, body):
    def step(n, carry):
        body(n)
        return carry

    lax.fori_loop(0, count, step, 0)


def start_all(copies):
    for copy in copies:
        copy.start()


def wait_all(copies):
    for copy in copies:
        copy.wait()


def run_all(copies):
    start_all(copies)
    wait_all(copies)


def step_kernel(x, g, wg_in, wi_in, wo_in,
                dx, dwg, dwi, dwo, late, act, wg, wi, wo, wx, part, rb, dots, kept, lhs_n, lhs_u, rhs_d, rhs_e,
                wcol, wrow, fab, ab, dd, ntb, utb, utw, pst, ld, tot, own, dsv, new, dxn, ecol, outs, wo_out,
                ag_send, ag_recv, rs_send, rs_recv, dt_send, dt_recv, w_send, w_recv, f_send, f_recv, h_send, h_recv, wo_send, wo_recv,
                op_send, op_recv, dx_send, dx_recv, gr_send, gr_recv, p_sem, l_sem, s_sem, k_sem, b_sem, o_sem, e_sem):
    chip = lax.axis_index('data')
    core = lax.axis_index('stage')
    cx, cy = chip % 2, chip // 2
    other = ONE - core
    x_chip, y_chip = cy * 2 + (ONE - cx), (ONE - cy) * 2 + cx
    twin = (chip, other)
    reds, nons = ((x_chip, core), (y_chip, core)), ((y_chip, core), (x_chip, core))
    rs, cs = (cx, cy), (cy, cx)

    def pick(pair, block):
        return pair[ZERO] + (pair[ONE] - pair[ZERO]) * block

    def red_of(block):
        return pick((x_chip, y_chip), block), core

    def local(src, dst, sem):
        return pltpu.make_async_copy(src, dst, sem)

    def remote(src, dst, send, recv, dev):
        return pltpu.make_async_remote_copy(src_ref=src, dst_ref=dst, send_sem=send, recv_sem=recv, device_id=dev, device_id_type=MESH)

    def arrived(ref, sem):
        local(ref, ref, sem).wait()

    def in_first(kind, i):
        block = kind // G
        mine = act.at[kind, :, :, i, ZERO, ZERO]
        return (remote(mine, act.at[kind, :, :, i, ONE, ZERO], ag_send.at[kind, i, ZERO], ag_recv.at[kind, i, ZERO], reds[block]),
                remote(mine, act.at[kind, :, :, i, ZERO, ONE], ag_send.at[kind, i, ONE], ag_recv.at[kind, i, ONE], nons[block]))

    def in_second(kind, i):
        block = kind // G
        return (remote(act.at[kind, :, :, i, ZERO, ONE], act.at[kind, :, :, i, ONE, ONE], ag_send.at[kind, i, 2], ag_recv.at[kind, i, 2], reds[block]),)

    def out_first(block, i):
        kind, c = (H1, E1)[block], cs[block]
        sends = [remote(act.at[kind, c, :, i, :, ZERO], act.at[kind, c, :, i, :, ONE], ag_send.at[kind, i, ZERO], ag_recv.at[kind, i, ZERO], reds[block])]
        for a in PAIR:
            sends.append(remote(act.at[kind, c, :, i, a, ZERO], act.at[kind, c, :, i, ONE - a, ZERO], ag_send.at[kind, i, ONE + a], ag_recv.at[kind, i, 2 - a], nons[block]))
        return sends

    def out_second(block, i):
        kind, c = (H1, E1)[block], cs[block]
        sends = []
        if block:
            sends.append(remote(act.at[kind, ONE - c, ZERO, i, :, ZERO], act.at[kind, ONE - c, ZERO, i, :, ONE], ag_send.at[kind, i, 3], ag_recv.at[kind, i, 3], reds[block]))
        for a in PAIR:
            for h in range(block, 2):
                sends.append(remote(act.at[kind, c, h, i, a, ONE], act.at[kind, c, h, i, ONE - a, ONE], ag_send.at[kind, i, 4 + 2 * a + h], ag_recv.at[kind, i, 6 - 2 * a + h], nons[block]))
        return sends

    def pass_on(first, second):
        for copy in first:
            copy.wait_recv()
        start_all(second)

    def all_recv(copies):
        for copy in copies:
            copy.wait_recv()

    def rs_copy(task):
        return remote(part.at[task, :, ONE], rb.at[task], rs_send.at[task], rs_recv.at[task], red_of((task // CHUNKS) % 2))

    def dot_copies(task):
        slot, n = task % 2, task - CHUNKS
        dev = pick((y_chip, x_chip), (task // CHUNKS) % 2), core
        return [remote(dsv.at[slot, b], dots.at[n, ONE - b], dt_send.at[n, b], dt_recv.at[n, ONE - b], dev) for b in PAIR]

    def own_half(kind_h, block, i):
        if block == ZERO:
            return act.at[X, cy, :, i, ZERO] if kind_h else act.at[E1, :, cy, i, ZERO]
        return act.at[H1, :, cx, i, ZERO] if kind_h else act.at[G, :, cx, i, ZERO]

    def rest_half(block, i):
        return act.at[X, ONE - cy, :, i, ZERO] if block == ZERO else act.at[H1, :, ONE - cx, i, ZERO]

    def when_kind(task):
        def run(body):
            for kind in range(3):
                @pl.when(task // CHUNKS == kind)
                def _(kind=kind):
                    body(kind)
        return run

    def send_result(block, i, slot):
        run_all([local(new.at[slot], act.at[(H1, E1)[block], cs[block], :, i, :, ZERO], l_sem.at[ZERO])])
        start_all(out_first(block, i))

    def pieces(body):
        def step(n):
            body(n // 4, (n // 2) % 2, pl.ds((n % 2) * (ROWS // 2), ROWS // 2))
        repeat(2 * 4, step)

    def rs_take(task):
        i, slot = task % CHUNKS, task % 2
        rs_copy(task).wait_recv()
        start_all([local(part.at[task, :, ZERO], ld.at[ZERO], l_sem.at[ZERO]), local(rb.at[task], ld.at[ONE], l_sem.at[ONE])])

        @when_kind(task)
        def _(kind):
            local(own_half(True, kind % 2, i), own.at[ZERO], l_sem.at[2]).start()

        wait_all([local(rb.at[task], ld.at[ZERO], l_sem.at[ZERO]), local(rb.at[task], ld.at[ONE], l_sem.at[ONE]), local(own_half(True, ZERO, i), own.at[ZERO], l_sem.at[2])])

        @pl.when(task < CHUNKS)
        def _():
            @pieces
            def _(q, b, rows):
                new[slot, q, b, rows, :] = own[ZERO, q, b, rows, :] + (ld[ZERO, q, b, rows, :] + ld[ONE, q, b, rows, :]).astype(BF16)

            send_result(ZERO, i, slot)

        @pl.when(task >= CHUNKS)
        def _():
            @pl.when(task >= CHUNKS + 2)
            def _():
                for copy in dot_copies(task - 2):
                    copy.wait_send()

            @pieces
            def _(q, b, rows):
                total = ld[ZERO, q, b, rows, :] + ld[ONE, q, b, rows, :]
                tot[slot, q, b, rows, :] = total
                dot = jnp.sum(total * own[ZERO, q, b, rows, :].astype(F32), axis=-ONE, keepdims=True) + jnp.zeros((ONE, ROWS), F32)

                @pl.when(q == ZERO)
                def _():
                    dsv[slot, b, rows, :] = dot

                @pl.when(q == ONE)
                def _():
                    dsv[slot, b, rows, :] = dsv[slot, b, rows, :] + dot

            start_all(dot_copies(task))

    def dx_copies(i, slot):
        spot = dx.at[i, pl.ds(core * ROWS, ROWS), pl.ds(cy * HALF, HALF)]
        return (local(dxn.at[slot, ZERO], spot, dx_send.at[i, ZERO]), remote(dxn.at[slot, ZERO], spot, dx_send.at[i, ONE], dx_recv.at[i, ZERO], twin),
                remote(dxn.at[slot, ONE], spot, dx_send.at[i, 2], dx_recv.at[i, ONE], (y_chip, core)),
                remote(dxn.at[slot, ONE], spot, dx_send.at[i, 3], dx_recv.at[i, 2], (y_chip, other)))

    def dx_sent(i):
        copies = dx_copies(i, i % 2)
        copies[ZERO].wait()
        for copy in copies[ONE:]:
            copy.wait_send()

    def rs_give(task):
        i, slot = task % CHUNKS, task % 2
        for b in PAIR:
            arrived(dots.at[task - CHUNKS, b], dt_recv.at[task - CHUNKS, b])
        local(dots.at[task - CHUNKS], ld.at[ZERO, ZERO, :, :, pl.ds(ZERO, ROWS)], l_sem.at[3]).start()
        for block in PAIR:
            @pl.when((task // CHUNKS) % 2 == block)
            def _(block=block):
                start_all([local(src, own.at[n], l_sem.at[n]) for n, src in enumerate((own_half(True, block, i), own_half(False, block, i), rest_half(block, i)))])
        wait_all([local(own_half(True, ZERO, i), own.at[n], l_sem.at[n]) for n in range(3)])
        local(dots.at[task - CHUNKS], ld.at[ZERO, ZERO, :, :, pl.ds(ZERO, ROWS)], l_sem.at[3]).wait()

        @pl.when(task >= 2 * CHUNKS + 2)
        def _():
            dx_sent(i - 2)

        def step(n):
            b, rows = n // 2, pl.ds((n % 2) * (ROWS // 2), ROWS // 2)

            def sq(slot_of, q):
                vals = own[slot_of, q, b, rows, :].astype(F32)
                return jnp.sum(vals * vals, axis=-ONE, keepdims=True)

            square = sq(ZERO, ZERO) + sq(ZERO, ONE) + sq(2, ZERO) + sq(2, ONE)
            inv = lax.rsqrt(square / WIDTH + EPS)
            dot = (dsv[slot, b, rows, ZERO:ONE] + ld[ZERO, ZERO, b, rows, ZERO:ONE]) / WIDTH
            for q in PAIR:
                tok = own[ZERO, q, b, rows, :].astype(F32)
                resid = tot[slot, q, b, rows, :] * inv - tok * (inv * inv * inv * dot)
                val = (own[ONE, q, b, rows, :].astype(F32) + resid).astype(BF16)
                new[slot, q, b, rows, :] = val
                dxn[slot, b, rows, pl.ds(q * QUARTER, QUARTER)] = val

        repeat(4, step)

        @pl.when(task < 2 * CHUNKS)
        def _():
            send_result(ONE, i, slot)

        @pl.when(task >= 2 * CHUNKS)
        def _():
            start_all(dx_copies(i, slot))

    def f_cols(block, place, fq):
        quarter = place + 2 * fq if block == ZERO else 2 * place + fq
        return pl.ds(quarter * WIDTH, WIDTH)

    def w_src(mtx, block):
        return ((wg_in, wx), (wx, wi_in))[mtx][block]

    def w_rows(mtx, block, fq, of):
        return (wg, wi)[mtx].at[block, fq, pl.ds(of * QUARTER, QUARTER)]

    def w_first(mtx, block, fq):
        src, mine = w_src(mtx, block), w_rows(mtx, block, fq, chip)
        return (remote(src.at[:, f_cols(block, rs[block], fq)], mine, w_send.at[block, fq, ZERO], w_recv.at[block, fq, ZERO], nons[block]),
                remote(src.at[:, f_cols(block, ONE - rs[block], fq)], mine, w_send.at[block, fq, ONE], w_recv.at[block, fq, ONE], reds[block]))

    def w_second(mtx, block, fq):
        piece = w_rows(mtx, block, fq, reds[block][ZERO])
        return remote(piece, piece, w_send.at[block, fq, 2], w_recv.at[block, fq, 2], nons[block])

    def w_twin(mtx, block, fq):
        far = 3 - chip
        srcs = [w_src(mtx, block).at[:, f_cols(block, rs[block], fq)]] + [w_rows(mtx, block, fq, of) for of in (nons[block][ZERO], reds[block][ZERO], far)]
        spots = [w_rows(mtx, block, fq, of) for of in (chip, nons[block][ZERO], reds[block][ZERO], far)]
        return [remote(src, spot, f_send.at[block, fq, n], f_recv.at[block, fq, n], twin) for n, (src, spot) in enumerate(zip(srcs, spots))]

    def per_mtx(body):
        for mtx in PAIR:
            @pl.when(core == mtx)
            def _(mtx=mtx):
                body(mtx)

    def w_start(block, to_red):
        @per_mtx
        def _(mtx):
            for fq in PAIR:
                w_first(mtx, block, fq)[to_red].start()
                if not to_red:
                    w_twin(mtx, block, fq)[ZERO].start()

    def w_pass(block, fq):
        @per_mtx
        def _(mtx):
            first, to_twin = w_first(mtx, block, fq), w_twin(mtx, block, fq)
            first[ONE].wait_recv()
            w_second(mtx, block, fq).start()
            to_twin[2].start()
            first[ZERO].wait_recv()
            to_twin[ONE].start()

    def w_end(block, fq):
        @per_mtx
        def _(mtx):
            w_second(mtx, block, fq).wait_recv()
            w_twin(mtx, block, fq)[3].start()

    def w_arrived(block):
        for fq in PAIR:
            all_recv(w_twin(ZERO, block, fq))

    def w_hand(mtx):
        return remote((wg_in, wi_in)[mtx], wx, h_send.at[ZERO], h_recv.at[ZERO], twin)

    def wo_copies(block, k):
        rows = pl.ds(k * QUARTER, QUARTER)
        spot, got = wo.at[block, cs[block], rows], wo.at[block, ONE - cs[block], rows]
        return (remote(wo_in.at[rows], spot, wo_send.at[block, ZERO, k], wo_recv.at[block, ZERO, k], twin),
                remote(wo_in.at[rows], spot, wo_send.at[block, ONE, k], wo_recv.at[block, ONE, k], nons[block]),
                remote(spot, spot, wo_send.at[block, ONE, k], wo_recv.at[block, ONE, k], nons[block]),
                remote(got, got, wo_send.at[block, 2, k], wo_recv.at[block, 2, k], twin))

    def halves(body):
        for half in PAIR:
            @pl.when(core == half)
            def _(half=half):
                for k in (2 * half, 2 * half + ONE):
                    body(k)

    def wo_hand(block):
        @pl.when(core == block)
        def _():
            for k in range(4):
                wo_copies(block, k)[ZERO].start()

    def wo_start(block):
        @pl.when(core == block)
        def _():
            for k in (2 * block, 2 * block + ONE):
                wo_copies(block, k)[ONE].start()

        @pl.when(core != block)
        def _():
            for k in range(4):
                wo_copies(block, k)[ZERO].wait_recv()
            for k in (2 - 2 * block, 3 - 2 * block):
                wo_copies(block, k)[2].start()

    def wo_pass(block):
        def body(k):
            wo_copies(block, k)[ONE].wait_recv()
            wo_copies(block, k)[3].start()
        halves(body)

    def wo_arrived(block):
        def body(k):
            wo_copies(block, 3 - k)[3].wait_recv()
        halves(body)

    def op_pairs(i, src):
        cols = pl.ds(i * BLOCK_ROWS, BLOCK_ROWS)
        return ((ntb, lhs_n.at[src, :, :, cols]), (utb, lhs_u.at[src, :, cols]), (dd.at[ZERO], rhs_d.at[ZERO, :, src, cols]),
                (dd.at[ONE], rhs_d.at[ONE, :, src, cols]), (ab.at[ONE], rhs_e.at[src, i]))

    def op_start(n, i, block):
        src, dst = op_pairs(i, core)[n]

        @pl.when(block == core)
        def _():
            local(src, dst, op_send.at[n]).start()

        @pl.when(block != core)
        def _():
            remote(src, dst, op_send.at[n], op_recv.at[i, n], twin).start()

    def op_sent(i):
        wait_all([local(src, dst, op_send.at[n]) for n, (src, dst) in enumerate(op_pairs(i, core))])

    def op_arrived(i):
        all_recv([remote(src, dst, op_send.at[n], op_recv.at[i, n], twin) for n, (src, dst) in enumerate(op_pairs(i, other))])

    def load_tokens(kind, i, slot):
        copies = []
        for hi in PAIR:
            for lo in PAIR:
                src = act.at[kind, lo, hi, i] if kind == E1 else act.at[kind, hi, lo, i]
                copies.append(local(src, ab.at[slot, :, :, :, pl.ds((2 * hi + lo) * QUARTER, QUARTER)], b_sem.at[slot, hi, lo]))
        return copies

    def tokens(slot):
        return ab[slot].reshape(BLOCK_ROWS, WIDTH)

    def normalize():
        def step(n):
            a, b, rows = n // 4, (n // 2) % 2, pl.ds((n % 2) * (ROWS // 2), ROWS // 2)
            tok = ab[ZERO, a, b, rows, :].astype(F32)
            inv = lax.rsqrt(jnp.mean(tok * tok, axis=-ONE, keepdims=True) + EPS)
            ab[ZERO, a, b, rows, :] = (tok * inv).astype(BF16)

        repeat(2 * 4, step)

    def stream(count, loads, body):
        start_all(loads(ZERO, ZERO))

        def step(n):
            slot = n % 2

            @pl.when(n + ONE < count)
            def _():
                start_all(loads(n + ONE, ONE - slot))

            wait_all(loads(n, slot))
            body(n, slot)

        repeat(count, step)

    def col_tile(n):
        return pl.ds((n % TILES) * TILE, TILE)

    def narrow(slot, n):
        return wcol.at[slot, n, :, pl.ds(ZERO, TILE)]

    def wide(n):
        return pl.ds((n % WIDES) * WIDE, WIDE)

    def w_cols(block, n, slot):
        return [local(src.at[block, n // WIDES, :, wide(n)], wcol.at[slot, m], s_sem.at[slot, m]) for m, src in enumerate((wg, wi))]

    def wo_rows(block, n, slot):
        return [local(wo.at[block, n // WIDES, pl.ds((n % WIDES) * WIDE + h * TILE, TILE)], wrow.at[slot, h], s_sem.at[slot, 2 + h]) for h in PAIR]

    def wo_tile(slot):
        return wrow[slot, ZERO:2].reshape(WIDE, WIDTH)

    def kept_load(which, i, n, slot):
        return local(kept.at[which, i, n], fab.at[which % 2, slot], k_sem.at[which % 2, slot])

    def kept_store(which, i, n, slot):
        return local(fab.at[which % 2, slot], kept.at[which, i, n], k_sem.at[which % 2, slot])

    def sum_cols(block, n):
        quarter = pick((2 * cy + n // 2, cx + 2 * (n // 2)), block)
        return pl.ds(quarter * QUARTER + (n % 2) * TILE, TILE)

    def sum_store(task, n, slot):
        return local(pst.at[slot], part.at[task, n // 2, :, :, :, pl.ds((n % 2) * TILE, TILE)], p_sem.at[slot])

    def write_sums(task, loads, product):
        def body(n, slot):
            @pl.when(n >= 2)
            def _():
                sum_store(task, n - 2, slot).wait()

            pst[slot] = product(slot).reshape(2, 2, ROWS, TILE)
            sum_store(task, n, slot).start()

        stream(SUM_TILES, loads, body)
        for slot in PAIR:
            sum_store(task, slot, slot).wait()
        rs_copy(task).start()

    def forward(i):
        all_recv(in_second(X, i))
        run_all(load_tokens(X, i, ZERO))
        normalize()

        def body(n, slot):
            pre_gate = mm(tokens(ZERO), wcol[slot, ZERO], ZERO)
            pre_in = mm(tokens(ZERO), wcol[slot, ONE], ZERO)

            @pl.when(n >= 2)
            def _():
                wait_all([kept_store(m, i, n - 2, slot) for m in PAIR])

            fab[ZERO, slot] = pre_gate
            fab[ONE, slot] = pre_in
            start_all([kept_store(m, i, n, slot) for m in PAIR])
            dd[i % 2, n // WIDES, :, wide(n)] = (pre_gate * jax.nn.sigmoid(pre_gate) * pre_in).astype(BF16)

        stream(HIDDEN_TILES, lambda n, slot: w_cols(ZERO, n, slot), body)
        wait_all([kept_store(m, i, slot, slot) for m in PAIR for slot in PAIR])

    def forward_out(i):
        def loads(n, slot):
            return [local(wo.at[ZERO, fq, :, sum_cols(ZERO, n)], narrow(slot, fq), s_sem.at[slot, fq]) for fq in PAIR]

        write_sums(i, loads, lambda slot: mm(dd[i % 2, ZERO], narrow(slot, ZERO)[...], ZERO) + mm(dd[i % 2, ONE], narrow(slot, ONE)[...], ZERO))

    def hidden_cotangent(i):
        all_recv(in_second(G, i))
        run_all(load_tokens(G, i, ONE))

        def body(n, slot):
            d_hidden = mm(tokens(ONE), wo_tile(slot), ONE)

            @pl.when(n >= 2)
            def _():
                kept_store(2, i, n - 2, slot).wait()

            fab[ZERO, slot] = d_hidden
            kept_store(2, i, n, slot).start()

        stream(HIDDEN_TILES, lambda n, slot: wo_rows(ONE, n, slot), body)
        wait_all([kept_store(2, i, slot, slot) for slot in PAIR])

    def gradients_of(n, h, pre_gate, pre_in, d_hidden):
        rows = pl.ds(h * PART, PART)
        sigma = jax.nn.sigmoid(pre_gate)
        gate_act = pre_gate * sigma
        utw[rows, :] = (gate_act * pre_in).astype(BF16)
        dd[ZERO, n // WIDES, rows, wide(n)] = (d_hidden * pre_in * sigma * (1.0 + pre_gate * (1.0 - sigma))).astype(BF16)
        dd[ONE, n // WIDES, rows, wide(n)] = (d_hidden * gate_act).astype(BF16)

    def keep_u(n, keeps_u):
        @pl.when(n // WIDES == keeps_u)
        def _():
            utb[wide(n), :] = utw[...].T

    def part_of(slot, h):
        return ab[slot, h].reshape(PART, WIDTH)

    def backward(task):
        i = task % CHUNKS
        block = (task // CHUNKS) % 2

        @pl.when(task > CHUNKS)
        def _():
            op_sent(i)

        @pl.when(block == ONE)
        def _():
            all_recv(out_second(ZERO, i))
            start_all(load_tokens(H1, i, ZERO) + load_tokens(G, i, ONE))

        @pl.when(block == ZERO)
        def _():
            all_recv(out_second(ONE, i))
            start_all(load_tokens(X, i, ZERO) + load_tokens(E1, i, ONE))

        wait_all(load_tokens(X, i, ZERO) + load_tokens(X, i, ONE))
        op_start(4, i, block)
        normalize()

        def turn(n):
            ntb[n] = ab[ZERO, :, :, :, sum_cols(block, n)].reshape(BLOCK_ROWS, TILE).T

        repeat(SUM_TILES, turn)
        op_start(ZERO, i, block)

        @pl.when(block == ONE)
        def _():
            def body(n, slot):
                for h in PAIR:
                    pre_gate = mm(part_of(ZERO, h), wcol[slot, ZERO], ZERO)
                    pre_in = mm(part_of(ZERO, h), wcol[slot, ONE], ZERO)
                    gradients_of(n, h, pre_gate, pre_in, fab[ZERO, slot, pl.ds(h * PART, PART)])
                keep_u(n, cx)

            stream(HIDDEN_TILES, lambda n, slot: w_cols(ONE, n, slot) + [kept_load(2, i, n, slot)], body)

        @pl.when(block == ZERO)
        def _():
            def body(n, slot):
                for h in PAIR:
                    rows = pl.ds(h * PART, PART)
                    gradients_of(n, h, fab[ZERO, slot, rows], fab[ONE, slot, rows], mm(part_of(ONE, h), wo_tile(slot), ONE))
                keep_u(n, cy)

            stream(HIDDEN_TILES, lambda n, slot: wo_rows(ZERO, n, slot) + [kept_load(m, i, n, slot) for m in PAIR], body)

        for n in (ONE, 2, 3):
            op_start(n, i, block)

    def backward_out(task):
        block = (task // CHUNKS) % 2

        def loads(n, slot):
            return [local(src.at[block, fq, sum_cols(block, n)], wrow.at[slot, 2 * m + fq], s_sem.at[slot, 2 * m + fq])
                    for m, src in enumerate((wg, wi)) for fq in PAIR]

        def product(slot):
            return sum(mm(dd[m, fq], wrow[slot, 2 * m + fq], ONE) for m in PAIR for fq in PAIR)

        write_sums(task, loads, product)

    def grad_loads(t, slot):
        return [local(rhs_d.at[t // (2 * TILES), (t // TILES) % 2, q, :, col_tile(t)], narrow(slot, q), s_sem.at[slot, q]) for q in PAIR]

    def grad_cols(t, place):
        fq = (t // TILES) % 2
        quarter = pick((place + 2 * fq, 2 * place + fq), core)
        return quarter * WIDTH + (t % TILES) * TILE

    def grad_sent(slot):
        for q in PAIR:
            local(outs.at[slot, q], dwg.at[:, pl.ds(ZERO, TILE)], gr_send.at[slot, q]).wait()

    my_place = pick(rs, core)

    def grad_tile(t):
        mtx, slot, at = t // (2 * TILES), t % SLOTS, t % 2

        @pl.when(t == ZERO)
        def _():
            op_sent(ZERO)
            for i in range(CHUNKS):
                op_arrived(i)
            start_all(grad_loads(ZERO, ZERO))
            run_all([local(lhs_n.at[q], wrow.at[q], l_sem.at[q]) for q in PAIR])

        @pl.when(t + ONE < SENT_TILES)
        def _():
            start_all(grad_loads(t + ONE, ONE - at))

        wait_all(grad_loads(t, at))

        @pl.when(t >= SLOTS)
        def _():
            grad_sent(slot)

        def half(n):
            q = (ONE - my_place) * (ONE - n) + my_place * n

            def rows(src):
                return wrow[src, pl.ds(2 * q, 2)].reshape(QUARTER, WIDTH)

            outs[slot, q] = mm(rows(ZERO), narrow(at, ZERO)[...], ZERO) + mm(rows(ONE), narrow(at, ONE)[...], ZERO)
            cols = pl.ds(grad_cols(t, my_place), TILE)
            for m, dst in enumerate((dwg, dwi)):
                @pl.when((mtx == m) & (n == ZERO) & (t < SENT_TILES - LATE_TILES))
                def _(m=m, dst=dst):
                    remote(outs.at[slot, q], dst.at[:, cols], gr_send.at[slot, q], gr_recv.at[m, (t // TILES) % 2], red_of(core)).start()

                @pl.when((mtx == m) & (n == ONE))
                def _(dst=dst):
                    local(outs.at[slot, q], dst.at[:, cols], gr_send.at[slot, q]).start()

            @pl.when((n == ZERO) & (t >= SENT_TILES - LATE_TILES))
            def _():
                local(outs.at[slot, q], late.at[:, pl.ds((t - SENT_TILES + LATE_TILES) * TILE, TILE)], gr_send.at[slot, q]).start()

        repeat(2, half)

    def out_loads(k, slot):
        return [local(lhs_u.at[q, pl.ds(k * QUARTER, QUARTER)], dd.at[slot, q], o_sem.at[slot, q]) for q in PAIR]

    def out_store(n, k, slot):
        return local(wo_out.at[slot], dwo.at[pl.ds(k * QUARTER, QUARTER), pl.ds(n * WIDE, WIDE)], o_sem.at[slot, 2])

    def out_tile(n):
        e_loads = [local(rhs_e.at[q, :, :, :, :, pl.ds(n * WIDE, WIDE)], ecol.at[q], e_sem.at[q]) for q in PAIR]
        start_all(e_loads + out_loads(ZERO, ZERO))
        wait_all(e_loads)

        def quarter(k):
            slot = k % 2

            @pl.when(k < 3)
            def _():
                start_all(out_loads(k + ONE, ONE - slot))

            wait_all(out_loads(k, slot))

            @pl.when(4 * n + k >= 2)
            def _():
                out_store(n, k, slot).wait()

            wo_out[slot] = mm(dd[slot, ZERO], ecol[ZERO].reshape(WIDTH, WIDE), ZERO) + mm(dd[slot, ONE], ecol[ONE].reshape(WIDTH, WIDE), ZERO)
            out_store(n, k, slot).start()

        repeat(4, quarter)

    barrier = pltpu.get_barrier_semaphore()
    for dev in (reds[ZERO], nons[ZERO], twin, (y_chip, other)):
        pl.semaphore_signal(barrier, inc=ONE, device_id=dev, device_id_type=MESH)
    pl.semaphore_wait(barrier, 4)

    for block in PAIR:
        wo_hand(block)
    per_mtx(lambda mtx: w_hand(ONE - mtx if mtx == ZERO else ZERO).start())

    def given(arr, i):
        return arr.at[i, pl.ds(core * ROWS, ROWS)]

    spots = [[ab.at[n, i // 2, i % 2] for i in range(CHUNKS)] for n in PAIR]
    run_all([local(given(arr, i), spots[n][i], b_sem.at[n, i // 2, i % 2]) for n, arr in enumerate((x, g)) for i in range(CHUNKS)])
    for hi in PAIR:
        for lo in PAIR:
            cols = pl.ds((2 * hi + lo) * QUARTER, QUARTER)
            run_all([local(spots[n][i].at[:, cols], act.at[kind, hi, lo, i, ZERO, ZERO], b_sem.at[n, i // 2, i % 2]) for n, kind in enumerate((X, G)) for i in range(CHUNKS)])

    start_all(in_first(X, ZERO))

    @pl.when(core == ZERO)
    def _():
        for to_red in (ONE, ZERO):
            w_start(ZERO, to_red)

    w_hand(ZERO).wait_recv()

    @pl.when(core == ONE)
    def _():
        for to_red in (ONE, ZERO):
            w_start(ZERO, to_red)

    for i in range(ONE, CHUNKS):
        start_all(in_first(X, i))

    @per_mtx
    def _(mtx):
        for block in PAIR:
            run_all([local(w_src(mtx, block).at[:, f_cols(block, rs[block], fq)], dd.at[ZERO, fq], o_sem.at[ZERO, fq]) for fq in PAIR])
            run_all([local(dd.at[ZERO, fq], w_rows(mtx, block, fq, chip), o_sem.at[ZERO, fq]) for fq in PAIR])
        rows = [pl.ds(k * QUARTER, QUARTER) for k in range(4)]
        run_all([local(wo_in.at[rows[k]], dd.at[k // 2, k % 2], o_sem.at[k // 2, k % 2]) for k in range(4)])
        run_all([local(dd.at[k // 2, k % 2], wo.at[mtx, cs[mtx], rows[k]], o_sem.at[k // 2, k % 2]) for k in range(4)])

    pass_on(in_first(X, ZERO), in_second(X, ZERO))
    for fq in PAIR:
        w_pass(ZERO, fq)
    for i in range(ONE, CHUNKS):
        pass_on(in_first(X, i), in_second(X, i))
    wo_start(ONE)
    wo_start(ZERO)
    w_start(ONE, ZERO)

    @pl.when(core == ZERO)
    def _():
        w_start(ONE, ONE)

    for fq in PAIR:
        w_end(ZERO, fq)
    w_arrived(ZERO)

    def when_forward(tick):
        def run(body):
            @pl.when((tick >= ZERO) & (tick < CHUNKS))
            def _():
                body(tick)
        return run

    def in_two_parts(offset, late):
        def run(body):
            @pl.when(((offset >= ZERO) & (offset < 2)) | ((offset >= late) & (offset < late + 2)))
            def _():
                body(jnp.where(offset < 2, offset, offset - late + 2))
        return run

    def tick_step(tick):
        for n in PAIR:
            @pl.when(tick == n)
            def _(n=n):
                for i in PAIR:
                    start_all(in_first(G, 2 * n + i))

        @pl.when(tick == CHUNKS)
        def _():
            wo_pass(ONE)
            wo_arrived(ONE)

        @pl.when(tick == BACK_AT)
        def _():
            w_arrived(ONE)

        when_forward(tick)(forward)

        @pl.when((tick >= CHUNKS) & (tick < BACK_AT))
        def _():
            hidden_cotangent(tick - CHUNKS)

        @pl.when((tick >= BACK_AT) & (tick < GRADS_AT))
        def _():
            backward(tick - CHUNKS)

        @pl.when(tick >= GRADS_AT)
        def _():
            grad_tile(tick - GRADS_AT)

        grad = tick - GRADS_AT

        @pl.when((grad >= OUT_AT) & ((grad - OUT_AT) % OUT_EVERY == ZERO))
        def _():
            out_tile((grad - OUT_AT) // OUT_EVERY)

        @in_two_parts(tick - PASS_H1, BACK_AT + ONE - PASS_H1)
        def _(i):
            pass_on(out_first(ZERO, i), out_second(ZERO, i))

        @pl.when((tick >= BACK_AT + 3) & (tick < BACK_AT + 3 + CHUNKS))
        def _():
            i = tick - BACK_AT - 3
            pass_on(out_first(ONE, i), out_second(ONE, i))

        last_give = tick == GRADS_AT + 2 * LAG

        @pl.when(((tick >= BACK_AT + 2) & (tick < GRADS_AT + ONE)) | last_give)
        def _():
            rs_give(jnp.where(last_give, TASKS - ONE, tick - CHUNKS - 2))

        in_two_parts(tick - TAKE_H1, BACK_AT - TAKE_H1)(rs_take)

        last_take = tick == GRADS_AT + LAG

        @pl.when(((tick >= BACK_AT + ONE) & (tick < GRADS_AT)) | last_take)
        def _():
            rs_take(jnp.where(last_take, TASKS - ONE, tick - CHUNKS - ONE))

        @pl.when(tick == ONE)
        def _():
            wo_pass(ZERO)
            wo_arrived(ZERO)

            @pl.when(core == ONE)
            def _():
                w_start(ONE, ONE)

        when_forward(tick - ONE)(forward_out)

        for n in PAIR:
            @pl.when(tick == 3 + n)
            def _(n=n):
                for i in PAIR:
                    pass_on(in_first(G, 2 * n + i), in_second(G, 2 * n + i))

            @pl.when(tick == W_PASS[n])
            def _(n=n):
                w_pass(ONE, n)

            @pl.when(tick == W_END[n])
            def _(n=n):
                w_end(ONE, n)

        @pl.when((tick >= BACK_AT) & (tick < GRADS_AT))
        def _():
            backward_out(tick - CHUNKS)

    repeat(GRADS_AT + SENT_TILES, tick_step)

    for m, dst in enumerate((dwg, dwi)):
        for fq in PAIR:
            arrived(dst.at[:, pl.ds(pick((ONE - cx + 2 * fq, 2 * (ONE - cy) + fq), core) * WIDTH, WIDTH - m * fq * LATE_TILES * TILE)], gr_recv.at[m, fq])
    for slot in range(SLOTS):
        grad_sent(slot)
    for slot in PAIR:
        out_store(ZERO, ZERO, slot).wait()
    for i in range(CHUNKS):
        all_recv(dx_copies(i, ZERO)[ONE:])
    for i in (CHUNKS - 2, CHUNKS - ONE):
        dx_sent(i)

    def sent(copies):
        for copy in copies:
            copy.wait_send()

    for i in range(CHUNKS):
        for kind in (X, G):
            sent(in_first(kind, i) + in_second(kind, i))
        for block in PAIR:
            sent(out_first(block, i) + out_second(block, i))
    repeat(TASKS, lambda task: rs_copy(task).wait_send())
    for task in (TASKS - 2, TASKS - ONE):
        sent(dot_copies(task))
    for block in PAIR:
        for fq in PAIR:
            sent(w_first(ZERO, block, fq) + (w_second(ZERO, block, fq),))
            sent(w_twin(ZERO, block, fq))
    for k in range(4):
        for block in PAIR:
            @pl.when(core == block)
            def _(block=block, k=k):
                wo_copies(block, k)[ZERO].wait_send()

    def wo_sent(k):
        for block in PAIR:
            sent((wo_copies(block, k)[ONE], wo_copies(block, k)[3]))

    halves(wo_sent)
    w_hand(ZERO).wait_send()


def settle_kernel(*refs):
    for src, dst in zip(refs[:4], refs[4:]):
        dst[...] = src[...]


def settle(arrays, steps=16):
    specs = [pl.BlockSpec((arr.shape[0] // steps, arr.shape[1]), lambda i: (i, 0)) for arr in arrays]
    size = sum(arr.size * arr.dtype.itemsize for arr in arrays)
    return pl.pallas_call(
        settle_kernel, grid=(steps,), out_shape=[jax.ShapeDtypeStruct(arr.shape, arr.dtype) for arr in arrays], in_specs=specs, out_specs=specs,
        name='settle', cost_estimate=pl.CostEstimate(flops=2 ** 30, bytes_accessed=2 * size, transcendentals=0),
        compiler_params=pltpu.CompilerParams(vmem_limit_bytes=67_043_328),
    )(*arrays)


def insert_kernel(spot, late, whole, out):
    out[...] = late[...]


def insert_late(whole, late, spot):
    block = (QUARTER, QUARTER)
    return pl.pallas_call(
        insert_kernel, out_shape=jax.ShapeDtypeStruct(whole.shape, whole.dtype),
        grid_spec=pltpu.PrefetchScalarGridSpec(
            num_scalar_prefetch=1, grid=(3,), in_specs=[pl.BlockSpec(block, lambda k, spot: (0, k)), pl.BlockSpec(memory_space=pl.ANY)],
            out_specs=pl.BlockSpec(block, lambda k, spot: (0, 4 * spot[0] + 1 + k))),
        input_output_aliases={2: 0}, name='insert_late',
    )(spot, late, whole)


def solution(mesh):
    act_spec = P(None, 'data', None, None)
    weight_spec = P('stage', None, 'data', None)

    def per_device(x, g, w_gate, w_in, w_out):
        flat = (CHUNKS, 2 * ROWS, WIDTH)
        any_space = pl.BlockSpec(memory_space=pl.ANY)
        pair = (2, 2)

        def arr(*shape, dtype=BF16):
            return jax.ShapeDtypeStruct(shape, dtype)

        def f32(*shape):
            return arr(*shape, dtype=F32)

        piece = (*pair, ROWS, QUARTER)
        out_shapes = [
            arr(*flat), f32(QUARTER, 4 * WIDTH), f32(QUARTER, 4 * WIDTH), f32(WIDTH, WIDTH), f32(QUARTER, LATE_TILES * TILE),
            arr(4, *pair, CHUNKS, *pair, ROWS, QUARTER), *[arr(*pair, WIDTH, WIDTH)] * 3, arr(QUARTER, 4 * WIDTH),
            f32(TASKS, 2, *piece), f32(TASKS, *piece), f32(2 * CHUNKS, 2, ROWS, ROWS), f32(3, CHUNKS, HIDDEN_TILES, BLOCK_ROWS, WIDE),
            arr(2, SUM_TILES, TILE, WIDTH), arr(2, WIDTH, WIDTH), arr(*pair, 2, WIDTH, WIDTH), arr(2, CHUNKS, *pair, ROWS, WIDTH),
        ]

        def bf(*shape):
            return pltpu.VMEM(shape, BF16)

        def fl(*shape):
            return pltpu.VMEM(shape, F32)

        scratch = [
            bf(*pair, WIDTH, WIDE), bf(2, 4, TILE, WIDTH), fl(*pair, BLOCK_ROWS, WIDE), bf(2, *pair, ROWS, WIDTH), bf(*pair, BLOCK_ROWS, WIDTH),
            bf(SUM_TILES, TILE, BLOCK_ROWS), bf(WIDTH, BLOCK_ROWS), bf(BLOCK_ROWS, WIDE), fl(2, *pair, ROWS, TILE), fl(2, *piece), fl(2, *piece), bf(3, *piece),
            fl(2, 2, ROWS, ROWS), bf(2, *piece), bf(2, 2, ROWS, HALF), bf(2, CHUNKS, *pair, ROWS, WIDE), fl(SLOTS, 2, QUARTER, TILE), fl(2, QUARTER, WIDE),
        ]
        counts = [(4, CHUNKS, 8), (4, CHUNKS, 8), (TASKS,), (TASKS,), (2 * CHUNKS, 2), (2 * CHUNKS, 2), (*pair, 3), (*pair, 3), (*pair, 4), (*pair, 4),
                  (1,), (1,), (2, 3, 4), (2, 3, 4), (5,), (CHUNKS, 5), (CHUNKS, 4), (CHUNKS, 3), (SLOTS, 2), pair, (2,), (4,), (2, 4), pair, (2, *pair), (2, 3), (2,)]
        results = pl.pallas_call(
            step_kernel, out_shape=out_shapes, in_specs=[any_space] * 5, out_specs=[any_space] * len(out_shapes),
            scratch_shapes=scratch + [pltpu.SemaphoreType.DMA(count) for count in counts], name='mlp_step',
            compiler_params=pltpu.CompilerParams(collective_id=0, has_side_effects=True, vmem_limit_bytes=67_043_328),
        )(x.reshape(flat), g.reshape(flat), w_gate[0, 0], w_in[0, 0], w_out[0, 0])
        late = lax.ppermute(results[4], ('data', 'stage'), [(2 * c + s, 2 * (c ^ (1 + s)) + s) for c in range(4) for s in PAIR])
        chip, core = lax.axis_index('data'), lax.axis_index('stage')
        spot = jnp.where(core == 0, 3 - chip % 2, 3 - 2 * (chip // 2))
        dx, d_gate, d_in, d_out = settle((results[0].reshape(-1, WIDTH), *results[1:4]))
        d_in = insert_late(d_in, late, spot.astype(jnp.int32).reshape(1))
        return dx.reshape(x.shape), d_gate[None, None], d_in[None, None], d_out[None, None]

    return jax.shard_map(per_device, mesh=mesh, in_specs=(act_spec, act_spec, weight_spec, weight_spec, weight_spec),
                         out_specs=(act_spec, weight_spec, weight_spec, weight_spec), check_vma=False)
```

```python
import jax
import jax.numpy as jnp
from jax import lax
from jax.experimental import pallas as pl
from jax.experimental.pallas import tpu as pltpu
from jax.sharding import PartitionSpec as P

MESH = pl.DeviceIdType.MESH
F32 = jnp.float32
BF16 = jnp.bfloat16
EPS = 1e-6

CHUNKS = 4
ROWS = 128
BLOCK_ROWS = 4 * ROWS
WIDTH = 2048
HALF = WIDTH // 2
QUARTER = WIDTH // 4
TILE = 256
TILES = WIDTH // TILE
WIDE = 2 * TILE
WIDES = WIDTH // WIDE
PART = BLOCK_ROWS // 2
HIDDEN_TILES = 2 * WIDES
SUM_TILES = HALF // TILE
TASKS = 3 * CHUNKS
BACK_AT = 2 * CHUNKS
GRADS_AT = 4 * CHUNKS
SENT_TILES = 4 * TILES
SLOTS = 4
OUT_AT, OUT_EVERY = 8, 7
LATE_TILES = 6
LAG = 6
W_PASS, W_END = (2, 3), (7, 7)
TAKE_H1, PASS_H1 = 4, 6
PAIR = ZERO, ONE = range(2)
X, H1, G, E1 = range(4)


def mm(lhs, rhs, rhs_dim):
    return lax.dot_general(lhs, rhs, (((1,), (rhs_dim,)), ((), ())), preferred_element_type=F32)


def repeat(count, body):
    def step(n, carry):
        body(n)
        return carry

    lax.fori_loop(0, count, step, 0)


def start_all(copies):
    for copy in copies:
        copy.start()


def wait_all(copies):
    for copy in copies:
        copy.wait()


def run_all(copies):
    start_all(copies)
    wait_all(copies)


def step_kernel(x, g, wg_in, wi_in, wo_in,
                dx, dwg, dwi, dwo, late, act, wg, wi, wo, wx, part, rb, dots, kept, lhs_n, lhs_u, rhs_d, rhs_e,
                wcol, wrow, fab, ab, dd, ntb, utb, utw, pst, ld, tot, own, dsv, new, dxn, ecol, outs, wo_out,
                ag_send, ag_recv, rs_send, rs_recv, dt_send, dt_recv, w_send, w_recv, f_send, f_recv, h_send, h_recv, wo_send, wo_recv,
                op_send, op_recv, dx_send, dx_recv, gr_send, gr_recv, p_sem, l_sem, s_sem, k_sem, b_sem, o_sem, e_sem):
    chip = lax.axis_index('data')
    core = lax.axis_index('stage')
    cx, cy = chip % 2, chip // 2
    other = ONE - core
    x_chip, y_chip = cy * 2 + (ONE - cx), (ONE - cy) * 2 + cx
    twin = (chip, other)
    reds, nons = ((x_chip, core), (y_chip, core)), ((y_chip, core), (x_chip, core))
    rs, cs = (cx, cy), (cy, cx)

    def pick(pair, block):
        return pair[ZERO] + (pair[ONE] - pair[ZERO]) * block

    def red_of(block):
        return pick((x_chip, y_chip), block), core

    def local(src, dst, sem):
        return pltpu.make_async_copy(src, dst, sem)

    def remote(src, dst, send, recv, dev):
        return pltpu.make_async_remote_copy(src_ref=src, dst_ref=dst, send_sem=send, recv_sem=recv, device_id=dev, device_id_type=MESH)

    def arrived(ref, sem):
        local(ref, ref, sem).wait()

    def in_first(kind, i):
        block = kind // G
        mine = act.at[kind, :, :, i, ZERO, ZERO]
        return (remote(mine, act.at[kind, :, :, i, ONE, ZERO], ag_send.at[kind, i, ZERO], ag_recv.at[kind, i, ZERO], reds[block]),
                remote(mine, act.at[kind, :, :, i, ZERO, ONE], ag_send.at[kind, i, ONE], ag_recv.at[kind, i, ONE], nons[block]))

    def in_second(kind, i):
        block = kind // G
        sends = [remote(act.at[kind, :2 - (kind == X), :, i, ZERO, ONE], act.at[kind, :2 - (kind == X), :, i, ONE, ONE], ag_send.at[kind, i, 2], ag_recv.at[kind, i, 2], reds[block])]
        if kind == X:
            sends.append(remote(act.at[kind, ONE, :, i, ONE, ZERO], act.at[kind, ONE, :, i, ONE, ONE], ag_send.at[kind, i, 3], ag_recv.at[kind, i, 3], nons[block]))
        return sends

    def out_first(block, i):
        kind, c = (H1, E1)[block], cs[block]
        sends = [remote(act.at[kind, c, :, i, :, ZERO], act.at[kind, c, :, i, :, ONE], ag_send.at[kind, i, ZERO], ag_recv.at[kind, i, ZERO], reds[block])]
        for a in PAIR:
            sends.append(remote(act.at[kind, c, :, i, a, ZERO], act.at[kind, c, :, i, ONE - a, ZERO], ag_send.at[kind, i, ONE + a], ag_recv.at[kind, i, 2 - a], nons[block]))
        return sends

    def out_second(block, i):
        kind, c = (H1, E1)[block], cs[block]
        sends = []
        if block:
            sends.append(remote(act.at[kind, ONE - c, ZERO, i, :, ZERO], act.at[kind, ONE - c, ZERO, i, :, ONE], ag_send.at[kind, i, 3], ag_recv.at[kind, i, 3], reds[block]))
        for a in PAIR:
            for h in range(block, 2):
                sends.append(remote(act.at[kind, c, h, i, a, ONE], act.at[kind, c, h, i, ONE - a, ONE], ag_send.at[kind, i, 4 + 2 * a + h], ag_recv.at[kind, i, 6 - 2 * a + h], nons[block]))
        return sends

    def pass_on(first, second):
        for copy in first:
            copy.wait_recv()
        start_all(second)

    def all_recv(copies):
        for copy in copies:
            copy.wait_recv()

    def rs_copy(task):
        return remote(part.at[task, :, ONE], rb.at[task], rs_send.at[task], rs_recv.at[task], red_of((task // CHUNKS) % 2))

    def dot_copies(task):
        slot, n = task % 2, task - CHUNKS
        dev = pick((y_chip, x_chip), (task // CHUNKS) % 2), core
        return [remote(dsv.at[slot, b], dots.at[n, ONE - b], dt_send.at[n, b], dt_recv.at[n, ONE - b], dev) for b in PAIR]

    def own_half(kind_h, block, i):
        if block == ZERO:
            return act.at[X, cy, :, i, ZERO] if kind_h else act.at[E1, :, cy, i, ZERO]
        return act.at[H1, :, cx, i, ZERO] if kind_h else act.at[G, :, cx, i, ZERO]

    def rest_half(block, i):
        return act.at[X, ONE - cy, :, i, ZERO] if block == ZERO else act.at[H1, :, ONE - cx, i, ZERO]

    def when_kind(task):
        def run(body):
            for kind in range(3):
                @pl.when(task // CHUNKS == kind)
                def _(kind=kind):
                    body(kind)
        return run

    def send_result(block, i, slot):
        run_all([local(new.at[slot], act.at[(H1, E1)[block], cs[block], :, i, :, ZERO], l_sem.at[ZERO])])
        start_all(out_first(block, i))

    def pieces(body):
        def step(n):
            body(n // 4, (n // 2) % 2, pl.ds((n % 2) * (ROWS // 2), ROWS // 2))
        repeat(2 * 4, step)

    def rs_take(task):
        i, slot = task % CHUNKS, task % 2
        rs_copy(task).wait_recv()
        start_all([local(part.at[task, :, ZERO], ld.at[ZERO], l_sem.at[ZERO]), local(rb.at[task], ld.at[ONE], l_sem.at[ONE])])

        @when_kind(task)
        def _(kind):
            local(own_half(True, kind % 2, i), own.at[ZERO], l_sem.at[2]).start()

        wait_all([local(rb.at[task], ld.at[ZERO], l_sem.at[ZERO]), local(rb.at[task], ld.at[ONE], l_sem.at[ONE]), local(own_half(True, ZERO, i), own.at[ZERO], l_sem.at[2])])

        @pl.when(task < CHUNKS)
        def _():
            @pieces
            def _(q, b, rows):
                new[slot, q, b, rows, :] = own[ZERO, q, b, rows, :] + (ld[ZERO, q, b, rows, :] + ld[ONE, q, b, rows, :]).astype(BF16)

            send_result(ZERO, i, slot)

        @pl.when(task >= CHUNKS)
        def _():
            @pl.when(task >= CHUNKS + 2)
            def _():
                for copy in dot_copies(task - 2):
                    copy.wait_send()

            @pieces
            def _(q, b, rows):
                total = ld[ZERO, q, b, rows, :] + ld[ONE, q, b, rows, :]
                tot[slot, q, b, rows, :] = total
                dot = jnp.sum(total * own[ZERO, q, b, rows, :].astype(F32), axis=-ONE, keepdims=True) + jnp.zeros((ONE, ROWS), F32)

                @pl.when(q == ZERO)
                def _():
                    dsv[slot, b, rows, :] = dot

                @pl.when(q == ONE)
                def _():
                    dsv[slot, b, rows, :] = dsv[slot, b, rows, :] + dot

            start_all(dot_copies(task))

    def dx_copies(i, slot):
        spot = dx.at[i, pl.ds(core * ROWS, ROWS), pl.ds(cy * HALF, HALF)]
        return (local(dxn.at[slot, ZERO], spot, dx_send.at[i, ZERO]), remote(dxn.at[slot, ZERO], spot, dx_send.at[i, ONE], dx_recv.at[i, ZERO], twin),
                remote(dxn.at[slot, ONE], spot, dx_send.at[i, 2], dx_recv.at[i, ONE], (y_chip, core)),
                remote(dxn.at[slot, ONE], spot, dx_send.at[i, 3], dx_recv.at[i, 2], (y_chip, other)))

    def dx_sent(i):
        copies = dx_copies(i, i % 2)
        copies[ZERO].wait()
        for copy in copies[ONE:]:
            copy.wait_send()

    def rs_give(task):
        i, slot = task % CHUNKS, task % 2
        for b in PAIR:
            arrived(dots.at[task - CHUNKS, b], dt_recv.at[task - CHUNKS, b])
        local(dots.at[task - CHUNKS], ld.at[ZERO, ZERO, :, :, pl.ds(ZERO, ROWS)], l_sem.at[3]).start()
        for block in PAIR:
            @pl.when((task // CHUNKS) % 2 == block)
            def _(block=block):
                start_all([local(src, own.at[n], l_sem.at[n]) for n, src in enumerate((own_half(True, block, i), own_half(False, block, i), rest_half(block, i)))])
        wait_all([local(own_half(True, ZERO, i), own.at[n], l_sem.at[n]) for n in range(3)])
        local(dots.at[task - CHUNKS], ld.at[ZERO, ZERO, :, :, pl.ds(ZERO, ROWS)], l_sem.at[3]).wait()

        @pl.when(task >= 2 * CHUNKS + 2)
        def _():
            dx_sent(i - 2)

        def step(n):
            b, rows = n // 2, pl.ds((n % 2) * (ROWS // 2), ROWS // 2)

            def sq(slot_of, q):
                vals = own[slot_of, q, b, rows, :].astype(F32)
                return jnp.sum(vals * vals, axis=-ONE, keepdims=True)

            square = sq(ZERO, ZERO) + sq(ZERO, ONE) + sq(2, ZERO) + sq(2, ONE)
            inv = lax.rsqrt(square / WIDTH + EPS)
            dot = (dsv[slot, b, rows, ZERO:ONE] + ld[ZERO, ZERO, b, rows, ZERO:ONE]) / WIDTH
            for q in PAIR:
                tok = own[ZERO, q, b, rows, :].astype(F32)
                resid = tot[slot, q, b, rows, :] * inv - tok * (inv * inv * inv * dot)
                val = (own[ONE, q, b, rows, :].astype(F32) + resid).astype(BF16)
                new[slot, q, b, rows, :] = val
                dxn[slot, b, rows, pl.ds(q * QUARTER, QUARTER)] = val

        repeat(4, step)

        @pl.when(task < 2 * CHUNKS)
        def _():
            send_result(ONE, i, slot)

        @pl.when(task >= 2 * CHUNKS)
        def _():
            start_all(dx_copies(i, slot))

    def f_cols(block, place, fq):
        quarter = place + 2 * fq if block == ZERO else 2 * place + fq
        return pl.ds(quarter * WIDTH, WIDTH)

    def w_src(mtx, block):
        return ((wg_in, wx), (wx, wi_in))[mtx][block]

    def w_rows(mtx, block, fq, of):
        return (wg, wi)[mtx].at[block, fq, pl.ds(of * QUARTER, QUARTER)]

    def w_first(mtx, block, fq):
        src, mine = w_src(mtx, block), w_rows(mtx, block, fq, chip)
        return (remote(src.at[:, f_cols(block, rs[block], fq)], mine, w_send.at[block, fq, ZERO], w_recv.at[block, fq, ZERO], nons[block]),
                remote(src.at[:, f_cols(block, ONE - rs[block], fq)], mine, w_send.at[block, fq, ONE], w_recv.at[block, fq, ONE], reds[block]))

    def w_second(mtx, block, fq):
        piece = w_rows(mtx, block, fq, reds[block][ZERO])
        return remote(piece, piece, w_send.at[block, fq, 2], w_recv.at[block, fq, 2], nons[block])

    def w_twin(mtx, block, fq):
        far = 3 - chip
        srcs = [w_src(mtx, block).at[:, f_cols(block, rs[block], fq)]] + [w_rows(mtx, block, fq, of) for of in (nons[block][ZERO], reds[block][ZERO], far)]
        spots = [w_rows(mtx, block, fq, of) for of in (chip, nons[block][ZERO], reds[block][ZERO], far)]
        return [remote(src, spot, f_send.at[block, fq, n], f_recv.at[block, fq, n], twin) for n, (src, spot) in enumerate(zip(srcs, spots))]

    def per_mtx(body):
        for mtx in PAIR:
            @pl.when(core == mtx)
            def _(mtx=mtx):
                body(mtx)

    def w_start(block, to_red):
        @per_mtx
        def _(mtx):
            for fq in PAIR:
                w_first(mtx, block, fq)[to_red].start()
                if not to_red:
                    w_twin(mtx, block, fq)[ZERO].start()

    def w_pass(block, fq):
        @per_mtx
        def _(mtx):
            first, to_twin = w_first(mtx, block, fq), w_twin(mtx, block, fq)
            first[ONE].wait_recv()
            w_second(mtx, block, fq).start()
            to_twin[2].start()
            first[ZERO].wait_recv()
            to_twin[ONE].start()

    def w_end(block, fq):
        @per_mtx
        def _(mtx):
            w_second(mtx, block, fq).wait_recv()
            w_twin(mtx, block, fq)[3].start()

    def w_arrived(block):
        for fq in PAIR:
            all_recv(w_twin(ZERO, block, fq))

    def w_hand(mtx):
        return remote((wg_in, wi_in)[mtx], wx, h_send.at[ZERO], h_recv.at[ZERO], twin)

    def wo_copies(block, k):
        rows = pl.ds(k * QUARTER, QUARTER)
        spot, got = wo.at[block, cs[block], rows], wo.at[block, ONE - cs[block], rows]
        return (remote(wo_in.at[rows], spot, wo_send.at[block, ZERO, k], wo_recv.at[block, ZERO, k], twin),
                remote(wo_in.at[rows], spot, wo_send.at[block, ONE, k], wo_recv.at[block, ONE, k], nons[block]),
                remote(spot, spot, wo_send.at[block, ONE, k], wo_recv.at[block, ONE, k], nons[block]),
                remote(got, got, wo_send.at[block, 2, k], wo_recv.at[block, 2, k], twin))

    def halves(body):
        for half in PAIR:
            @pl.when(core == half)
            def _(half=half):
                for k in (2 * half, 2 * half + ONE):
                    body(k)

    def wo_hand(block):
        @pl.when(core == block)
        def _():
            for k in range(4):
                wo_copies(block, k)[ZERO].start()

    def wo_start(block):
        @pl.when(core == block)
        def _():
            for k in (2 * block, 2 * block + ONE):
                wo_copies(block, k)[ONE].start()

        @pl.when(core != block)
        def _():
            for k in range(4):
                wo_copies(block, k)[ZERO].wait_recv()
            for k in (2 - 2 * block, 3 - 2 * block):
                wo_copies(block, k)[2].start()

    def wo_pass(block):
        def body(k):
            wo_copies(block, k)[ONE].wait_recv()
            wo_copies(block, k)[3].start()
        halves(body)

    def wo_arrived(block):
        def body(k):
            wo_copies(block, 3 - k)[3].wait_recv()
        halves(body)

    def op_pairs(i, src):
        cols = pl.ds(i * BLOCK_ROWS, BLOCK_ROWS)
        return ((ntb, lhs_n.at[src, :, :, cols]), (utb, lhs_u.at[src, :, cols]), (dd.at[ZERO], rhs_d.at[ZERO, :, src, cols]),
                (dd.at[ONE], rhs_d.at[ONE, :, src, cols]), (ab.at[ONE], rhs_e.at[src, i]))

    def op_start(n, i, block):
        src, dst = op_pairs(i, core)[n]

        @pl.when(block == core)
        def _():
            local(src, dst, op_send.at[n]).start()

        @pl.when(block != core)
        def _():
            remote(src, dst, op_send.at[n], op_recv.at[i, n], twin).start()

    def op_sent(i, which):
        for n in which:
            local(*op_pairs(i, core)[n], op_send.at[n]).wait()

    def op_arrived(i):
        all_recv([remote(src, dst, op_send.at[n], op_recv.at[i, n], twin) for n, (src, dst) in enumerate(op_pairs(i, other))])

    def load_tokens(kind, i, slot):
        copies = []
        for hi in PAIR:
            for lo in PAIR:
                src = act.at[kind, lo, hi, i] if kind == E1 else act.at[kind, hi, lo, i]
                copies.append(local(src, ab.at[slot, :, :, :, pl.ds((2 * hi + lo) * QUARTER, QUARTER)], b_sem.at[slot, hi, lo]))
        return copies

    def tokens(slot):
        return ab[slot].reshape(BLOCK_ROWS, WIDTH)

    def normalize():
        def step(n):
            a, b, rows = n // 4, (n // 2) % 2, pl.ds((n % 2) * (ROWS // 2), ROWS // 2)
            tok = ab[ZERO, a, b, rows, :].astype(F32)
            inv = lax.rsqrt(jnp.mean(tok * tok, axis=-ONE, keepdims=True) + EPS)
            ab[ZERO, a, b, rows, :] = (tok * inv).astype(BF16)

        repeat(2 * 4, step)

    def stream(count, loads, body, started=False):
        if not started:
            start_all(loads(ZERO, ZERO))

        def step(n):
            slot = n % 2

            @pl.when(n + ONE < count)
            def _():
                start_all(loads(n + ONE, ONE - slot))

            wait_all(loads(n, slot))
            body(n, slot)

        repeat(count, step)

    def col_tile(n):
        return pl.ds((n % TILES) * TILE, TILE)

    def narrow(slot, n):
        return wcol.at[slot, n, :, pl.ds(ZERO, TILE)]

    def wide(n):
        return pl.ds((n % WIDES) * WIDE, WIDE)

    def w_cols(block, n, slot):
        return [local(src.at[block, n // WIDES, :, wide(n)], wcol.at[slot, m], s_sem.at[slot, m]) for m, src in enumerate((wg, wi))]

    def wo_rows(block, n, slot):
        return [local(wo.at[block, n // WIDES, pl.ds((n % WIDES) * WIDE + h * TILE, TILE)], wrow.at[slot, h], s_sem.at[slot, 2 + h]) for h in PAIR]

    def wo_tile(slot):
        return wrow[slot, ZERO:2].reshape(WIDE, WIDTH)

    def kept_load(which, i, n, slot):
        return local(kept.at[which, i, n], fab.at[which % 2, slot], k_sem.at[which % 2, slot])

    def kept_store(which, i, n, slot):
        return local(fab.at[which % 2, slot], kept.at[which, i, n], k_sem.at[which % 2, slot])

    def sum_cols(block, n):
        quarter = pick((2 * cy + n // 2, cx + 2 * (n // 2)), block)
        return pl.ds(quarter * QUARTER + (n % 2) * TILE, TILE)

    def sum_store(task, n, slot):
        return local(pst.at[slot], part.at[task, n // 2, :, :, :, pl.ds((n % 2) * TILE, TILE)], p_sem.at[slot])

    def write_sums(task, loads, product, started=False):
        def body(n, slot):
            @pl.when(n >= 2)
            def _():
                sum_store(task, n - 2, slot).wait()

            pst[slot] = product(slot).reshape(2, 2, ROWS, TILE)
            sum_store(task, n, slot).start()

        stream(SUM_TILES, loads, body, started)
        for slot in PAIR:
            sum_store(task, slot, slot).wait()
        rs_copy(task).start()

    def forward(i):
        all_recv(in_second(X, i))
        run_all(load_tokens(X, i, ZERO))
        normalize()

        @pl.when(i > ZERO)
        def _():
            op_sent(i, PAIR)

        turn_tokens(i, ZERO)

        def body(n, slot):
            pre_gate = mm(tokens(ZERO), wcol[slot, ZERO], ZERO)
            pre_in = mm(tokens(ZERO), wcol[slot, ONE], ZERO)

            @pl.when(n >= 2)
            def _():
                wait_all([kept_store(m, i, n - 2, slot) for m in PAIR])

            fab[ZERO, slot] = pre_gate
            fab[ONE, slot] = pre_in
            start_all([kept_store(m, i, n, slot) for m in PAIR])
            hidden = (pre_gate * jax.nn.sigmoid(pre_gate) * pre_in).astype(BF16)
            dd[i % 2, n // WIDES, :, wide(n)] = hidden
            keep_u(n, cy, hidden)

        stream(HIDDEN_TILES, lambda n, slot: w_cols(ZERO, n, slot), body)
        wait_all([kept_store(m, i, slot, slot) for m in PAIR for slot in PAIR])
        op_start(ONE, i, ZERO)

    def forward_out(i):
        def loads(n, slot):
            return [local(wo.at[ZERO, fq, :, sum_cols(ZERO, n)], narrow(slot, fq), s_sem.at[slot, fq]) for fq in PAIR]

        write_sums(i, loads, lambda slot: mm(dd[i % 2, ZERO], narrow(slot, ZERO)[...], ZERO) + mm(dd[i % 2, ONE], narrow(slot, ONE)[...], ZERO))

    def hidden_cotangent(i):
        all_recv(in_second(G, i))
        run_all(load_tokens(G, i, ONE))

        def body(n, slot):
            d_hidden = mm(tokens(ONE), wo_tile(slot), ONE)

            @pl.when(n >= 2)
            def _():
                kept_store(2, i, n - 2, slot).wait()

            fab[ZERO, slot] = d_hidden
            kept_store(2, i, n, slot).start()

        stream(HIDDEN_TILES, lambda n, slot: wo_rows(ONE, n, slot), body)
        wait_all([kept_store(2, i, slot, slot) for slot in PAIR])

    def gradients_of(n, h, pre_gate, pre_in, d_hidden):
        rows = pl.ds(h * PART, PART)
        sigma = jax.nn.sigmoid(pre_gate)
        gate_act = pre_gate * sigma
        dd[ZERO, n // WIDES, rows, wide(n)] = (d_hidden * pre_in * sigma * (1.0 + pre_gate * (1.0 - sigma))).astype(BF16)
        dd[ONE, n // WIDES, rows, wide(n)] = (d_hidden * gate_act).astype(BF16)
        return gate_act

    def keep_u(n, keeps_u, hidden):
        @pl.when(n // WIDES == keeps_u)
        def _():
            utb[wide(n), :] = hidden.T

    def turn_tokens(i, block):
        def turn(n):
            ntb[n] = ab[ZERO, :, :, :, sum_cols(block, n)].reshape(BLOCK_ROWS, TILE).T

        repeat(SUM_TILES, turn)
        op_start(ZERO, i, block)

    def part_of(slot, h):
        return ab[slot, h].reshape(PART, WIDTH)

    def backward(task):
        i = task % CHUNKS
        block = (task // CHUNKS) % 2

        def loads_1(n, slot):
            return w_cols(ONE, n, slot) + [kept_load(2, i, n, slot)]

        def loads_0(n, slot):
            return wo_rows(ZERO, n, slot) + [kept_load(m, i, n, slot) for m in PAIR]

        for n, loads in enumerate((loads_0, loads_1)):
            @pl.when(block == n)
            def _(loads=loads):
                start_all(loads(ZERO, ZERO))

        @pl.when(task <= BACK_AT)
        def _():
            op_sent(i, PAIR)

        @pl.when(task > CHUNKS)
        def _():
            op_sent(i, range(2, 5))

        @pl.when(block == ONE)
        def _():
            all_recv(out_second(ZERO, i))
            run_all(load_tokens(H1, i, ZERO) + load_tokens(G, i, ONE))
            op_start(4, i, ONE)
            normalize()
            turn_tokens(i, ONE)

        @pl.when(block == ZERO)
        def _():
            all_recv(out_second(ONE, i))
            run_all(load_tokens(E1, i, ONE))
            op_start(4, i, ZERO)

        @pl.when(block == ONE)
        def _():
            def body(n, slot):
                for h in PAIR:
                    pre_gate = mm(part_of(ZERO, h), wcol[slot, ZERO], ZERO)
                    pre_in = mm(part_of(ZERO, h), wcol[slot, ONE], ZERO)
                    gate_act = gradients_of(n, h, pre_gate, pre_in, fab[ZERO, slot, pl.ds(h * PART, PART)])
                    utw[pl.ds(h * PART, PART), :] = (gate_act * pre_in).astype(BF16)
                keep_u(n, cx, utw[...])

            stream(HIDDEN_TILES, loads_1, body, started=True)

        @pl.when(block == ZERO)
        def _():
            def body(n, slot):
                for h in PAIR:
                    rows = pl.ds(h * PART, PART)
                    gradients_of(n, h, fab[ZERO, slot, rows], fab[ONE, slot, rows], mm(part_of(ONE, h), wo_tile(slot), ONE))

            stream(HIDDEN_TILES, loads_0, body, started=True)

        @pl.when(block == ONE)
        def _():
            op_start(ONE, i, ONE)

        for n in (2, 3):
            op_start(n, i, block)

    def back_loads(block, n, slot):
        return [local(src.at[block, fq, sum_cols(block, n)], wrow.at[slot, 2 * m + fq], s_sem.at[slot, 2 * m + fq])
                for m, src in enumerate((wg, wi)) for fq in PAIR]

    def backward_out(task):
        block = (task // CHUNKS) % 2

        def loads(n, slot):
            return back_loads(block, n, slot)

        def product(slot):
            return sum(mm(dd[m, fq], wrow[slot, 2 * m + fq], ONE) for m in PAIR for fq in PAIR)

        write_sums(task, loads, product, started=True)

    def grad_loads(t, slot):
        return [local(rhs_d.at[t // (2 * TILES), (t // TILES) % 2, q, :, col_tile(t)], narrow(slot, q), s_sem.at[slot, q]) for q in PAIR]

    def grad_cols(t, place):
        fq = (t // TILES) % 2
        quarter = pick((place + 2 * fq, 2 * place + fq), core)
        return quarter * WIDTH + (t % TILES) * TILE

    def grad_sent(slot):
        for q in PAIR:
            local(outs.at[slot, q], dwg.at[:, pl.ds(ZERO, TILE)], gr_send.at[slot, q]).wait()

    my_place = pick(rs, core)

    def grad_tile(t):
        mtx, slot, at = t // (2 * TILES), t % SLOTS, t % 2

        @pl.when(t == ZERO)
        def _():
            op_sent(ZERO, range(2, 5))
            for i in range(CHUNKS):
                op_arrived(i)
            start_all(grad_loads(ZERO, ZERO))
            run_all([local(lhs_n.at[q], wrow.at[q], l_sem.at[q]) for q in PAIR])

        @pl.when(t + ONE < SENT_TILES)
        def _():
            start_all(grad_loads(t + ONE, ONE - at))

        wait_all(grad_loads(t, at))

        @pl.when(t >= SLOTS)
        def _():
            grad_sent(slot)

        def half(n):
            q = (ONE - my_place) * (ONE - n) + my_place * n

            def rows(src):
                return wrow[src, pl.ds(2 * q, 2)].reshape(QUARTER, WIDTH)

            outs[slot, q] = mm(rows(ZERO), narrow(at, ZERO)[...], ZERO) + mm(rows(ONE), narrow(at, ONE)[...], ZERO)
            cols = pl.ds(grad_cols(t, my_place), TILE)
            for m, dst in enumerate((dwg, dwi)):
                @pl.when((mtx == m) & (n == ZERO) & (t < SENT_TILES - LATE_TILES))
                def _(m=m, dst=dst):
                    remote(outs.at[slot, q], dst.at[:, cols], gr_send.at[slot, q], gr_recv.at[m, (t // TILES) % 2], red_of(core)).start()

                @pl.when((mtx == m) & (n == ONE))
                def _(dst=dst):
                    local(outs.at[slot, q], dst.at[:, cols], gr_send.at[slot, q]).start()

            @pl.when((n == ZERO) & (t >= SENT_TILES - LATE_TILES))
            def _():
                local(outs.at[slot, q], late.at[:, pl.ds((t - SENT_TILES + LATE_TILES) * TILE, TILE)], gr_send.at[slot, q]).start()

        repeat(2, half)

    def out_loads(k, slot):
        return [local(lhs_u.at[q, pl.ds(k * QUARTER, QUARTER)], dd.at[slot, q], o_sem.at[slot, q]) for q in PAIR]

    def out_store(n, k, slot):
        return local(wo_out.at[slot], dwo.at[pl.ds(k * QUARTER, QUARTER), pl.ds(n * WIDE, WIDE)], o_sem.at[slot, 2])

    def e_loads(n):
        return [local(rhs_e.at[q, :, :, :, :, pl.ds(n * WIDE, WIDE)], ecol.at[q], e_sem.at[q]) for q in PAIR]

    def out_tile(n):
        wait_all(e_loads(n))

        def quarter(k):
            slot = k % 2

            @pl.when(k < 3)
            def _():
                start_all(out_loads(k + ONE, ONE - slot))

            wait_all(out_loads(k, slot))

            @pl.when(4 * n + k >= 2)
            def _():
                out_store(n, k, slot).wait()

            wo_out[slot] = mm(dd[slot, ZERO], ecol[ZERO].reshape(WIDTH, WIDE), ZERO) + mm(dd[slot, ONE], ecol[ONE].reshape(WIDTH, WIDE), ZERO)
            out_store(n, k, slot).start()

        repeat(4, quarter)

    barrier = pltpu.get_barrier_semaphore()
    for dev in (reds[ZERO], nons[ZERO], twin, (y_chip, other)):
        pl.semaphore_signal(barrier, inc=ONE, device_id=dev, device_id_type=MESH)
    pl.semaphore_wait(barrier, 4)

    for block in PAIR:
        wo_hand(block)
    per_mtx(lambda mtx: w_hand(ONE - mtx if mtx == ZERO else ZERO).start())

    def given(arr, i):
        return arr.at[i, pl.ds(core * ROWS, ROWS)]

    spots = [[ab.at[n, i // 2, i % 2] for i in range(CHUNKS)] for n in PAIR]
    run_all([local(given(arr, i), spots[n][i], b_sem.at[n, i // 2, i % 2]) for n, arr in enumerate((x, g)) for i in range(CHUNKS)])
    for hi in PAIR:
        for lo in PAIR:
            cols = pl.ds((2 * hi + lo) * QUARTER, QUARTER)
            run_all([local(spots[n][i].at[:, cols], act.at[kind, hi, lo, i, ZERO, ZERO], b_sem.at[n, i // 2, i % 2]) for n, kind in enumerate((X, G)) for i in range(CHUNKS)])

    start_all(in_first(X, ZERO))

    @pl.when(core == ZERO)
    def _():
        for to_red in (ONE, ZERO):
            w_start(ZERO, to_red)

    w_hand(ZERO).wait_recv()

    @pl.when(core == ONE)
    def _():
        for to_red in (ONE, ZERO):
            w_start(ZERO, to_red)

    for i in range(ONE, CHUNKS):
        start_all(in_first(X, i))

    @per_mtx
    def _(mtx):
        for block in PAIR:
            run_all([local(w_src(mtx, block).at[:, f_cols(block, rs[block], fq)], dd.at[ZERO, fq], o_sem.at[ZERO, fq]) for fq in PAIR])
            run_all([local(dd.at[ZERO, fq], w_rows(mtx, block, fq, chip), o_sem.at[ZERO, fq]) for fq in PAIR])
        rows = [pl.ds(k * QUARTER, QUARTER) for k in range(4)]
        run_all([local(wo_in.at[rows[k]], dd.at[k // 2, k % 2], o_sem.at[k // 2, k % 2]) for k in range(4)])
        run_all([local(dd.at[k // 2, k % 2], wo.at[mtx, cs[mtx], rows[k]], o_sem.at[k // 2, k % 2]) for k in range(4)])

    pass_on(in_first(X, ZERO), in_second(X, ZERO))
    for fq in PAIR:
        w_pass(ZERO, fq)
    for i in range(ONE, CHUNKS):
        pass_on(in_first(X, i), in_second(X, i))
    wo_start(ONE)
    wo_start(ZERO)
    w_start(ONE, ZERO)

    @pl.when(core == ZERO)
    def _():
        w_start(ONE, ONE)

    for fq in PAIR:
        w_end(ZERO, fq)
    w_arrived(ZERO)

    def when_forward(tick):
        def run(body):
            @pl.when((tick >= ZERO) & (tick < CHUNKS))
            def _():
                body(tick)
        return run

    def in_two_parts(offset, late):
        def run(body):
            @pl.when(((offset >= ZERO) & (offset < 2)) | ((offset >= late) & (offset < late + 2)))
            def _():
                body(jnp.where(offset < 2, offset, offset - late + 2))
        return run

    def tick_step(tick):
        for n in PAIR:
            @pl.when(tick == n)
            def _(n=n):
                for i in PAIR:
                    start_all(in_first(G, 2 * n + i))

        @pl.when(tick == CHUNKS)
        def _():
            wo_pass(ONE)
            wo_arrived(ONE)

        @pl.when(tick == BACK_AT)
        def _():
            w_arrived(ONE)

        when_forward(tick)(forward)

        @pl.when((tick >= CHUNKS) & (tick < BACK_AT))
        def _():
            hidden_cotangent(tick - CHUNKS)

        @pl.when((tick >= BACK_AT) & (tick < GRADS_AT))
        def _():
            backward(tick - CHUNKS)

        @pl.when(tick >= GRADS_AT)
        def _():
            grad_tile(tick - GRADS_AT)

        grad = tick - GRADS_AT

        @pl.when((grad >= OUT_AT - 2) & ((grad - OUT_AT + 2) % OUT_EVERY == ZERO) & (grad < OUT_AT + 4 * OUT_EVERY - 2))
        def _():
            start_all(e_loads((grad - OUT_AT + 2) // OUT_EVERY) + out_loads(ZERO, ZERO))

        @pl.when((grad >= OUT_AT) & ((grad - OUT_AT) % OUT_EVERY == ZERO))
        def _():
            out_tile((grad - OUT_AT) // OUT_EVERY)

        @in_two_parts(tick - PASS_H1, BACK_AT + ONE - PASS_H1)
        def _(i):
            pass_on(out_first(ZERO, i), out_second(ZERO, i))

        @pl.when((tick >= BACK_AT + 3) & (tick < BACK_AT + 3 + CHUNKS))
        def _():
            i = tick - BACK_AT - 3
            pass_on(out_first(ONE, i), out_second(ONE, i))

        last_give = tick == GRADS_AT + 2 * LAG

        @pl.when(((tick >= BACK_AT + 2) & (tick < GRADS_AT + ONE)) | last_give)
        def _():
            rs_give(jnp.where(last_give, TASKS - ONE, tick - CHUNKS - 2))

        in_two_parts(tick - TAKE_H1, BACK_AT - TAKE_H1)(rs_take)

        @pl.when((tick >= BACK_AT) & (tick < GRADS_AT))
        def _():
            start_all(back_loads((tick // CHUNKS + ONE) % 2, ZERO, ZERO))

        last_take = tick == GRADS_AT + LAG

        @pl.when(((tick >= BACK_AT + ONE) & (tick < GRADS_AT)) | last_take)
        def _():
            rs_take(jnp.where(last_take, TASKS - ONE, tick - CHUNKS - ONE))

        @pl.when(tick == ONE)
        def _():
            wo_pass(ZERO)
            wo_arrived(ZERO)

            @pl.when(core == ONE)
            def _():
                w_start(ONE, ONE)

        when_forward(tick - ONE)(forward_out)

        for n in PAIR:
            @pl.when(tick == 3 + n)
            def _(n=n):
                for i in PAIR:
                    pass_on(in_first(G, 2 * n + i), in_second(G, 2 * n + i))

            @pl.when(tick == W_PASS[n])
            def _(n=n):
                w_pass(ONE, n)

            @pl.when(tick == W_END[n])
            def _(n=n):
                w_end(ONE, n)

        @pl.when((tick >= BACK_AT) & (tick < GRADS_AT))
        def _():
            backward_out(tick - CHUNKS)

    repeat(GRADS_AT + SENT_TILES, tick_step)

    for m, dst in enumerate((dwg, dwi)):
        for fq in PAIR:
            arrived(dst.at[:, pl.ds(pick((ONE - cx + 2 * fq, 2 * (ONE - cy) + fq), core) * WIDTH, WIDTH - m * fq * LATE_TILES * TILE)], gr_recv.at[m, fq])
    for slot in range(SLOTS):
        grad_sent(slot)
    for slot in PAIR:
        out_store(ZERO, ZERO, slot).wait()
    for i in range(CHUNKS):
        all_recv(dx_copies(i, ZERO)[ONE:])
    for i in (CHUNKS - 2, CHUNKS - ONE):
        dx_sent(i)

    def sent(copies):
        for copy in copies:
            copy.wait_send()

    for i in range(CHUNKS):
        for kind in (X, G):
            sent([*in_first(kind, i), *in_second(kind, i)])
        for block in PAIR:
            sent(out_first(block, i) + out_second(block, i))
    repeat(TASKS, lambda task: rs_copy(task).wait_send())
    for task in (TASKS - 2, TASKS - ONE):
        sent(dot_copies(task))
    for block in PAIR:
        for fq in PAIR:
            sent(w_first(ZERO, block, fq) + (w_second(ZERO, block, fq),))
            sent(w_twin(ZERO, block, fq))
    for k in range(4):
        for block in PAIR:
            @pl.when(core == block)
            def _(block=block, k=k):
                wo_copies(block, k)[ZERO].wait_send()

    def wo_sent(k):
        for block in PAIR:
            sent((wo_copies(block, k)[ONE], wo_copies(block, k)[3]))

    halves(wo_sent)
    w_hand(ZERO).wait_send()


def settle_kernel(*refs):
    for src, dst in zip(refs[:4], refs[4:]):
        dst[...] = src[...]


def settle(arrays, steps=16):
    specs = [pl.BlockSpec((arr.shape[0] // steps, arr.shape[1]), lambda i: (i, 0)) for arr in arrays]
    size = sum(arr.size * arr.dtype.itemsize for arr in arrays)
    return pl.pallas_call(
        settle_kernel, grid=(steps,), out_shape=[jax.ShapeDtypeStruct(arr.shape, arr.dtype) for arr in arrays], in_specs=specs, out_specs=specs,
        name='settle', cost_estimate=pl.CostEstimate(flops=2 ** 30, bytes_accessed=2 * size, transcendentals=0),
        compiler_params=pltpu.CompilerParams(vmem_limit_bytes=67_043_328),
    )(*arrays)


def insert_kernel(spot, late, whole, out):
    out[...] = late[...]


def insert_late(whole, late, spot):
    block = (QUARTER, QUARTER)
    return pl.pallas_call(
        insert_kernel, out_shape=jax.ShapeDtypeStruct(whole.shape, whole.dtype),
        grid_spec=pltpu.PrefetchScalarGridSpec(
            num_scalar_prefetch=1, grid=(3,), in_specs=[pl.BlockSpec(block, lambda k, spot: (0, k)), pl.BlockSpec(memory_space=pl.ANY)],
            out_specs=pl.BlockSpec(block, lambda k, spot: (0, 4 * spot[0] + 1 + k))),
        input_output_aliases={2: 0}, name='insert_late',
    )(spot, late, whole)


def solution(mesh):
    act_spec = P(None, 'data', None, None)
    weight_spec = P('stage', None, 'data', None)

    def per_device(x, g, w_gate, w_in, w_out):
        flat = (CHUNKS, 2 * ROWS, WIDTH)
        any_space = pl.BlockSpec(memory_space=pl.ANY)
        pair = (2, 2)

        def arr(*shape, dtype=BF16):
            return jax.ShapeDtypeStruct(shape, dtype)

        def f32(*shape):
            return arr(*shape, dtype=F32)

        piece = (*pair, ROWS, QUARTER)
        out_shapes = [
            arr(*flat), f32(QUARTER, 4 * WIDTH), f32(QUARTER, 4 * WIDTH), f32(WIDTH, WIDTH), f32(QUARTER, LATE_TILES * TILE),
            arr(4, *pair, CHUNKS, *pair, ROWS, QUARTER), *[arr(*pair, WIDTH, WIDTH)] * 3, arr(QUARTER, 4 * WIDTH),
            f32(TASKS, 2, *piece), f32(TASKS, *piece), f32(2 * CHUNKS, 2, ROWS, ROWS), f32(3, CHUNKS, HIDDEN_TILES, BLOCK_ROWS, WIDE),
            arr(2, SUM_TILES, TILE, WIDTH), arr(2, WIDTH, WIDTH), arr(*pair, 2, WIDTH, WIDTH), arr(2, CHUNKS, *pair, ROWS, WIDTH),
        ]

        def bf(*shape):
            return pltpu.VMEM(shape, BF16)

        def fl(*shape):
            return pltpu.VMEM(shape, F32)

        scratch = [
            bf(*pair, WIDTH, WIDE), bf(2, 4, TILE, WIDTH), fl(*pair, BLOCK_ROWS, WIDE), bf(2, *pair, ROWS, WIDTH), bf(*pair, BLOCK_ROWS, WIDTH),
            bf(SUM_TILES, TILE, BLOCK_ROWS), bf(WIDTH, BLOCK_ROWS), bf(BLOCK_ROWS, WIDE), fl(2, *pair, ROWS, TILE), fl(2, *piece), fl(2, *piece), bf(3, *piece),
            fl(2, 2, ROWS, ROWS), bf(2, *piece), bf(2, 2, ROWS, HALF), bf(2, CHUNKS, *pair, ROWS, WIDE), fl(SLOTS, 2, QUARTER, TILE), fl(2, QUARTER, WIDE),
        ]
        counts = [(4, CHUNKS, 8), (4, CHUNKS, 8), (TASKS,), (TASKS,), (2 * CHUNKS, 2), (2 * CHUNKS, 2), (*pair, 3), (*pair, 3), (*pair, 4), (*pair, 4),
                  (1,), (1,), (2, 3, 4), (2, 3, 4), (5,), (CHUNKS, 5), (CHUNKS, 4), (CHUNKS, 3), (SLOTS, 2), pair, (2,), (4,), (2, 4), pair, (2, *pair), (2, 3), (2,)]
        results = pl.pallas_call(
            step_kernel, out_shape=out_shapes, in_specs=[any_space] * 5, out_specs=[any_space] * len(out_shapes),
            scratch_shapes=scratch + [pltpu.SemaphoreType.DMA(count) for count in counts], name='mlp_step',
            compiler_params=pltpu.CompilerParams(collective_id=0, has_side_effects=True, vmem_limit_bytes=67_043_328),
        )(x.reshape(flat), g.reshape(flat), w_gate[0, 0], w_in[0, 0], w_out[0, 0])
        late = lax.ppermute(results[4], ('data', 'stage'), [(2 * c + s, 2 * (c ^ (1 + s)) + s) for c in range(4) for s in PAIR])
        chip, core = lax.axis_index('data'), lax.axis_index('stage')
        spot = jnp.where(core == 0, 3 - chip % 2, 3 - 2 * (chip // 2))
        dx, d_gate, d_in, d_out = settle((results[0].reshape(-1, WIDTH), *results[1:4]))
        d_in = insert_late(d_in, late, spot.astype(jnp.int32).reshape(1))
        return dx.reshape(x.shape), d_gate[None, None], d_in[None, None], d_out[None, None]

    return jax.shard_map(per_device, mesh=mesh, in_specs=(act_spec, act_spec, weight_spec, weight_spec, weight_spec),
                         out_specs=(act_spec, weight_spec, weight_spec, weight_spec), check_vma=False)
```

```python
import jax
import jax.numpy as jnp
from jax import lax
from jax.experimental import pallas as pl
from jax.experimental.pallas import tpu as pltpu
from jax.sharding import PartitionSpec as P

MESH = pl.DeviceIdType.MESH
F32 = jnp.float32
BF16 = jnp.bfloat16
EPS = 1e-6

CHUNKS = 4
ROWS = 128
BLOCK_ROWS = 4 * ROWS
WIDTH = 2048
HALF = WIDTH // 2
QUARTER = WIDTH // 4
TILE = 256
TILES = WIDTH // TILE
WIDE = 2 * TILE
WIDES = WIDTH // WIDE
PART = BLOCK_ROWS // 2
HIDDEN_TILES = 2 * WIDES
SUM_TILES = HALF // TILE
TASKS = 3 * CHUNKS
BACK_AT = 2 * CHUNKS
GRADS_AT = 4 * CHUNKS
SENT_TILES = 4 * TILES
SLOTS = 4
OUT_AT, OUT_EVERY = 8, 7
LATE_TILES = 6
LAG = 6
W_PASS, W_END = (2, 3), (7, 7)
TAKE_H1, PASS_H1 = 4, 6
PAIR = ZERO, ONE = range(2)
X, H1, G, E1 = range(4)


def mm(lhs, rhs, rhs_dim):
    return lax.dot_general(lhs, rhs, (((1,), (rhs_dim,)), ((), ())), preferred_element_type=F32)


def repeat(count, body):
    def step(n, carry):
        body(n)
        return carry

    lax.fori_loop(0, count, step, 0)


def start_all(copies):
    for copy in copies:
        copy.start()


def wait_all(copies):
    for copy in copies:
        copy.wait()


def run_all(copies):
    start_all(copies)
    wait_all(copies)


def step_kernel(x, g, wg_in, wi_in, wo_in,
                dx, dwg, dwi, dwo, late, act, wg, wi, wo, wx, part, rb, dots, kept, lhs_n, lhs_u, rhs_d, rhs_e,
                wcol, wrow, fab, ab, dd, ntb, utb, utw, pst, ld, tot, own, dsv, new, dxn, ecol, outs, wo_out,
                ag_send, ag_recv, rs_send, rs_recv, dt_send, dt_recv, w_send, w_recv, f_send, f_recv, h_send, h_recv, wo_send, wo_recv,
                op_send, op_recv, dx_send, dx_recv, gr_send, gr_recv, p_sem, l_sem, g_sem, s_sem, k_sem, b_sem, o_sem, e_sem):
    chip = lax.axis_index('data')
    core = lax.axis_index('stage')
    cx, cy = chip % 2, chip // 2
    other = ONE - core
    x_chip, y_chip = cy * 2 + (ONE - cx), (ONE - cy) * 2 + cx
    twin = (chip, other)
    reds, nons = ((x_chip, core), (y_chip, core)), ((y_chip, core), (x_chip, core))
    rs, cs = (cx, cy), (cy, cx)

    def pick(pair, block):
        return pair[ZERO] + (pair[ONE] - pair[ZERO]) * block

    def red_of(block):
        return pick((x_chip, y_chip), block), core

    def local(src, dst, sem):
        return pltpu.make_async_copy(src, dst, sem)

    def remote(src, dst, send, recv, dev):
        return pltpu.make_async_remote_copy(src_ref=src, dst_ref=dst, send_sem=send, recv_sem=recv, device_id=dev, device_id_type=MESH)

    def arrived(ref, sem):
        local(ref, ref, sem).wait()

    def in_first(kind, i):
        block = kind // G
        mine = act.at[kind, :, :, i, ZERO, ZERO]
        return (remote(mine, act.at[kind, :, :, i, ONE, ZERO], ag_send.at[kind, i, ZERO], ag_recv.at[kind, i, ZERO], reds[block]),
                remote(mine, act.at[kind, :, :, i, ZERO, ONE], ag_send.at[kind, i, ONE], ag_recv.at[kind, i, ONE], nons[block]))

    def in_second(kind, i):
        block = kind // G
        sends = [remote(act.at[kind, :2 - (kind == X), :, i, ZERO, ONE], act.at[kind, :2 - (kind == X), :, i, ONE, ONE], ag_send.at[kind, i, 2], ag_recv.at[kind, i, 2], reds[block])]
        if kind == X:
            sends.append(remote(act.at[kind, ONE, :, i, ONE, ZERO], act.at[kind, ONE, :, i, ONE, ONE], ag_send.at[kind, i, 3], ag_recv.at[kind, i, 3], nons[block]))
        return sends

    def out_first(block, i):
        kind, c = (H1, E1)[block], cs[block]
        sends = [remote(act.at[kind, c, :, i, :, ZERO], act.at[kind, c, :, i, :, ONE], ag_send.at[kind, i, ZERO], ag_recv.at[kind, i, ZERO], reds[block])]
        for a in PAIR:
            sends.append(remote(act.at[kind, c, :, i, a, ZERO], act.at[kind, c, :, i, ONE - a, ZERO], ag_send.at[kind, i, ONE + a], ag_recv.at[kind, i, 2 - a], nons[block]))
        return sends

    def out_second(block, i):
        kind, c = (H1, E1)[block], cs[block]
        if block:
            came, spot = act.at[kind, ONE - c, :, i, :, ZERO], act.at[kind, ONE - c, :, i, :, ONE]
            return [remote(came, spot, ag_send.at[kind, i, 3], ag_recv.at[kind, i, 3], reds[block])]
        return [remote(act.at[kind, c, h, i, a, ONE], act.at[kind, c, h, i, ONE - a, ONE], ag_send.at[kind, i, 4 + 2 * a + h], ag_recv.at[kind, i, 6 - 2 * a + h], nons[block])
                for a in PAIR for h in PAIR]

    def pass_on(first, second):
        for copy in first:
            copy.wait_recv()
        start_all(second)

    def all_recv(copies):
        for copy in copies:
            copy.wait_recv()

    def rs_copy(task):
        return remote(part.at[task, :, ONE], rb.at[task], rs_send.at[task], rs_recv.at[task], red_of((task // CHUNKS) % 2))

    def dot_copies(task):
        slot, n = task % 2, task - CHUNKS
        dev = pick((y_chip, x_chip), (task // CHUNKS) % 2), core
        return [remote(dsv.at[slot, b], dots.at[n, ONE - b], dt_send.at[n, b], dt_recv.at[n, ONE - b], dev) for b in PAIR]

    def own_half(kind_h, block, i):
        if block == ZERO:
            return act.at[X, cy, :, i, ZERO] if kind_h else act.at[E1, :, cy, i, ZERO]
        return act.at[H1, :, cx, i, ZERO] if kind_h else act.at[G, :, cx, i, ZERO]

    def rest_half(block, i):
        return act.at[X, ONE - cy, :, i, ZERO] if block == ZERO else act.at[H1, :, ONE - cx, i, ZERO]

    def when_kind(task):
        def run(body):
            for kind in range(3):
                @pl.when(task // CHUNKS == kind)
                def _(kind=kind):
                    body(kind)
        return run

    def send_result(block, i, slot):
        run_all([local(new.at[slot], act.at[(H1, E1)[block], cs[block], :, i, :, ZERO], l_sem.at[ZERO])])
        start_all(out_first(block, i))

    def pieces(body):
        def step(n):
            body(n // 2, n % 2, pl.ds(ZERO, ROWS))
        repeat(4, step)

    def rs_take(task):
        i, slot = task % CHUNKS, task % 2
        rs_copy(task).wait_recv()
        start_all([local(part.at[task, :, ZERO], ld.at[ZERO], l_sem.at[ZERO]), local(rb.at[task], ld.at[ONE], l_sem.at[ONE])])

        @when_kind(task)
        def _(kind):
            local(own_half(True, kind % 2, i), own.at[ZERO], l_sem.at[2]).start()

        wait_all([local(rb.at[task], ld.at[ZERO], l_sem.at[ZERO]), local(rb.at[task], ld.at[ONE], l_sem.at[ONE]), local(own_half(True, ZERO, i), own.at[ZERO], l_sem.at[2])])

        @pl.when(task < CHUNKS)
        def _():
            @pieces
            def _(q, b, rows):
                new[slot, q, b, rows, :] = own[ZERO, q, b, rows, :] + (ld[ZERO, q, b, rows, :] + ld[ONE, q, b, rows, :]).astype(BF16)

            send_result(ZERO, i, slot)

        @pl.when(task >= CHUNKS)
        def _():
            @pl.when(task >= CHUNKS + 2)
            def _():
                for copy in dot_copies(task - 2):
                    copy.wait_send()

            @pieces
            def _(q, b, rows):
                total = ld[ZERO, q, b, rows, :] + ld[ONE, q, b, rows, :]
                tot[slot, q, b, rows, :] = total
                dot = jnp.sum(total * own[ZERO, q, b, rows, :].astype(F32), axis=-ONE, keepdims=True) + jnp.zeros((ONE, ROWS), F32)

                @pl.when(q == ZERO)
                def _():
                    dsv[slot, b, rows, :] = dot

                @pl.when(q == ONE)
                def _():
                    dsv[slot, b, rows, :] = dsv[slot, b, rows, :] + dot

            start_all(dot_copies(task))

    def dx_copies(i, slot):
        spot = dx.at[i, pl.ds(core * ROWS, ROWS), pl.ds(cy * HALF, HALF)]
        return (local(dxn.at[slot, ZERO], spot, dx_send.at[i, ZERO]), remote(dxn.at[slot, ZERO], spot, dx_send.at[i, ONE], dx_recv.at[i, ZERO], twin),
                remote(dxn.at[slot, ONE], spot, dx_send.at[i, 2], dx_recv.at[i, ONE], (y_chip, core)),
                remote(dxn.at[slot, ONE], spot, dx_send.at[i, 3], dx_recv.at[i, 2], (y_chip, other)))

    def dx_sent(i):
        copies = dx_copies(i, i % 2)
        copies[ZERO].wait()
        for copy in copies[ONE:]:
            copy.wait_send()

    def give_loads(task):
        for block in PAIR:
            @pl.when((task // CHUNKS) % 2 == block)
            def _(block=block):
                i = task % CHUNKS
                start_all([local(src, own.at[n], g_sem.at[n]) for n, src in enumerate((own_half(True, block, i), own_half(False, block, i), rest_half(block, i)))])

    def rs_give(task):
        i, slot = task % CHUNKS, task % 2
        for b in PAIR:
            arrived(dots.at[task - CHUNKS, b], dt_recv.at[task - CHUNKS, b])
        local(dots.at[task - CHUNKS], ld.at[ZERO, ZERO, :, :, pl.ds(ZERO, ROWS)], l_sem.at[3]).start()
        wait_all([local(own_half(True, ZERO, i), own.at[n], g_sem.at[n]) for n in range(3)])
        local(dots.at[task - CHUNKS], ld.at[ZERO, ZERO, :, :, pl.ds(ZERO, ROWS)], l_sem.at[3]).wait()

        @pl.when(task >= 2 * CHUNKS + 2)
        def _():
            dx_sent(i - 2)

        def step(n):
            b, rows = n // 2, pl.ds((n % 2) * (ROWS // 2), ROWS // 2)

            def sq(slot_of, q):
                vals = own[slot_of, q, b, rows, :].astype(F32)
                return jnp.sum(vals * vals, axis=-ONE, keepdims=True)

            square = sq(ZERO, ZERO) + sq(ZERO, ONE) + sq(2, ZERO) + sq(2, ONE)
            inv = lax.rsqrt(square / WIDTH + EPS)
            dot = (dsv[slot, b, rows, ZERO:ONE] + ld[ZERO, ZERO, b, rows, ZERO:ONE]) / WIDTH
            for q in PAIR:
                tok = own[ZERO, q, b, rows, :].astype(F32)
                resid = tot[slot, q, b, rows, :] * inv - tok * (inv * inv * inv * dot)
                val = (own[ONE, q, b, rows, :].astype(F32) + resid).astype(BF16)
                new[slot, q, b, rows, :] = val
                dxn[slot, b, rows, pl.ds(q * QUARTER, QUARTER)] = val

        repeat(4, step)

        @pl.when(task < 2 * CHUNKS)
        def _():
            send_result(ONE, i, slot)

        @pl.when(task >= 2 * CHUNKS)
        def _():
            start_all(dx_copies(i, slot))

    def f_cols(block, place, fq):
        quarter = place + 2 * fq if block == ZERO else 2 * place + fq
        return pl.ds(quarter * WIDTH, WIDTH)

    def w_src(mtx, block):
        return ((wg_in, wx), (wx, wi_in))[mtx][block]

    def w_rows(mtx, block, fq, of):
        return (wg, wi)[mtx].at[block, fq, pl.ds(of * QUARTER, QUARTER)]

    def w_first(mtx, block, fq):
        src, mine = w_src(mtx, block), w_rows(mtx, block, fq, chip)
        return (remote(src.at[:, f_cols(block, rs[block], fq)], mine, w_send.at[block, fq, ZERO], w_recv.at[block, fq, ZERO], nons[block]),
                remote(src.at[:, f_cols(block, ONE - rs[block], fq)], mine, w_send.at[block, fq, ONE], w_recv.at[block, fq, ONE], reds[block]))

    def w_second(mtx, block, fq):
        piece = w_rows(mtx, block, fq, reds[block][ZERO])
        return remote(piece, piece, w_send.at[block, fq, 2], w_recv.at[block, fq, 2], nons[block])

    def w_twin(mtx, block, fq):
        far = 3 - chip
        srcs = [w_src(mtx, block).at[:, f_cols(block, rs[block], fq)]] + [w_rows(mtx, block, fq, of) for of in (nons[block][ZERO], reds[block][ZERO], far)]
        spots = [w_rows(mtx, block, fq, of) for of in (chip, nons[block][ZERO], reds[block][ZERO], far)]
        return [remote(src, spot, f_send.at[block, fq, n], f_recv.at[block, fq, n], twin) for n, (src, spot) in enumerate(zip(srcs, spots))]

    def per_mtx(body):
        for mtx in PAIR:
            @pl.when(core == mtx)
            def _(mtx=mtx):
                body(mtx)

    def w_start(block, to_red):
        @per_mtx
        def _(mtx):
            for fq in PAIR:
                w_first(mtx, block, fq)[to_red].start()
                if not to_red:
                    w_twin(mtx, block, fq)[ZERO].start()

    def w_pass(block, fq):
        @per_mtx
        def _(mtx):
            first, to_twin = w_first(mtx, block, fq), w_twin(mtx, block, fq)
            first[ONE].wait_recv()
            w_second(mtx, block, fq).start()
            to_twin[2].start()
            first[ZERO].wait_recv()
            to_twin[ONE].start()

    def w_end(block, fq):
        @per_mtx
        def _(mtx):
            w_second(mtx, block, fq).wait_recv()
            w_twin(mtx, block, fq)[3].start()

    def w_arrived(block):
        for fq in PAIR:
            all_recv(w_twin(ZERO, block, fq))

    def w_hand(mtx):
        return remote((wg_in, wi_in)[mtx], wx, h_send.at[ZERO], h_recv.at[ZERO], twin)

    def wo_copies(block, k):
        rows = pl.ds(k * QUARTER, QUARTER)
        spot, got = wo.at[block, cs[block], rows], wo.at[block, ONE - cs[block], rows]
        return (remote(wo_in.at[rows], spot, wo_send.at[block, ZERO, k], wo_recv.at[block, ZERO, k], twin),
                remote(wo_in.at[rows], spot, wo_send.at[block, ONE, k], wo_recv.at[block, ONE, k], nons[block]),
                remote(spot, spot, wo_send.at[block, ONE, k], wo_recv.at[block, ONE, k], nons[block]),
                remote(got, got, wo_send.at[block, 2, k], wo_recv.at[block, 2, k], twin))

    def halves(body):
        for half in PAIR:
            @pl.when(core == half)
            def _(half=half):
                for k in (2 * half, 2 * half + ONE):
                    body(k)

    def wo_hand(block):
        @pl.when(core == block)
        def _():
            for k in range(4):
                wo_copies(block, k)[ZERO].start()

    def wo_start(block):
        @pl.when(core == block)
        def _():
            for k in (2 * block, 2 * block + ONE):
                wo_copies(block, k)[ONE].start()

        @pl.when(core != block)
        def _():
            for k in range(4):
                wo_copies(block, k)[ZERO].wait_recv()
            for k in (2 - 2 * block, 3 - 2 * block):
                wo_copies(block, k)[2].start()

    def wo_pass(block):
        def body(k):
            wo_copies(block, k)[ONE].wait_recv()
            wo_copies(block, k)[3].start()
        halves(body)

    def wo_arrived(block):
        def body(k):
            wo_copies(block, 3 - k)[3].wait_recv()
        halves(body)

    def op_pairs(i, src):
        cols = pl.ds(i * BLOCK_ROWS, BLOCK_ROWS)
        return ((ntb, lhs_n.at[src, :, :, cols]), (utb, lhs_u.at[src, :, cols]), (dd.at[ZERO], rhs_d.at[ZERO, :, src, cols]),
                (dd.at[ONE], rhs_d.at[ONE, :, src, cols]), (ab.at[ONE], rhs_e.at[src, i]))

    def op_start(n, i, block):
        src, dst = op_pairs(i, core)[n]

        @pl.when(block == core)
        def _():
            local(src, dst, op_send.at[n]).start()

        @pl.when(block != core)
        def _():
            remote(src, dst, op_send.at[n], op_recv.at[i, n], twin).start()

    def op_sent(i, which):
        for n in which:
            local(*op_pairs(i, core)[n], op_send.at[n]).wait()

    def op_arrived(i):
        all_recv([remote(src, dst, op_send.at[n], op_recv.at[i, n], twin) for n, (src, dst) in enumerate(op_pairs(i, other))])

    def load_tokens(kind, i, slot):
        copies = []
        for hi in PAIR:
            for lo in PAIR:
                src = act.at[kind, lo, hi, i] if kind == E1 else act.at[kind, hi, lo, i]
                copies.append(local(src, ab.at[slot, :, :, :, pl.ds((2 * hi + lo) * QUARTER, QUARTER)], b_sem.at[slot, hi, lo]))
        return copies

    def tokens(slot):
        return ab[slot].reshape(BLOCK_ROWS, WIDTH)

    def normalize():
        def step(n):
            a, b, rows = n // 4, (n // 2) % 2, pl.ds((n % 2) * (ROWS // 2), ROWS // 2)
            tok = ab[ZERO, a, b, rows, :].astype(F32)
            inv = lax.rsqrt(jnp.mean(tok * tok, axis=-ONE, keepdims=True) + EPS)
            ab[ZERO, a, b, rows, :] = (tok * inv).astype(BF16)

        repeat(2 * 4, step)

    def stream(count, loads, body, started=False):
        if not started:
            start_all(loads(ZERO, ZERO))

        def step(n):
            slot = n % 2

            @pl.when(n + ONE < count)
            def _():
                start_all(loads(n + ONE, ONE - slot))

            wait_all(loads(n, slot))
            body(n, slot)

        repeat(count, step)

    def col_tile(n):
        return pl.ds((n % TILES) * TILE, TILE)

    def narrow(slot, n):
        return wcol.at[slot, n, :, pl.ds(ZERO, TILE)]

    def wide(n):
        return pl.ds((n % WIDES) * WIDE, WIDE)

    def w_cols(block, n, slot):
        return [local(src.at[block, n // WIDES, :, wide(n)], wcol.at[slot, m], s_sem.at[slot, m]) for m, src in enumerate((wg, wi))]

    def wo_rows(block, n, slot):
        return [local(wo.at[block, n // WIDES, pl.ds((n % WIDES) * WIDE + h * TILE, TILE)], wrow.at[slot, h], s_sem.at[slot, 2 + h]) for h in PAIR]

    def wo_tile(slot):
        return wrow[slot, ZERO:2].reshape(WIDE, WIDTH)

    def kept_load(which, i, n, slot):
        return local(kept.at[which, i, n], fab.at[which % 2, slot], k_sem.at[which % 2, slot])

    def kept_store(which, i, n, slot):
        return local(fab.at[which % 2, slot], kept.at[which, i, n], k_sem.at[which % 2, slot])

    def sum_cols(block, n):
        quarter = pick((2 * cy + n // 2, cx + 2 * (n // 2)), block)
        return pl.ds(quarter * QUARTER + (n % 2) * TILE, TILE)

    def sum_store(task, n, slot):
        return local(pst.at[slot], part.at[task, n // 2, :, :, :, pl.ds((n % 2) * TILE, TILE)], p_sem.at[slot])

    def write_sums(task, loads, product, started=False):
        def body(n, slot):
            @pl.when(n >= 2)
            def _():
                sum_store(task, n - 2, slot).wait()

            pst[slot] = product(slot).reshape(2, 2, ROWS, TILE)
            sum_store(task, n, slot).start()

        stream(SUM_TILES, loads, body, started)
        for slot in PAIR:
            sum_store(task, slot, slot).wait()
        rs_copy(task).start()

    def forward(i):
        all_recv(in_second(X, i))
        run_all(load_tokens(X, i, ZERO))
        normalize()

        @pl.when(i > ZERO)
        def _():
            op_sent(i, PAIR)

        turn_tokens(i, ZERO)

        def body(n, slot):
            pre_gate = mm(tokens(ZERO), wcol[slot, ZERO], ZERO)
            pre_in = mm(tokens(ZERO), wcol[slot, ONE], ZERO)

            @pl.when(n >= 2)
            def _():
                wait_all([kept_store(m, i, n - 2, slot) for m in PAIR])

            fab[ZERO, slot] = pre_gate
            fab[ONE, slot] = pre_in
            start_all([kept_store(m, i, n, slot) for m in PAIR])
            hidden = (pre_gate * jax.nn.sigmoid(pre_gate) * pre_in).astype(BF16)
            dd[i % 2, n // WIDES, :, wide(n)] = hidden
            keep_u(n, cy, hidden)

        stream(HIDDEN_TILES, lambda n, slot: w_cols(ZERO, n, slot), body)
        wait_all([kept_store(m, i, slot, slot) for m in PAIR for slot in PAIR])
        op_start(ONE, i, ZERO)

    def forward_out(i):
        def loads(n, slot):
            return [local(wo.at[ZERO, fq, :, sum_cols(ZERO, n)], narrow(slot, fq), s_sem.at[slot, fq]) for fq in PAIR]

        write_sums(i, loads, lambda slot: mm(dd[i % 2, ZERO], narrow(slot, ZERO)[...], ZERO) + mm(dd[i % 2, ONE], narrow(slot, ONE)[...], ZERO))

    def hidden_cotangent(i):
        all_recv(in_second(G, i))
        run_all(load_tokens(G, i, ONE))

        def body(n, slot):
            d_hidden = mm(tokens(ONE), wo_tile(slot), ONE)

            @pl.when(n >= 2)
            def _():
                kept_store(2, i, n - 2, slot).wait()

            fab[ZERO, slot] = d_hidden
            kept_store(2, i, n, slot).start()

        stream(HIDDEN_TILES, lambda n, slot: wo_rows(ONE, n, slot), body)
        wait_all([kept_store(2, i, slot, slot) for slot in PAIR])

    def gradients_of(n, h, pre_gate, pre_in, d_hidden):
        rows = pl.ds(h * PART, PART)
        sigma = jax.nn.sigmoid(pre_gate)
        gate_act = pre_gate * sigma
        dd[ZERO, n // WIDES, rows, wide(n)] = (d_hidden * pre_in * sigma * (1.0 + pre_gate * (1.0 - sigma))).astype(BF16)
        dd[ONE, n // WIDES, rows, wide(n)] = (d_hidden * gate_act).astype(BF16)
        return gate_act

    def keep_u(n, keeps_u, hidden):
        @pl.when(n // WIDES == keeps_u)
        def _():
            utb[wide(n), :] = hidden.T

    def turn_tokens(i, block):
        def turn(n):
            ntb[n] = ab[ZERO, :, :, :, sum_cols(block, n)].reshape(BLOCK_ROWS, TILE).T

        repeat(SUM_TILES, turn)
        op_start(ZERO, i, block)

    def part_of(slot, h):
        return ab[slot, h].reshape(PART, WIDTH)

    def backward(task):
        i = task % CHUNKS
        block = (task // CHUNKS) % 2

        def loads_1(n, slot):
            return w_cols(ONE, n, slot) + [kept_load(2, i, n, slot)]

        def loads_0(n, slot):
            return wo_rows(ZERO, n, slot) + [kept_load(m, i, n, slot) for m in PAIR]

        for n, loads in enumerate((loads_0, loads_1)):
            @pl.when(block == n)
            def _(loads=loads):
                start_all(loads(ZERO, ZERO))

        @pl.when(task <= BACK_AT)
        def _():
            op_sent(i, PAIR)

        @pl.when(task > CHUNKS)
        def _():
            op_sent(i, range(2, 5))

        @pl.when(block == ONE)
        def _():
            all_recv(out_second(ZERO, i))
            run_all(load_tokens(H1, i, ZERO) + load_tokens(G, i, ONE))
            op_start(4, i, ONE)
            normalize()
            turn_tokens(i, ONE)

        @pl.when(block == ZERO)
        def _():
            all_recv(out_second(ONE, i))
            run_all(load_tokens(E1, i, ONE))
            op_start(4, i, ZERO)

        @pl.when(block == ONE)
        def _():
            def body(n, slot):
                for h in PAIR:
                    pre_gate = mm(part_of(ZERO, h), wcol[slot, ZERO], ZERO)
                    pre_in = mm(part_of(ZERO, h), wcol[slot, ONE], ZERO)
                    gate_act = gradients_of(n, h, pre_gate, pre_in, fab[ZERO, slot, pl.ds(h * PART, PART)])
                    utw[pl.ds(h * PART, PART), :] = (gate_act * pre_in).astype(BF16)
                keep_u(n, cx, utw[...])

            stream(HIDDEN_TILES, loads_1, body, started=True)

        @pl.when(block == ZERO)
        def _():
            def body(n, slot):
                for h in PAIR:
                    rows = pl.ds(h * PART, PART)
                    gradients_of(n, h, fab[ZERO, slot, rows], fab[ONE, slot, rows], mm(part_of(ONE, h), wo_tile(slot), ONE))

            stream(HIDDEN_TILES, loads_0, body, started=True)

        @pl.when(block == ONE)
        def _():
            op_start(ONE, i, ONE)

        for n in (2, 3):
            op_start(n, i, block)

    def back_loads(block, n, slot):
        return [local(src.at[block, fq, sum_cols(block, n)], wrow.at[slot, 2 * m + fq], s_sem.at[slot, 2 * m + fq])
                for m, src in enumerate((wg, wi)) for fq in PAIR]

    def backward_out(task):
        block = (task // CHUNKS) % 2

        def loads(n, slot):
            return back_loads(block, n, slot)

        def product(slot):
            return sum(mm(dd[m, fq], wrow[slot, 2 * m + fq], ONE) for m in PAIR for fq in PAIR)

        write_sums(task, loads, product, started=True)

    def grad_loads(t, slot):
        return [local(rhs_d.at[t // (2 * TILES), (t // TILES) % 2, q, :, col_tile(t)], narrow(slot, q), s_sem.at[slot, q]) for q in PAIR]

    def grad_cols(t, place):
        fq = (t // TILES) % 2
        quarter = pick((place + 2 * fq, 2 * place + fq), core)
        return quarter * WIDTH + (t % TILES) * TILE

    def grad_sent(slot):
        for q in PAIR:
            local(outs.at[slot, q], dwg.at[:, pl.ds(ZERO, TILE)], gr_send.at[slot, q]).wait()

    my_place = pick(rs, core)

    def grad_tile(t):
        mtx, slot, at = t // (2 * TILES), t % SLOTS, t % 2

        @pl.when(t == ZERO)
        def _():
            op_sent(ZERO, range(2, 5))
            for i in range(CHUNKS):
                op_arrived(i)
            start_all(grad_loads(ZERO, ZERO))
            run_all([local(lhs_n.at[q], wrow.at[q], l_sem.at[q]) for q in PAIR])

        @pl.when(t + ONE < SENT_TILES)
        def _():
            start_all(grad_loads(t + ONE, ONE - at))

        wait_all(grad_loads(t, at))

        @pl.when(t >= SLOTS)
        def _():
            grad_sent(slot)

        def half(n):
            q = (ONE - my_place) * (ONE - n) + my_place * n

            def rows(src):
                return wrow[src, pl.ds(2 * q, 2)].reshape(QUARTER, WIDTH)

            outs[slot, q] = mm(rows(ZERO), narrow(at, ZERO)[...], ZERO) + mm(rows(ONE), narrow(at, ONE)[...], ZERO)
            cols = pl.ds(grad_cols(t, my_place), TILE)
            for m, dst in enumerate((dwg, dwi)):
                @pl.when((mtx == m) & (n == ZERO) & (t < SENT_TILES - LATE_TILES))
                def _(m=m, dst=dst):
                    remote(outs.at[slot, q], dst.at[:, cols], gr_send.at[slot, q], gr_recv.at[m, (t // TILES) % 2], red_of(core)).start()

                @pl.when((mtx == m) & (n == ONE))
                def _(dst=dst):
                    local(outs.at[slot, q], dst.at[:, cols], gr_send.at[slot, q]).start()

            @pl.when((n == ZERO) & (t >= SENT_TILES - LATE_TILES))
            def _():
                local(outs.at[slot, q], late.at[:, pl.ds((t - SENT_TILES + LATE_TILES) * TILE, TILE)], gr_send.at[slot, q]).start()

        repeat(2, half)

    def out_loads(k, slot):
        return [local(lhs_u.at[q, pl.ds(k * QUARTER, QUARTER)], dd.at[slot, q], o_sem.at[slot, q]) for q in PAIR]

    def out_store(n, k, slot):
        return local(wo_out.at[slot], dwo.at[pl.ds(k * QUARTER, QUARTER), pl.ds(n * WIDE, WIDE)], o_sem.at[slot, 2])

    def e_loads(n):
        return [local(rhs_e.at[q, :, :, :, :, pl.ds(n * WIDE, WIDE)], ecol.at[q], e_sem.at[q]) for q in PAIR]

    def out_tile(n):
        wait_all(e_loads(n))

        def quarter(k):
            slot = k % 2

            @pl.when(k < 3)
            def _():
                start_all(out_loads(k + ONE, ONE - slot))

            wait_all(out_loads(k, slot))

            @pl.when(4 * n + k >= 2)
            def _():
                out_store(n, k, slot).wait()

            wo_out[slot] = mm(dd[slot, ZERO], ecol[ZERO].reshape(WIDTH, WIDE), ZERO) + mm(dd[slot, ONE], ecol[ONE].reshape(WIDTH, WIDE), ZERO)
            out_store(n, k, slot).start()

        repeat(4, quarter)

    barrier = pltpu.get_barrier_semaphore()
    for dev in (reds[ZERO], nons[ZERO], twin, (y_chip, other)):
        pl.semaphore_signal(barrier, inc=ONE, device_id=dev, device_id_type=MESH)
    pl.semaphore_wait(barrier, 4)

    for block in PAIR:
        wo_hand(block)
    per_mtx(lambda mtx: w_hand(ONE - mtx if mtx == ZERO else ZERO).start())

    def given(arr, i):
        return arr.at[i, pl.ds(core * ROWS, ROWS)]

    spots = [[ab.at[n, i // 2, i % 2] for i in range(CHUNKS)] for n in PAIR]
    run_all([local(given(arr, i), spots[n][i], b_sem.at[n, i // 2, i % 2]) for n, arr in enumerate((x, g)) for i in range(CHUNKS)])
    for hi in PAIR:
        for lo in PAIR:
            cols = pl.ds((2 * hi + lo) * QUARTER, QUARTER)
            run_all([local(spots[n][i].at[:, cols], act.at[kind, hi, lo, i, ZERO, ZERO], b_sem.at[n, i // 2, i % 2]) for n, kind in enumerate((X, G)) for i in range(CHUNKS)])

    start_all(in_first(X, ZERO))

    @pl.when(core == ZERO)
    def _():
        for to_red in (ONE, ZERO):
            w_start(ZERO, to_red)

    w_hand(ZERO).wait_recv()

    @pl.when(core == ONE)
    def _():
        for to_red in (ONE, ZERO):
            w_start(ZERO, to_red)

    for i in range(ONE, CHUNKS):
        start_all(in_first(X, i))

    @per_mtx
    def _(mtx):
        for block in PAIR:
            run_all([local(w_src(mtx, block).at[:, f_cols(block, rs[block], fq)], dd.at[ZERO, fq], o_sem.at[ZERO, fq]) for fq in PAIR])
            run_all([local(dd.at[ZERO, fq], w_rows(mtx, block, fq, chip), o_sem.at[ZERO, fq]) for fq in PAIR])
        rows = [pl.ds(k * QUARTER, QUARTER) for k in range(4)]
        run_all([local(wo_in.at[rows[k]], dd.at[k // 2, k % 2], o_sem.at[k // 2, k % 2]) for k in range(4)])
        run_all([local(dd.at[k // 2, k % 2], wo.at[mtx, cs[mtx], rows[k]], o_sem.at[k // 2, k % 2]) for k in range(4)])

    pass_on(in_first(X, ZERO), in_second(X, ZERO))
    for fq in PAIR:
        w_pass(ZERO, fq)
    for i in range(ONE, CHUNKS):
        pass_on(in_first(X, i), in_second(X, i))
    wo_start(ONE)
    wo_start(ZERO)
    w_start(ONE, ZERO)

    for i in PAIR:
        start_all(in_first(G, i))

    @pl.when(core == ZERO)
    def _():
        w_start(ONE, ONE)

    for fq in PAIR:
        w_end(ZERO, fq)
    w_arrived(ZERO)

    def when_forward(tick):
        def run(body):
            @pl.when((tick >= ZERO) & (tick < CHUNKS))
            def _():
                body(tick)
        return run

    def in_two_parts(offset, late):
        def run(body):
            @pl.when(((offset >= ZERO) & (offset < 2)) | ((offset >= late) & (offset < late + 2)))
            def _():
                body(jnp.where(offset < 2, offset, offset - late + 2))
        return run

    def tick_step(tick):
        @pl.when(tick == ONE)
        def _():
            for i in (2, 3):
                start_all(in_first(G, i))

        @pl.when(tick == CHUNKS)
        def _():
            wo_pass(ONE)
            wo_arrived(ONE)

        last_give = tick == GRADS_AT + 2 * LAG
        gives = ((tick >= BACK_AT + 2) & (tick < GRADS_AT + ONE)) | last_give
        given_task = jnp.where(last_give, TASKS - ONE, tick - CHUNKS - 2)

        @pl.when(gives)
        def _():
            give_loads(given_task)

        @pl.when(tick == BACK_AT)
        def _():
            w_arrived(ONE)

        when_forward(tick)(forward)

        @pl.when((tick >= CHUNKS) & (tick < BACK_AT))
        def _():
            hidden_cotangent(tick - CHUNKS)

        @pl.when((tick >= BACK_AT) & (tick < GRADS_AT))
        def _():
            backward(tick - CHUNKS)

        @pl.when(tick >= GRADS_AT)
        def _():
            grad_tile(tick - GRADS_AT)

        grad = tick - GRADS_AT

        @pl.when((grad >= OUT_AT - 2) & ((grad - OUT_AT + 2) % OUT_EVERY == ZERO) & (grad < OUT_AT + 4 * OUT_EVERY - 2))
        def _():
            start_all(e_loads((grad - OUT_AT + 2) // OUT_EVERY) + out_loads(ZERO, ZERO))

        @pl.when((grad >= OUT_AT) & ((grad - OUT_AT) % OUT_EVERY == ZERO))
        def _():
            out_tile((grad - OUT_AT) // OUT_EVERY)

        @in_two_parts(tick - PASS_H1, BACK_AT + ONE - PASS_H1)
        def _(i):
            pass_on(out_first(ZERO, i), out_second(ZERO, i))

        @pl.when((tick >= BACK_AT + 3) & (tick < BACK_AT + 3 + CHUNKS))
        def _():
            i = tick - BACK_AT - 3
            pass_on(out_first(ONE, i), out_second(ONE, i))

        @pl.when(gives)
        def _():
            rs_give(given_task)

        in_two_parts(tick - TAKE_H1, BACK_AT - TAKE_H1)(rs_take)

        @pl.when((tick >= BACK_AT) & (tick < GRADS_AT))
        def _():
            start_all(back_loads((tick // CHUNKS + ONE) % 2, ZERO, ZERO))

        last_take = tick == GRADS_AT + LAG

        @pl.when(((tick >= BACK_AT + ONE) & (tick < GRADS_AT)) | last_take)
        def _():
            rs_take(jnp.where(last_take, TASKS - ONE, tick - CHUNKS - ONE))

        @pl.when(tick == ONE)
        def _():
            wo_pass(ZERO)
            wo_arrived(ZERO)

            @pl.when(core == ONE)
            def _():
                w_start(ONE, ONE)

        when_forward(tick - ONE)(forward_out)

        for n in PAIR:
            @pl.when(tick == 3 + n)
            def _(n=n):
                for i in PAIR:
                    pass_on(in_first(G, 2 * n + i), in_second(G, 2 * n + i))

            @pl.when(tick == W_PASS[n])
            def _(n=n):
                w_pass(ONE, n)

            @pl.when(tick == W_END[n])
            def _(n=n):
                w_end(ONE, n)

        @pl.when((tick >= BACK_AT) & (tick < GRADS_AT))
        def _():
            backward_out(tick - CHUNKS)

    repeat(GRADS_AT + SENT_TILES, tick_step)

    for m, dst in enumerate((dwg, dwi)):
        for fq in PAIR:
            arrived(dst.at[:, pl.ds(pick((ONE - cx + 2 * fq, 2 * (ONE - cy) + fq), core) * WIDTH, WIDTH - m * fq * LATE_TILES * TILE)], gr_recv.at[m, fq])
    for slot in range(SLOTS):
        grad_sent(slot)
    for slot in PAIR:
        out_store(ZERO, ZERO, slot).wait()
    for i in range(CHUNKS):
        all_recv(dx_copies(i, ZERO)[ONE:])
    for i in (CHUNKS - 2, CHUNKS - ONE):
        dx_sent(i)

    def sent(copies):
        for copy in copies:
            copy.wait_send()

    for i in range(CHUNKS):
        for kind in (X, G):
            sent([*in_first(kind, i), *in_second(kind, i)])
        for block in PAIR:
            sent(out_first(block, i) + out_second(block, i))
    repeat(TASKS, lambda task: rs_copy(task).wait_send())
    for task in (TASKS - 2, TASKS - ONE):
        sent(dot_copies(task))
    for block in PAIR:
        for fq in PAIR:
            sent(w_first(ZERO, block, fq) + (w_second(ZERO, block, fq),))
            sent(w_twin(ZERO, block, fq))
    for k in range(4):
        for block in PAIR:
            @pl.when(core == block)
            def _(block=block, k=k):
                wo_copies(block, k)[ZERO].wait_send()

    def wo_sent(k):
        for block in PAIR:
            sent((wo_copies(block, k)[ONE], wo_copies(block, k)[3]))

    halves(wo_sent)
    w_hand(ZERO).wait_send()


def settle_kernel(*refs):
    for src, dst in zip(refs[:4], refs[4:]):
        dst[...] = src[...]


def settle(arrays, steps=16):
    specs = [pl.BlockSpec((arr.shape[0] // steps, arr.shape[1]), lambda i: (i, 0)) for arr in arrays]
    size = sum(arr.size * arr.dtype.itemsize for arr in arrays)
    return pl.pallas_call(
        settle_kernel, grid=(steps,), out_shape=[jax.ShapeDtypeStruct(arr.shape, arr.dtype) for arr in arrays], in_specs=specs, out_specs=specs,
        name='settle', cost_estimate=pl.CostEstimate(flops=2 ** 30, bytes_accessed=2 * size, transcendentals=0),
        compiler_params=pltpu.CompilerParams(vmem_limit_bytes=67_043_328),
    )(*arrays)


def insert_kernel(spot, late, whole, out):
    out[...] = late[...]


def insert_late(whole, late, spot):
    block = (QUARTER, QUARTER)
    return pl.pallas_call(
        insert_kernel, out_shape=jax.ShapeDtypeStruct(whole.shape, whole.dtype),
        grid_spec=pltpu.PrefetchScalarGridSpec(
            num_scalar_prefetch=1, grid=(3,), in_specs=[pl.BlockSpec(block, lambda k, spot: (0, k)), pl.BlockSpec(memory_space=pl.ANY)],
            out_specs=pl.BlockSpec(block, lambda k, spot: (0, 4 * spot[0] + 1 + k))),
        input_output_aliases={2: 0}, name='insert_late',
    )(spot, late, whole)


def solution(mesh):
    act_spec = P(None, 'data', None, None)
    weight_spec = P('stage', None, 'data', None)

    def per_device(x, g, w_gate, w_in, w_out):
        flat = (CHUNKS, 2 * ROWS, WIDTH)
        any_space = pl.BlockSpec(memory_space=pl.ANY)
        pair = (2, 2)

        def arr(*shape, dtype=BF16):
            return jax.ShapeDtypeStruct(shape, dtype)

        def f32(*shape):
            return arr(*shape, dtype=F32)

        piece = (*pair, ROWS, QUARTER)
        out_shapes = [
            arr(*flat), f32(QUARTER, 4 * WIDTH), f32(QUARTER, 4 * WIDTH), f32(WIDTH, WIDTH), f32(QUARTER, LATE_TILES * TILE),
            arr(4, *pair, CHUNKS, *pair, ROWS, QUARTER), *[arr(*pair, WIDTH, WIDTH)] * 3, arr(QUARTER, 4 * WIDTH),
            f32(TASKS, 2, *piece), f32(TASKS, *piece), f32(2 * CHUNKS, 2, ROWS, ROWS), f32(3, CHUNKS, HIDDEN_TILES, BLOCK_ROWS, WIDE),
            arr(2, SUM_TILES, TILE, WIDTH), arr(2, WIDTH, WIDTH), arr(*pair, 2, WIDTH, WIDTH), arr(2, CHUNKS, *pair, ROWS, WIDTH),
        ]

        def bf(*shape):
            return pltpu.VMEM(shape, BF16)

        def fl(*shape):
            return pltpu.VMEM(shape, F32)

        scratch = [
            bf(*pair, WIDTH, WIDE), bf(2, 4, TILE, WIDTH), fl(*pair, BLOCK_ROWS, WIDE), bf(2, *pair, ROWS, WIDTH), bf(*pair, BLOCK_ROWS, WIDTH),
            bf(SUM_TILES, TILE, BLOCK_ROWS), bf(WIDTH, BLOCK_ROWS), bf(BLOCK_ROWS, WIDE), fl(2, *pair, ROWS, TILE), fl(2, *piece), fl(2, *piece), bf(3, *piece),
            fl(2, 2, ROWS, ROWS), bf(2, *piece), bf(2, 2, ROWS, HALF), bf(2, CHUNKS, *pair, ROWS, WIDE), fl(SLOTS, 2, QUARTER, TILE), fl(2, QUARTER, WIDE),
        ]
        counts = [(4, CHUNKS, 8), (4, CHUNKS, 8), (TASKS,), (TASKS,), (2 * CHUNKS, 2), (2 * CHUNKS, 2), (*pair, 3), (*pair, 3), (*pair, 4), (*pair, 4),
                  (1,), (1,), (2, 3, 4), (2, 3, 4), (5,), (CHUNKS, 5), (CHUNKS, 4), (CHUNKS, 3), (SLOTS, 2), pair, (2,), (4,), (3,), (2, 4), pair, (2, *pair), (2, 3), (2,)]
        results = pl.pallas_call(
            step_kernel, out_shape=out_shapes, in_specs=[any_space] * 5, out_specs=[any_space] * len(out_shapes),
            scratch_shapes=scratch + [pltpu.SemaphoreType.DMA(count) for count in counts], name='mlp_step',
            compiler_params=pltpu.CompilerParams(collective_id=0, has_side_effects=True, vmem_limit_bytes=67_043_328),
        )(x.reshape(flat), g.reshape(flat), w_gate[0, 0], w_in[0, 0], w_out[0, 0])
        late = lax.ppermute(results[4], ('data', 'stage'), [(2 * c + s, 2 * (c ^ (1 + s)) + s) for c in range(4) for s in PAIR])
        chip, core = lax.axis_index('data'), lax.axis_index('stage')
        spot = jnp.where(core == 0, 3 - chip % 2, 3 - 2 * (chip // 2))
        dx, d_gate, d_in, d_out = settle((results[0].reshape(-1, WIDTH), *results[1:4]))
        d_in = insert_late(d_in, late, spot.astype(jnp.int32).reshape(1))
        return dx.reshape(x.shape), d_gate[None, None], d_in[None, None], d_out[None, None]

    return jax.shard_map(per_device, mesh=mesh, in_specs=(act_spec, act_spec, weight_spec, weight_spec, weight_spec),
                         out_specs=(act_spec, weight_spec, weight_spec, weight_spec), check_vma=False)
```

```python
import jax
import jax.numpy as jnp
from jax import lax
from jax.experimental import pallas as pl
from jax.experimental.pallas import tpu as pltpu
from jax.sharding import PartitionSpec as P

MESH = pl.DeviceIdType.MESH
F32 = jnp.float32
BF16 = jnp.bfloat16
EPS = 1e-6

CHUNKS = 4
ROWS = 128
BLOCK_ROWS = 4 * ROWS
WIDTH = 2048
HALF = WIDTH // 2
QUARTER = WIDTH // 4
TILE = 256
TILES = WIDTH // TILE
WIDE = 2 * TILE
WIDES = WIDTH // WIDE
PART = BLOCK_ROWS // 2
HIDDEN_TILES = 2 * WIDES
SUM_TILES = HALF // TILE
TASKS = 3 * CHUNKS
BACK_AT = 2 * CHUNKS
GRADS_AT = 4 * CHUNKS
SENT_TILES = 4 * TILES
SLOTS = 4
OUT_AT, OUT_EVERY = 4, 7
LATE_TILES = 6
LAG = 6
W_PASS, W_END = (2, 3), (7, 7)
TAKE_H1, PASS_H1 = 4, 6
PAIR = ZERO, ONE = range(2)
X, H1, G, E1 = range(4)


def mm(lhs, rhs, rhs_dim):
    return lax.dot_general(lhs, rhs, (((1,), (rhs_dim,)), ((), ())), preferred_element_type=F32)


def repeat(count, body):
    def step(n, carry):
        body(n)
        return carry

    lax.fori_loop(0, count, step, 0)


def start_all(copies):
    for copy in copies:
        copy.start()


def wait_all(copies):
    for copy in copies:
        copy.wait()


def run_all(copies):
    start_all(copies)
    wait_all(copies)


def step_kernel(x, g, wg_in, wi_in, wo_in,
                dx, dwg, dwi, dwo, late, act, wg, wi, wo, wx, part, rb, dots, kept, lhs_n, lhs_u, rhs_d, rhs_e,
                wcol, wrow, fab, ab, dd, ntb, utb, utw, pst, ld, tot, own, dsv, new, dxn, ecol, outs, wo_out,
                ag_send, ag_recv, rs_send, rs_recv, dt_send, dt_recv, w_send, w_recv, f_send, f_recv, h_send, h_recv, wo_send, wo_recv,
                op_send, op_recv, dx_send, dx_recv, gr_send, gr_recv, p_sem, l_sem, g_sem, s_sem, k_sem, b_sem, o_sem, e_sem):
    chip = lax.axis_index('data')
    core = lax.axis_index('stage')
    cx, cy = chip % 2, chip // 2
    other = ONE - core
    x_chip, y_chip = cy * 2 + (ONE - cx), (ONE - cy) * 2 + cx
    twin = (chip, other)
    reds, nons = ((x_chip, core), (y_chip, core)), ((y_chip, core), (x_chip, core))
    rs, cs = (cx, cy), (cy, cx)

    def pick(pair, block):
        return pair[ZERO] + (pair[ONE] - pair[ZERO]) * block

    def red_of(block):
        return pick((x_chip, y_chip), block), core

    def local(src, dst, sem):
        return pltpu.make_async_copy(src, dst, sem)

    def remote(src, dst, send, recv, dev):
        return pltpu.make_async_remote_copy(src_ref=src, dst_ref=dst, send_sem=send, recv_sem=recv, device_id=dev, device_id_type=MESH)

    def arrived(ref, sem):
        local(ref, ref, sem).wait()

    def in_first(kind, i):
        block = kind // G
        mine = act.at[kind, :, :, i, ZERO, ZERO]
        return (remote(mine, act.at[kind, :, :, i, ONE, ZERO], ag_send.at[kind, i, ZERO], ag_recv.at[kind, i, ZERO], reds[block]),
                remote(mine, act.at[kind, :, :, i, ZERO, ONE], ag_send.at[kind, i, ONE], ag_recv.at[kind, i, ONE], nons[block]))

    def in_second(kind, i):
        block = kind // G
        sends = [remote(act.at[kind, :2 - (kind == X), :, i, ZERO, ONE], act.at[kind, :2 - (kind == X), :, i, ONE, ONE], ag_send.at[kind, i, 2], ag_recv.at[kind, i, 2], reds[block])]
        if kind == X:
            sends.append(remote(act.at[kind, ONE, :, i, ONE, ZERO], act.at[kind, ONE, :, i, ONE, ONE], ag_send.at[kind, i, 3], ag_recv.at[kind, i, 3], nons[block]))
        return sends

    def out_first(block, i):
        kind, c = (H1, E1)[block], cs[block]
        sends = [remote(act.at[kind, c, :, i, :, ZERO], act.at[kind, c, :, i, :, ONE], ag_send.at[kind, i, ZERO], ag_recv.at[kind, i, ZERO], reds[block])]
        for a in PAIR:
            sends.append(remote(act.at[kind, c, :, i, a, ZERO], act.at[kind, c, :, i, ONE - a, ZERO], ag_send.at[kind, i, ONE + a], ag_recv.at[kind, i, 2 - a], nons[block]))
        return sends

    def out_second(block, i):
        kind, c = (H1, E1)[block], cs[block]
        if block:
            came, spot = act.at[kind, ONE - c, :, i, :, ZERO], act.at[kind, ONE - c, :, i, :, ONE]
            return [remote(came, spot, ag_send.at[kind, i, 3], ag_recv.at[kind, i, 3], reds[block])]
        return [remote(act.at[kind, c, h, i, a, ONE], act.at[kind, c, h, i, ONE - a, ONE], ag_send.at[kind, i, 4 + 2 * a + h], ag_recv.at[kind, i, 6 - 2 * a + h], nons[block])
                for a in PAIR for h in PAIR]

    def pass_on(first, second):
        for copy in first:
            copy.wait_recv()
        start_all(second)

    def all_recv(copies):
        for copy in copies:
            copy.wait_recv()

    def rs_copy(task):
        return remote(part.at[task, :, ONE], rb.at[task], rs_send.at[task], rs_recv.at[task], red_of((task // CHUNKS) % 2))

    def dot_copies(task):
        slot, n = task % 2, task - CHUNKS
        dev = pick((y_chip, x_chip), (task // CHUNKS) % 2), core
        return [remote(dsv.at[slot, b], dots.at[n, ONE - b], dt_send.at[n, b], dt_recv.at[n, ONE - b], dev) for b in PAIR]

    def own_half(kind_h, block, i):
        if block == ZERO:
            return act.at[X, cy, :, i, ZERO] if kind_h else act.at[E1, :, cy, i, ZERO]
        return act.at[H1, :, cx, i, ZERO] if kind_h else act.at[G, :, cx, i, ZERO]

    def rest_half(block, i):
        return act.at[X, ONE - cy, :, i, ZERO] if block == ZERO else act.at[H1, :, ONE - cx, i, ZERO]

    def when_kind(task):
        def run(body):
            for kind in range(3):
                @pl.when(task // CHUNKS == kind)
                def _(kind=kind):
                    body(kind)
        return run

    def send_result(block, i, slot):
        run_all([local(new.at[slot], act.at[(H1, E1)[block], cs[block], :, i, :, ZERO], l_sem.at[ZERO])])
        start_all(out_first(block, i))

    def pieces(body):
        def step(n):
            body(n // 2, n % 2, pl.ds(ZERO, ROWS))
        repeat(4, step)

    def rs_take(task):
        i, slot = task % CHUNKS, task % 2
        rs_copy(task).wait_recv()
        start_all([local(part.at[task, :, ZERO], ld.at[ZERO], l_sem.at[ZERO]), local(rb.at[task], ld.at[ONE], l_sem.at[ONE])])

        @when_kind(task)
        def _(kind):
            local(own_half(True, kind % 2, i), own.at[ZERO], l_sem.at[2]).start()

        wait_all([local(rb.at[task], ld.at[ZERO], l_sem.at[ZERO]), local(rb.at[task], ld.at[ONE], l_sem.at[ONE]), local(own_half(True, ZERO, i), own.at[ZERO], l_sem.at[2])])

        @pl.when(task < CHUNKS)
        def _():
            @pieces
            def _(q, b, rows):
                new[slot, q, b, rows, :] = own[ZERO, q, b, rows, :] + (ld[ZERO, q, b, rows, :] + ld[ONE, q, b, rows, :]).astype(BF16)

            send_result(ZERO, i, slot)

        @pl.when(task >= CHUNKS)
        def _():
            @pl.when(task >= CHUNKS + 2)
            def _():
                for copy in dot_copies(task - 2):
                    copy.wait_send()

            @pieces
            def _(q, b, rows):
                total = ld[ZERO, q, b, rows, :] + ld[ONE, q, b, rows, :]
                tot[slot, q, b, rows, :] = total
                dot = jnp.sum(total * own[ZERO, q, b, rows, :].astype(F32), axis=-ONE, keepdims=True) + jnp.zeros((ONE, ROWS), F32)

                @pl.when(q == ZERO)
                def _():
                    dsv[slot, b, rows, :] = dot

                @pl.when(q == ONE)
                def _():
                    dsv[slot, b, rows, :] = dsv[slot, b, rows, :] + dot

            start_all(dot_copies(task))

    def dx_copies(i, slot):
        spot = dx.at[i, pl.ds(core * ROWS, ROWS), pl.ds(cy * HALF, HALF)]
        return (local(dxn.at[slot, ZERO], spot, dx_send.at[i, ZERO]), remote(dxn.at[slot, ZERO], spot, dx_send.at[i, ONE], dx_recv.at[i, ZERO], twin),
                remote(dxn.at[slot, ONE], spot, dx_send.at[i, 2], dx_recv.at[i, ONE], (y_chip, core)),
                remote(dxn.at[slot, ONE], spot, dx_send.at[i, 3], dx_recv.at[i, 2], (y_chip, other)))

    def dx_sent(i):
        copies = dx_copies(i, i % 2)
        copies[ZERO].wait()
        for copy in copies[ONE:]:
            copy.wait_send()

    def give_loads(task):
        for block in PAIR:
            @pl.when((task // CHUNKS) % 2 == block)
            def _(block=block):
                i = task % CHUNKS
                start_all([local(src, own.at[n], g_sem.at[n]) for n, src in enumerate((own_half(True, block, i), own_half(False, block, i), rest_half(block, i)))])

    def rs_give(task):
        i, slot = task % CHUNKS, task % 2
        for b in PAIR:
            arrived(dots.at[task - CHUNKS, b], dt_recv.at[task - CHUNKS, b])
        local(dots.at[task - CHUNKS], ld.at[ZERO, ZERO, :, :, pl.ds(ZERO, ROWS)], l_sem.at[3]).start()
        wait_all([local(own_half(True, ZERO, i), own.at[n], g_sem.at[n]) for n in range(3)])
        local(dots.at[task - CHUNKS], ld.at[ZERO, ZERO, :, :, pl.ds(ZERO, ROWS)], l_sem.at[3]).wait()

        @pl.when(task >= 2 * CHUNKS + 2)
        def _():
            dx_sent(i - 2)

        def step(n):
            b, rows = n // 2, pl.ds((n % 2) * (ROWS // 2), ROWS // 2)

            def sq(slot_of, q):
                vals = own[slot_of, q, b, rows, :].astype(F32)
                return jnp.sum(vals * vals, axis=-ONE, keepdims=True)

            square = sq(ZERO, ZERO) + sq(ZERO, ONE) + sq(2, ZERO) + sq(2, ONE)
            inv = lax.rsqrt(square / WIDTH + EPS)
            dot = (dsv[slot, b, rows, ZERO:ONE] + ld[ZERO, ZERO, b, rows, ZERO:ONE]) / WIDTH
            for q in PAIR:
                tok = own[ZERO, q, b, rows, :].astype(F32)
                resid = tot[slot, q, b, rows, :] * inv - tok * (inv * inv * inv * dot)
                val = (own[ONE, q, b, rows, :].astype(F32) + resid).astype(BF16)
                new[slot, q, b, rows, :] = val
                dxn[slot, b, rows, pl.ds(q * QUARTER, QUARTER)] = val

        repeat(4, step)

        @pl.when(task < 2 * CHUNKS)
        def _():
            send_result(ONE, i, slot)

        @pl.when(task >= 2 * CHUNKS)
        def _():
            start_all(dx_copies(i, slot))

    def f_cols(block, place, fq):
        quarter = place + 2 * fq if block == ZERO else 2 * place + fq
        return pl.ds(quarter * WIDTH, WIDTH)

    def w_src(mtx, block):
        return ((wg_in, wx), (wx, wi_in))[mtx][block]

    def w_rows(mtx, block, fq, of):
        return (wg, wi)[mtx].at[block, fq, pl.ds(of * QUARTER, QUARTER)]

    def w_first(mtx, block, fq):
        src, mine = w_src(mtx, block), w_rows(mtx, block, fq, chip)
        return (remote(src.at[:, f_cols(block, rs[block], fq)], mine, w_send.at[block, fq, ZERO], w_recv.at[block, fq, ZERO], nons[block]),
                remote(src.at[:, f_cols(block, ONE - rs[block], fq)], mine, w_send.at[block, fq, ONE], w_recv.at[block, fq, ONE], reds[block]))

    def w_second(mtx, block, fq):
        piece = w_rows(mtx, block, fq, reds[block][ZERO])
        return remote(piece, piece, w_send.at[block, fq, 2], w_recv.at[block, fq, 2], nons[block])

    def w_twin(mtx, block, fq):
        far = 3 - chip
        srcs = [w_src(mtx, block).at[:, f_cols(block, rs[block], fq)]] + [w_rows(mtx, block, fq, of) for of in (nons[block][ZERO], reds[block][ZERO], far)]
        spots = [w_rows(mtx, block, fq, of) for of in (chip, nons[block][ZERO], reds[block][ZERO], far)]
        return [remote(src, spot, f_send.at[block, fq, n], f_recv.at[block, fq, n], twin) for n, (src, spot) in enumerate(zip(srcs, spots))]

    def per_mtx(body):
        for mtx in PAIR:
            @pl.when(core == mtx)
            def _(mtx=mtx):
                body(mtx)

    def w_start(block, to_red):
        @per_mtx
        def _(mtx):
            for fq in PAIR:
                w_first(mtx, block, fq)[to_red].start()
                if not to_red:
                    w_twin(mtx, block, fq)[ZERO].start()

    def w_pass(block, fq):
        @per_mtx
        def _(mtx):
            first, to_twin = w_first(mtx, block, fq), w_twin(mtx, block, fq)
            first[ONE].wait_recv()
            w_second(mtx, block, fq).start()
            to_twin[2].start()
            first[ZERO].wait_recv()
            to_twin[ONE].start()

    def w_end(block, fq):
        @per_mtx
        def _(mtx):
            w_second(mtx, block, fq).wait_recv()
            w_twin(mtx, block, fq)[3].start()

    def w_arrived(block):
        for fq in PAIR:
            all_recv(w_twin(ZERO, block, fq))

    def w_hand(mtx):
        return remote((wg_in, wi_in)[mtx], wx, h_send.at[ZERO], h_recv.at[ZERO], twin)

    def wo_copies(block, k):
        rows = pl.ds(k * QUARTER, QUARTER)
        spot, got = wo.at[block, cs[block], rows], wo.at[block, ONE - cs[block], rows]
        return (remote(wo_in.at[rows], spot, wo_send.at[block, ZERO, k], wo_recv.at[block, ZERO, k], twin),
                remote(wo_in.at[rows], spot, wo_send.at[block, ONE, k], wo_recv.at[block, ONE, k], nons[block]),
                remote(spot, spot, wo_send.at[block, ONE, k], wo_recv.at[block, ONE, k], nons[block]),
                remote(got, got, wo_send.at[block, 2, k], wo_recv.at[block, 2, k], twin))

    def halves(body):
        for half in PAIR:
            @pl.when(core == half)
            def _(half=half):
                for k in (2 * half, 2 * half + ONE):
                    body(k)

    def wo_hand(block):
        @pl.when(core == block)
        def _():
            for k in range(4):
                wo_copies(block, k)[ZERO].start()

    def wo_start(block):
        @pl.when(core == block)
        def _():
            for k in (2 * block, 2 * block + ONE):
                wo_copies(block, k)[ONE].start()

        @pl.when(core != block)
        def _():
            for k in range(4):
                wo_copies(block, k)[ZERO].wait_recv()
            for k in (2 - 2 * block, 3 - 2 * block):
                wo_copies(block, k)[2].start()

    def wo_pass(block):
        def body(k):
            wo_copies(block, k)[ONE].wait_recv()
            wo_copies(block, k)[3].start()
        halves(body)

    def wo_arrived(block):
        def body(k):
            wo_copies(block, 3 - k)[3].wait_recv()
        halves(body)

    def op_pairs(i, src):
        cols = pl.ds(i * BLOCK_ROWS, BLOCK_ROWS)
        return ((ntb, lhs_n.at[src, :, :, cols]), (utb, lhs_u.at[src, :, cols]), (dd.at[ZERO], rhs_d.at[ZERO, :, src, cols]),
                (dd.at[ONE], rhs_d.at[ONE, :, src, cols]), (ab.at[ONE], rhs_e.at[src, i]))

    def op_start(n, i, block):
        src, dst = op_pairs(i, core)[n]

        @pl.when(block == core)
        def _():
            local(src, dst, op_send.at[n]).start()

        @pl.when(block != core)
        def _():
            remote(src, dst, op_send.at[n], op_recv.at[i, n], twin).start()

    def op_sent(i, which):
        for n in which:
            local(*op_pairs(i, core)[n], op_send.at[n]).wait()

    def op_arrived(i):
        all_recv([remote(src, dst, op_send.at[n], op_recv.at[i, n], twin) for n, (src, dst) in enumerate(op_pairs(i, other))])

    def load_tokens(kind, i, slot):
        copies = []
        for hi in PAIR:
            for lo in PAIR:
                src = act.at[kind, lo, hi, i] if kind == E1 else act.at[kind, hi, lo, i]
                copies.append(local(src, ab.at[slot, :, :, :, pl.ds((2 * hi + lo) * QUARTER, QUARTER)], b_sem.at[slot, hi, lo]))
        return copies

    def tokens(slot):
        return ab[slot].reshape(BLOCK_ROWS, WIDTH)

    def normalize():
        def step(n):
            a, b, rows = n // 4, (n // 2) % 2, pl.ds((n % 2) * (ROWS // 2), ROWS // 2)
            tok = ab[ZERO, a, b, rows, :].astype(F32)
            inv = lax.rsqrt(jnp.mean(tok * tok, axis=-ONE, keepdims=True) + EPS)
            ab[ZERO, a, b, rows, :] = (tok * inv).astype(BF16)

        repeat(2 * 4, step)

    def stream(count, loads, body, started=False):
        if not started:
            start_all(loads(ZERO, ZERO))

        def step(n):
            slot = n % 2

            @pl.when(n + ONE < count)
            def _():
                start_all(loads(n + ONE, ONE - slot))

            wait_all(loads(n, slot))
            body(n, slot)

        repeat(count, step)

    def col_tile(n):
        return pl.ds((n % TILES) * TILE, TILE)

    def narrow(slot, n):
        return wcol.at[slot, n, :, pl.ds(ZERO, TILE)]

    def wide(n):
        return pl.ds((n % WIDES) * WIDE, WIDE)

    def w_cols(block, n, slot):
        return [local(src.at[block, n // WIDES, :, wide(n)], wcol.at[slot, m], s_sem.at[slot, m]) for m, src in enumerate((wg, wi))]

    def wo_rows(block, n, slot):
        return [local(wo.at[block, n // WIDES, pl.ds((n % WIDES) * WIDE + h * TILE, TILE)], wrow.at[slot, h], s_sem.at[slot, 2 + h]) for h in PAIR]

    def wo_tile(slot):
        return wrow[slot, ZERO:2].reshape(WIDE, WIDTH)

    def kept_load(which, i, n, slot):
        return local(kept.at[which, i, n], fab.at[which % 2, slot], k_sem.at[which % 2, slot])

    def kept_store(which, i, n, slot):
        return local(fab.at[which % 2, slot], kept.at[which, i, n], k_sem.at[which % 2, slot])

    def sum_cols(block, n):
        quarter = pick((2 * cy + n // 2, cx + 2 * (n // 2)), block)
        return pl.ds(quarter * QUARTER + (n % 2) * TILE, TILE)

    def sum_store(task, n, slot):
        return local(pst.at[slot], part.at[task, n // 2, :, :, :, pl.ds((n % 2) * TILE, TILE)], p_sem.at[slot])

    def write_sums(task, loads, product, started=False):
        def body(n, slot):
            @pl.when(n >= 2)
            def _():
                sum_store(task, n - 2, slot).wait()

            pst[slot] = product(slot).reshape(2, 2, ROWS, TILE)
            sum_store(task, n, slot).start()

        stream(SUM_TILES, loads, body, started)
        for slot in PAIR:
            sum_store(task, slot, slot).wait()
        rs_copy(task).start()

    def forward(i):
        all_recv(in_second(X, i))
        run_all(load_tokens(X, i, ZERO))
        normalize()

        @pl.when(i > ZERO)
        def _():
            op_sent(i, PAIR)

        turn_tokens(i, ZERO)

        def body(n, slot):
            pre_gate = mm(tokens(ZERO), wcol[slot, ZERO], ZERO)
            pre_in = mm(tokens(ZERO), wcol[slot, ONE], ZERO)

            @pl.when(n >= 2)
            def _():
                wait_all([kept_store(m, i, n - 2, slot) for m in PAIR])

            fab[ZERO, slot] = pre_gate
            fab[ONE, slot] = pre_in
            start_all([kept_store(m, i, n, slot) for m in PAIR])
            hidden = (pre_gate * jax.nn.sigmoid(pre_gate) * pre_in).astype(BF16)
            dd[i % 2, n // WIDES, :, wide(n)] = hidden
            keep_u(n, cy, hidden)

        stream(HIDDEN_TILES, lambda n, slot: w_cols(ZERO, n, slot), body)
        wait_all([kept_store(m, i, slot, slot) for m in PAIR for slot in PAIR])
        op_start(ONE, i, ZERO)

    def forward_out(i):
        def loads(n, slot):
            return [local(wo.at[ZERO, fq, :, sum_cols(ZERO, n)], narrow(slot, fq), s_sem.at[slot, fq]) for fq in PAIR]

        write_sums(i, loads, lambda slot: mm(dd[i % 2, ZERO], narrow(slot, ZERO)[...], ZERO) + mm(dd[i % 2, ONE], narrow(slot, ONE)[...], ZERO))

    def hidden_cotangent(i):
        all_recv(in_second(G, i))
        run_all(load_tokens(G, i, ONE))

        def body(n, slot):
            d_hidden = mm(tokens(ONE), wo_tile(slot), ONE)

            @pl.when(n >= 2)
            def _():
                kept_store(2, i, n - 2, slot).wait()

            fab[ZERO, slot] = d_hidden
            kept_store(2, i, n, slot).start()

        stream(HIDDEN_TILES, lambda n, slot: wo_rows(ONE, n, slot), body)
        wait_all([kept_store(2, i, slot, slot) for slot in PAIR])

    def gradients_of(n, h, pre_gate, pre_in, d_hidden):
        rows = pl.ds(h * PART, PART)
        sigma = jax.nn.sigmoid(pre_gate)
        gate_act = pre_gate * sigma
        dd[ZERO, n // WIDES, rows, wide(n)] = (d_hidden * pre_in * sigma * (1.0 + pre_gate * (1.0 - sigma))).astype(BF16)
        dd[ONE, n // WIDES, rows, wide(n)] = (d_hidden * gate_act).astype(BF16)
        return gate_act

    def keep_u(n, keeps_u, hidden):
        @pl.when(n // WIDES == keeps_u)
        def _():
            utb[wide(n), :] = hidden.T

    def turn_tokens(i, block):
        def turn(n):
            ntb[n] = ab[ZERO, :, :, :, sum_cols(block, n)].reshape(BLOCK_ROWS, TILE).T

        repeat(SUM_TILES, turn)
        op_start(ZERO, i, block)

    def part_of(slot, h):
        return ab[slot, h].reshape(PART, WIDTH)

    def backward(task):
        i = task % CHUNKS
        block = (task // CHUNKS) % 2

        def loads_1(n, slot):
            return w_cols(ONE, n, slot) + [kept_load(2, i, n, slot)]

        def loads_0(n, slot):
            return wo_rows(ZERO, n, slot) + [kept_load(m, i, n, slot) for m in PAIR]

        for n, loads in enumerate((loads_0, loads_1)):
            @pl.when(block == n)
            def _(loads=loads):
                start_all(loads(ZERO, ZERO))

        @pl.when(task <= BACK_AT)
        def _():
            op_sent(i, PAIR)

        @pl.when(task > CHUNKS)
        def _():
            op_sent(i, range(2, 5))

        @pl.when(block == ONE)
        def _():
            all_recv(out_second(ZERO, i))
            run_all(load_tokens(H1, i, ZERO) + load_tokens(G, i, ONE))
            op_start(4, i, ONE)
            normalize()
            turn_tokens(i, ONE)

        @pl.when(block == ZERO)
        def _():
            all_recv(out_second(ONE, i))
            run_all(load_tokens(E1, i, ONE))
            op_start(4, i, ZERO)

        @pl.when(block == ONE)
        def _():
            def body(n, slot):
                for h in PAIR:
                    pre_gate = mm(part_of(ZERO, h), wcol[slot, ZERO], ZERO)
                    pre_in = mm(part_of(ZERO, h), wcol[slot, ONE], ZERO)
                    gate_act = gradients_of(n, h, pre_gate, pre_in, fab[ZERO, slot, pl.ds(h * PART, PART)])
                    utw[pl.ds(h * PART, PART), :] = (gate_act * pre_in).astype(BF16)
                keep_u(n, cx, utw[...])

            stream(HIDDEN_TILES, loads_1, body, started=True)

        @pl.when(block == ZERO)
        def _():
            def body(n, slot):
                for h in PAIR:
                    rows = pl.ds(h * PART, PART)
                    gradients_of(n, h, fab[ZERO, slot, rows], fab[ONE, slot, rows], mm(part_of(ONE, h), wo_tile(slot), ONE))

            stream(HIDDEN_TILES, loads_0, body, started=True)

        @pl.when(block == ONE)
        def _():
            op_start(ONE, i, ONE)

        for n in (2, 3):
            op_start(n, i, block)

    def back_loads(block, n, slot):
        return [local(src.at[block, fq, sum_cols(block, n)], wrow.at[slot, 2 * m + fq], s_sem.at[slot, 2 * m + fq])
                for m, src in enumerate((wg, wi)) for fq in PAIR]

    def backward_out(task):
        block = (task // CHUNKS) % 2

        def loads(n, slot):
            return back_loads(block, n, slot)

        def product(slot):
            return sum(mm(dd[m, fq], wrow[slot, 2 * m + fq], ONE) for m in PAIR for fq in PAIR)

        write_sums(task, loads, product, started=True)

    def grad_loads(t, slot):
        return [local(rhs_d.at[t // (2 * TILES), (t // TILES) % 2, q, :, col_tile(t)], narrow(slot, q), s_sem.at[slot, q]) for q in PAIR]

    def grad_cols(t, place):
        fq = (t // TILES) % 2
        quarter = pick((place + 2 * fq, 2 * place + fq), core)
        return quarter * WIDTH + (t % TILES) * TILE

    def grad_sent(slot):
        for q in PAIR:
            local(outs.at[slot, q], dwg.at[:, pl.ds(ZERO, TILE)], gr_send.at[slot, q]).wait()

    my_place = pick(rs, core)

    def grad_tile(t):
        mtx, slot, at = t // (2 * TILES), t % SLOTS, t % 2

        @pl.when(t == ZERO)
        def _():
            op_sent(ZERO, range(2, 5))
            for i in range(CHUNKS):
                op_arrived(i)
            start_all(grad_loads(ZERO, ZERO))
            run_all([local(lhs_n.at[q], wrow.at[q], l_sem.at[q]) for q in PAIR])

        @pl.when(t + ONE < SENT_TILES)
        def _():
            start_all(grad_loads(t + ONE, ONE - at))

        wait_all(grad_loads(t, at))

        @pl.when(t >= SLOTS)
        def _():
            grad_sent(slot)

        def half(n):
            q = (ONE - my_place) * (ONE - n) + my_place * n

            def rows(src):
                return wrow[src, pl.ds(2 * q, 2)].reshape(QUARTER, WIDTH)

            outs[slot, q] = mm(rows(ZERO), narrow(at, ZERO)[...], ZERO) + mm(rows(ONE), narrow(at, ONE)[...], ZERO)
            cols = pl.ds(grad_cols(t, my_place), TILE)
            for m, dst in enumerate((dwg, dwi)):
                @pl.when((mtx == m) & (n == ZERO) & (t < SENT_TILES - LATE_TILES))
                def _(m=m, dst=dst):
                    remote(outs.at[slot, q], dst.at[:, cols], gr_send.at[slot, q], gr_recv.at[m, (t // TILES) % 2], red_of(core)).start()

                @pl.when((mtx == m) & (n == ONE))
                def _(dst=dst):
                    local(outs.at[slot, q], dst.at[:, cols], gr_send.at[slot, q]).start()

            @pl.when((n == ZERO) & (t >= SENT_TILES - LATE_TILES))
            def _():
                local(outs.at[slot, q], late.at[:, pl.ds((t - SENT_TILES + LATE_TILES) * TILE, TILE)], gr_send.at[slot, q]).start()

        repeat(2, half)

    def out_loads(k, slot):
        return [local(lhs_u.at[q, pl.ds(k * QUARTER, QUARTER)], dd.at[slot, q], o_sem.at[slot, q]) for q in PAIR]

    def out_store(n, k, slot):
        return local(wo_out.at[slot], dwo.at[pl.ds(k * QUARTER, QUARTER), pl.ds(n * WIDE, WIDE)], o_sem.at[slot, 2])

    def e_loads(n):
        return [local(rhs_e.at[q, :, :, :, :, pl.ds(n * WIDE, WIDE)], ecol.at[q], e_sem.at[q]) for q in PAIR]

    def out_tile(n):
        wait_all(e_loads(n))

        def quarter(k):
            slot = k % 2

            @pl.when(k < 3)
            def _():
                start_all(out_loads(k + ONE, ONE - slot))

            wait_all(out_loads(k, slot))

            @pl.when(4 * n + k >= 2)
            def _():
                out_store(n, k, slot).wait()

            wo_out[slot] = mm(dd[slot, ZERO], ecol[ZERO].reshape(WIDTH, WIDE), ZERO) + mm(dd[slot, ONE], ecol[ONE].reshape(WIDTH, WIDE), ZERO)
            out_store(n, k, slot).start()

        repeat(4, quarter)

    barrier = pltpu.get_barrier_semaphore()
    for dev in (reds[ZERO], nons[ZERO], twin, (y_chip, other)):
        pl.semaphore_signal(barrier, inc=ONE, device_id=dev, device_id_type=MESH)
    pl.semaphore_wait(barrier, 4)

    for block in PAIR:
        wo_hand(block)
    per_mtx(lambda mtx: w_hand(ONE - mtx if mtx == ZERO else ZERO).start())

    def given(arr, i):
        return arr.at[i, pl.ds(core * ROWS, ROWS)]

    spots = [[ab.at[n, i // 2, i % 2] for i in range(CHUNKS)] for n in PAIR]
    run_all([local(given(arr, i), spots[n][i], b_sem.at[n, i // 2, i % 2]) for n, arr in enumerate((x, g)) for i in range(CHUNKS)])
    for hi in PAIR:
        for lo in PAIR:
            cols = pl.ds((2 * hi + lo) * QUARTER, QUARTER)
            run_all([local(spots[n][i].at[:, cols], act.at[kind, hi, lo, i, ZERO, ZERO], b_sem.at[n, i // 2, i % 2]) for n, kind in enumerate((X, G)) for i in range(CHUNKS)])

    start_all(in_first(X, ZERO))

    @pl.when(core == ZERO)
    def _():
        for to_red in (ONE, ZERO):
            w_start(ZERO, to_red)

    w_hand(ZERO).wait_recv()

    @pl.when(core == ONE)
    def _():
        for to_red in (ONE, ZERO):
            w_start(ZERO, to_red)

    for i in range(ONE, CHUNKS):
        start_all(in_first(X, i))

    @per_mtx
    def _(mtx):
        for block in PAIR:
            run_all([local(w_src(mtx, block).at[:, f_cols(block, rs[block], fq)], dd.at[ZERO, fq], o_sem.at[ZERO, fq]) for fq in PAIR])
            run_all([local(dd.at[ZERO, fq], w_rows(mtx, block, fq, chip), o_sem.at[ZERO, fq]) for fq in PAIR])
        rows = [pl.ds(k * QUARTER, QUARTER) for k in range(4)]
        run_all([local(wo_in.at[rows[k]], dd.at[k // 2, k % 2], o_sem.at[k // 2, k % 2]) for k in range(4)])
        run_all([local(dd.at[k // 2, k % 2], wo.at[mtx, cs[mtx], rows[k]], o_sem.at[k // 2, k % 2]) for k in range(4)])

    pass_on(in_first(X, ZERO), in_second(X, ZERO))
    for fq in PAIR:
        w_pass(ZERO, fq)
    for i in range(ONE, CHUNKS):
        pass_on(in_first(X, i), in_second(X, i))
    wo_start(ONE)
    wo_start(ZERO)
    w_start(ONE, ZERO)

    for i in PAIR:
        start_all(in_first(G, i))

    @pl.when(core == ZERO)
    def _():
        w_start(ONE, ONE)

    for fq in PAIR:
        w_end(ZERO, fq)
    w_arrived(ZERO)

    def when_forward(tick):
        def run(body):
            @pl.when((tick >= ZERO) & (tick < CHUNKS))
            def _():
                body(tick)
        return run

    def in_two_parts(offset, late):
        def run(body):
            @pl.when(((offset >= ZERO) & (offset < 2)) | ((offset >= late) & (offset < late + 2)))
            def _():
                body(jnp.where(offset < 2, offset, offset - late + 2))
        return run

    def tick_step(tick):
        @pl.when(tick == ONE)
        def _():
            for i in (2, 3):
                start_all(in_first(G, i))

        @pl.when(tick == CHUNKS)
        def _():
            wo_pass(ONE)
            wo_arrived(ONE)

        last_give = tick == GRADS_AT + 2 * LAG
        gives = ((tick >= BACK_AT + 2) & (tick < GRADS_AT + ONE)) | last_give
        given_task = jnp.where(last_give, TASKS - ONE, tick - CHUNKS - 2)

        @pl.when(gives)
        def _():
            give_loads(given_task)

        @pl.when(tick == BACK_AT)
        def _():
            w_arrived(ONE)

        when_forward(tick)(forward)

        @pl.when((tick >= CHUNKS) & (tick < BACK_AT))
        def _():
            hidden_cotangent(tick - CHUNKS)

        @pl.when((tick >= BACK_AT) & (tick < GRADS_AT))
        def _():
            backward(tick - CHUNKS)

        @pl.when(tick >= GRADS_AT)
        def _():
            grad_tile(tick - GRADS_AT)

        grad = tick - GRADS_AT

        @pl.when((grad >= OUT_AT - 2) & ((grad - OUT_AT + 2) % OUT_EVERY == ZERO) & (grad < OUT_AT + 4 * OUT_EVERY - 2))
        def _():
            start_all(e_loads((grad - OUT_AT + 2) // OUT_EVERY) + out_loads(ZERO, ZERO))

        @pl.when((grad >= OUT_AT) & ((grad - OUT_AT) % OUT_EVERY == ZERO))
        def _():
            out_tile((grad - OUT_AT) // OUT_EVERY)

        @in_two_parts(tick - PASS_H1, BACK_AT + ONE - PASS_H1)
        def _(i):
            pass_on(out_first(ZERO, i), out_second(ZERO, i))

        @pl.when((tick >= BACK_AT + 3) & (tick < BACK_AT + 3 + CHUNKS))
        def _():
            i = tick - BACK_AT - 3
            pass_on(out_first(ONE, i), out_second(ONE, i))

        @pl.when(gives)
        def _():
            rs_give(given_task)

        in_two_parts(tick - TAKE_H1, BACK_AT - TAKE_H1)(rs_take)

        @pl.when((tick >= BACK_AT) & (tick < GRADS_AT))
        def _():
            start_all(back_loads((tick // CHUNKS + ONE) % 2, ZERO, ZERO))

        last_take = tick == GRADS_AT + LAG

        @pl.when(((tick >= BACK_AT + ONE) & (tick < GRADS_AT)) | last_take)
        def _():
            rs_take(jnp.where(last_take, TASKS - ONE, tick - CHUNKS - ONE))

        @pl.when(tick == ONE)
        def _():
            wo_pass(ZERO)
            wo_arrived(ZERO)

            @pl.when(core == ONE)
            def _():
                w_start(ONE, ONE)

        when_forward(tick - ONE)(forward_out)

        for n in PAIR:
            @pl.when(tick == 3 + n)
            def _(n=n):
                for i in PAIR:
                    pass_on(in_first(G, 2 * n + i), in_second(G, 2 * n + i))

            @pl.when(tick == W_PASS[n])
            def _(n=n):
                w_pass(ONE, n)

            @pl.when(tick == W_END[n])
            def _(n=n):
                w_end(ONE, n)

        @pl.when((tick >= BACK_AT) & (tick < GRADS_AT))
        def _():
            backward_out(tick - CHUNKS)

    repeat(GRADS_AT + SENT_TILES, tick_step)

    for m, dst in enumerate((dwg, dwi)):
        for fq in PAIR:
            arrived(dst.at[:, pl.ds(pick((ONE - cx + 2 * fq, 2 * (ONE - cy) + fq), core) * WIDTH, WIDTH - m * fq * LATE_TILES * TILE)], gr_recv.at[m, fq])
    for slot in range(SLOTS):
        grad_sent(slot)
    for slot in PAIR:
        out_store(ZERO, ZERO, slot).wait()
    for i in range(CHUNKS):
        all_recv(dx_copies(i, ZERO)[ONE:])
    for i in (CHUNKS - 2, CHUNKS - ONE):
        dx_sent(i)

    def sent(copies):
        for copy in copies:
            copy.wait_send()

    for i in range(CHUNKS):
        for kind in (X, G):
            sent([*in_first(kind, i), *in_second(kind, i)])
        for block in PAIR:
            sent(out_first(block, i) + out_second(block, i))
    repeat(TASKS, lambda task: rs_copy(task).wait_send())
    for task in (TASKS - 2, TASKS - ONE):
        sent(dot_copies(task))
    for block in PAIR:
        for fq in PAIR:
            sent(w_first(ZERO, block, fq) + (w_second(ZERO, block, fq),))
            sent(w_twin(ZERO, block, fq))
    for k in range(4):
        for block in PAIR:
            @pl.when(core == block)
            def _(block=block, k=k):
                wo_copies(block, k)[ZERO].wait_send()

    def wo_sent(k):
        for block in PAIR:
            sent((wo_copies(block, k)[ONE], wo_copies(block, k)[3]))

    halves(wo_sent)
    w_hand(ZERO).wait_send()


def settle_kernel(*refs):
    for src, dst in zip(refs[:4], refs[4:]):
        dst[...] = src[...]


def settle(arrays, steps=16):
    specs = [pl.BlockSpec((arr.shape[0] // steps, arr.shape[1]), lambda i: (i, 0)) for arr in arrays]
    size = sum(arr.size * arr.dtype.itemsize for arr in arrays)
    return pl.pallas_call(
        settle_kernel, grid=(steps,), out_shape=[jax.ShapeDtypeStruct(arr.shape, arr.dtype) for arr in arrays], in_specs=specs, out_specs=specs,
        name='settle', cost_estimate=pl.CostEstimate(flops=2 ** 30, bytes_accessed=2 * size, transcendentals=0),
        compiler_params=pltpu.CompilerParams(vmem_limit_bytes=67_043_328),
    )(*arrays)


def insert_kernel(spot, late, whole, out):
    out[...] = late[...]


def insert_late(whole, late, spot):
    block = (QUARTER, QUARTER)
    return pl.pallas_call(
        insert_kernel, out_shape=jax.ShapeDtypeStruct(whole.shape, whole.dtype),
        grid_spec=pltpu.PrefetchScalarGridSpec(
            num_scalar_prefetch=1, grid=(3,), in_specs=[pl.BlockSpec(block, lambda k, spot: (0, k)), pl.BlockSpec(memory_space=pl.ANY)],
            out_specs=pl.BlockSpec(block, lambda k, spot: (0, 4 * spot[0] + 1 + k))),
        input_output_aliases={2: 0}, name='insert_late',
    )(spot, late, whole)


def solution(mesh):
    act_spec = P(None, 'data', None, None)
    weight_spec = P('stage', None, 'data', None)

    def per_device(x, g, w_gate, w_in, w_out):
        flat = (CHUNKS, 2 * ROWS, WIDTH)
        any_space = pl.BlockSpec(memory_space=pl.ANY)
        pair = (2, 2)

        def arr(*shape, dtype=BF16):
            return jax.ShapeDtypeStruct(shape, dtype)

        def f32(*shape):
            return arr(*shape, dtype=F32)

        piece = (*pair, ROWS, QUARTER)
        out_shapes = [
            arr(*flat), f32(QUARTER, 4 * WIDTH), f32(QUARTER, 4 * WIDTH), f32(WIDTH, WIDTH), f32(QUARTER, LATE_TILES * TILE),
            arr(4, *pair, CHUNKS, *pair, ROWS, QUARTER), *[arr(*pair, WIDTH, WIDTH)] * 3, arr(QUARTER, 4 * WIDTH),
            f32(TASKS, 2, *piece), f32(TASKS, *piece), f32(2 * CHUNKS, 2, ROWS, ROWS), f32(3, CHUNKS, HIDDEN_TILES, BLOCK_ROWS, WIDE),
            arr(2, SUM_TILES, TILE, WIDTH), arr(2, WIDTH, WIDTH), arr(*pair, 2, WIDTH, WIDTH), arr(2, CHUNKS, *pair, ROWS, WIDTH),
        ]

        def bf(*shape):
            return pltpu.VMEM(shape, BF16)

        def fl(*shape):
            return pltpu.VMEM(shape, F32)

        scratch = [
            bf(*pair, WIDTH, WIDE), bf(2, 4, TILE, WIDTH), fl(*pair, BLOCK_ROWS, WIDE), bf(2, *pair, ROWS, WIDTH), bf(*pair, BLOCK_ROWS, WIDTH),
            bf(SUM_TILES, TILE, BLOCK_ROWS), bf(WIDTH, BLOCK_ROWS), bf(BLOCK_ROWS, WIDE), fl(2, *pair, ROWS, TILE), fl(2, *piece), fl(2, *piece), bf(3, *piece),
            fl(2, 2, ROWS, ROWS), bf(2, *piece), bf(2, 2, ROWS, HALF), bf(2, CHUNKS, *pair, ROWS, WIDE), fl(SLOTS, 2, QUARTER, TILE), fl(2, QUARTER, WIDE),
        ]
        counts = [(4, CHUNKS, 8), (4, CHUNKS, 8), (TASKS,), (TASKS,), (2 * CHUNKS, 2), (2 * CHUNKS, 2), (*pair, 3), (*pair, 3), (*pair, 4), (*pair, 4),
                  (1,), (1,), (2, 3, 4), (2, 3, 4), (5,), (CHUNKS, 5), (CHUNKS, 4), (CHUNKS, 3), (SLOTS, 2), pair, (2,), (4,), (3,), (2, 4), pair, (2, *pair), (2, 3), (2,)]
        results = pl.pallas_call(
            step_kernel, out_shape=out_shapes, in_specs=[any_space] * 5, out_specs=[any_space] * len(out_shapes),
            scratch_shapes=scratch + [pltpu.SemaphoreType.DMA(count) for count in counts], name='mlp_step',
            compiler_params=pltpu.CompilerParams(collective_id=0, has_side_effects=True, vmem_limit_bytes=67_043_328),
        )(x.reshape(flat), g.reshape(flat), w_gate[0, 0], w_in[0, 0], w_out[0, 0])
        late = lax.ppermute(results[4], ('data', 'stage'), [(2 * c + s, 2 * (c ^ (1 + s)) + s) for c in range(4) for s in PAIR])
        chip, core = lax.axis_index('data'), lax.axis_index('stage')
        spot = jnp.where(core == 0, 3 - chip % 2, 3 - 2 * (chip // 2))
        dx, d_gate, d_in, d_out = settle((results[0].reshape(-1, WIDTH), *results[1:4]))
        d_in = insert_late(d_in, late, spot.astype(jnp.int32).reshape(1))
        return dx.reshape(x.shape), d_gate[None, None], d_in[None, None], d_out[None, None]

    return jax.shard_map(per_device, mesh=mesh, in_specs=(act_spec, act_spec, weight_spec, weight_spec, weight_spec),
                         out_specs=(act_spec, weight_spec, weight_spec, weight_spec), check_vma=False)
```
